32 devices in a mesh: gx: 8 (over y, x, core), gy: 4 (over z).
Axes of the slice: x: 2, y: 2, z: 4, core: 2. Of those that a mesh axis runs over, the one named last changes fastest.
Arguments:
- core_one: bfloat16 [200, 128], replicated, may hold values from -6 to 6
- core_two: bfloat16 [200, 4096], replicated, may hold values from -1 to 1
- core_three: bfloat16 [250, 256], replicated, may hold values from -1 to 1
- dense_rows: bfloat16 [2048, 128], P(('gx', 'gy')), may hold values from -6 to 6
- w_top: bfloat16 [256, 256], replicated, may hold values from -0.375 to 0.375
- bias_top: float32 [256], replicated, may hold values from -3 to 3
- w_out: float32 [256], replicated, may hold values from -0.75 to 0.75
- labels: int32 [2048], P(('gx', 'gy')), may hold values 0 or 1
- bag_ids: int32 [32, 256], P(('gx', 'gy')), may hold values from 0 to 63, never falling along the last dimension, each value on 1 to 8 neighbouring positions
- digit_one: int32 [32, 256], P(('gx', 'gy')), may hold values from 0 to 199
- digit_two: int32 [32, 256], P(('gx', 'gy')), may hold values from 0 to 199
- digit_three: int32 [32, 256], P(('gx', 'gy')), may hold values from 0 to 249
Outputs:
- core_grad: float32 [908800], P(('gx', 'gy'))
- top_grad: float32 [258, 256], replicated
The draws below stay inside these ranges and needn't reach their ends.
Inputs may be any that keep to these rules, and one draw needn't show every extreme that they name: `bag_ids`: along a row, never falling; every sample of the block gets 1 to 8 lookups, one exactly 8.
All inputs are finite; a program needn't handle non-finite values. No bound on the sum of `labels` on one device may be relied on, other than what follows from the above.
Results may differ from the reference program's by a relative error of at most 0.0018.
The reference program's roundings to bfloat16 on the way (of `joined` and `dpre`) count: a program that leaves them out, or rounds other values in their place, can miss the bound.
Values sent between devices are 32-bit elements; how exact they have to be, the bound alone decides.
A program may use at most 64 MiB of HBM per device.

```python
import math
import jax
import jax.numpy as jnp
import numpy as np
from jax import lax

N1 = 200
N2 = 200
N3 = 250
D1 = 4
D2 = 4
D3 = 8
R = 32
HID = 256
BAG_MOST = 8
BATCH_DEV = 64
DIM = 128
LOOKS = 256
BATCH = 2048
N_GX = 8
N_GY = 4
DEVICES = 32


def touch_ends(drawn, rng, low, largest):
    longest = drawn.shape.index(max(drawn.shape))
    spots = []
    for shift in (0, 1):
        where = [jax.random.randint(jax.random.fold_in(rng, axis), (), 0, length) for axis, length in enumerate(drawn.shape)]
        where[longest] = (where[longest] + shift) % drawn.shape[longest]
        spots.append(tuple(where))
    return drawn.at[spots[0]].set(low).at[spots[1]].set(largest)


def spiked(array, stream_key, source, target, blocks, factor):
    owner, partner = [(jnp.arange(array.shape[position]) // (array.shape[position] // blocks)).reshape([-1 if axis == position else 1 for axis in range(array.ndim)]) for position in (source, target)]
    chosen = jax.random.permutation(stream_key, blocks)[partner]
    strong = (owner == chosen) | (owner == (partner + blocks // 2) % blocks)
    return jnp.where(strong, factor * array, array)


def levels(stream_key, dims, cuts, smallest, top_value):
    def one(dim, shards_of):
        steps = jax.random.uniform(jax.random.fold_in(jax.random.fold_in(stream_key, 6), dim), (shards_of,), jnp.float32, smallest / len(cuts), top_value / len(cuts))
        return jnp.repeat(jnp.exp(steps), dims[dim] // shards_of).reshape((-1,) + (1,) * (len(dims) - dim - 1))

    factor_of = one(*cuts[0])
    for cut in cuts[1:]:
        factor_of = factor_of * one(*cut)
    return factor_of


def split_up(amount, total, reach, slope):
    loads = [(1 << 20) // math.isqrt(standing ** slope) + 1 for standing in range(2, amount + 1)]
    spare, given = total - reach - (amount - 1), [1] * (amount - 1)
    while spare > 0:
        movable = [i for i in range(amount - 1) if given[i] < reach]
        pool, left = sum([loads[i] for i in movable]), spare
        for i in movable:
            more = min(reach - given[i], max(1, left * loads[i] // pool), spare)
            given[i] = given[i] + more
            spare = spare - more
    return np.array([reach] + given)


def uneven_parts(key, number_of, total, reach, slope):
    if number_of == 2:
        one = jax.random.randint(key, (), max(1, total - reach), min(reach, total - 1) + 1)
        return jnp.stack([one, total - one])
    sizes = jnp.asarray(split_up(number_of, total, reach, slope), jnp.int32)
    pairs = (number_of - 1) // 2
    giver, receiver = sizes[1:1 + 2 * pairs:2], sizes[2:2 + 2 * pairs:2]
    room = jnp.minimum(giver - 1, reach - receiver)
    passed = jax.random.randint(jax.random.fold_in(key, 1), (pairs,), 0, 1 << 20) % (room + 1)
    sizes = sizes.at[1:1 + 2 * pairs:2].set(giver - passed).at[2:2 + 2 * pairs:2].set(receiver + passed)
    return sizes[jax.random.permutation(jax.random.fold_in(key, 2), number_of)]


def bell_draw(stream_key, shape, spread, most, cuts=(), kind=jnp.bfloat16):
    level = levels(stream_key, shape, cuts, -0.22, 0.18) if cuts else 1.0
    array = jax.random.normal(stream_key, shape, jnp.float32) * spread * level
    return jnp.minimum(jnp.maximum(array, -most), most).astype(kind)


def heavy_noise(key, shape, width, limit, cuts, heavy, held_as=jnp.bfloat16):
    result = width * jax.random.normal(key, shape, jnp.float32)
    if cuts:
        result = result * levels(key, shape, cuts, -0.22, 0.18)
    return jnp.clip(spiked(result, jax.random.fold_in(key, 3), *heavy), -limit, limit).astype(held_as)


def setup_inputs(seed: int = 0) -> dict:
    keys = jax.random.split(jax.random.key(seed), 13)
    core_one = bell_draw(keys[0], (N1, D1 * R), 1.0, 6.0)
    core_two = bell_draw(keys[1], (N2, R * D2 * R), R ** -0.5, 1.0)
    core_three = bell_draw(keys[2], (N3, R * D3), R ** -0.5, 1.0)
    dense_rows = heavy_noise(keys[3], (BATCH, DIM), 1.0, 6.0, ((0, 32),), (0, 1, 32, 2.75))
    w_top = bell_draw(keys[4], (2 * DIM, HID), (2 * DIM) ** -0.5, 0.375)
    bias_top = bell_draw(keys[5], (HID,), 0.5, 3.0, (), jnp.float32)
    w_out = bell_draw(keys[6], (HID,), (HID // 4) ** -0.5, 0.75, (), jnp.float32)
    labels = touch_ends((jax.random.randint(keys[7], (BATCH,), 0, 4) < 1).astype(jnp.int32), jax.random.fold_in(keys[7], 1), 0, 1)
    bag_ids = jax.vmap(lambda own: jnp.searchsorted(jnp.cumsum(uneven_parts(own, BATCH_DEV, LOOKS, BAG_MOST, 1)), jnp.arange(LOOKS), side="right"))(jax.random.split(keys[8], DEVICES)).reshape((DEVICES, LOOKS)).astype(jnp.int32)
    digit_one = touch_ends(jax.random.randint(keys[9], (DEVICES, LOOKS), 0, N1), jax.random.fold_in(keys[9], 1), 0, N1 - 1).astype(jnp.int32)
    digit_two = touch_ends(jax.random.randint(keys[10], (DEVICES, LOOKS), 0, N2), jax.random.fold_in(keys[10], 1), 0, N2 - 1).astype(jnp.int32)
    digit_three = touch_ends(jax.random.randint(keys[11], (DEVICES, LOOKS), 0, N3), jax.random.fold_in(keys[11], 1), 0, N3 - 1).astype(jnp.int32)
    return {"core_one": core_one, "core_two": core_two, "core_three": core_three, "dense_rows": dense_rows, "w_top": w_top, "bias_top": bias_top, "w_out": w_out, "labels": labels, "bag_ids": bag_ids, "digit_one": digit_one, "digit_two": digit_two, "digit_three": digit_three}


def reference(core_one, core_two, core_three, dense_rows, w_top, bias_top, w_out, labels, bag_ids, digit_one, digit_two, digit_three):
    high = lax.Precision.HIGHEST
    groups = N_GX * N_GY
    dense_view = dense_rows.reshape(groups, BATCH_DEV, DIM)
    label_view = labels.reshape(groups, BATCH_DEV)

    def device_terms(carry, item):
        dense_block, label_block, bags, first_digit, second_digit, third_digit = item
        first = core_one[first_digit].astype(jnp.float32).reshape(-1, D1, R)
        middle = core_two[second_digit].astype(jnp.float32).reshape(-1, R, D2 * R)
        last = core_three[third_digit].astype(jnp.float32).reshape(-1, R, D3)
        left = jnp.einsum("nia,nab->nib", first, middle, precision=high).reshape(-1, D1 * D2, R)
        embedded = jnp.einsum("npa,nad->npd", left, last, precision=high).reshape(-1, D1 * D2 * D3)
        pooled = jax.ops.segment_sum(embedded, bags, num_segments=BATCH_DEV)
        joined = jnp.concatenate([dense_block, pooled.astype(jnp.bfloat16)], axis=1)
        pre = jnp.dot(joined, w_top, preferred_element_type=jnp.float32) + bias_top[None, :]
        sig = jax.nn.sigmoid(pre)
        hidden = pre * sig
        logit = jnp.dot(hidden, w_out, precision=high)
        dlogit = (jax.nn.sigmoid(logit) - label_block.astype(jnp.float32)) / BATCH_DEV
        dpre = dlogit[:, None] * w_out[None, :] * (sig * (1.0 + pre * (1.0 - sig)))
        dpre_low = dpre.astype(jnp.bfloat16)
        grad_weight = jnp.dot(joined.T, dpre_low, preferred_element_type=jnp.float32)
        grad_bias = jnp.sum(dpre, axis=0)
        grad_output = jnp.sum(hidden * dlogit[:, None], axis=0)
        top_local = jnp.concatenate([grad_weight, grad_bias[None, :], grad_output[None, :]], axis=0)
        grad_pooled = jnp.dot(dpre_low, w_top[D1 * D2 * D3:].T, preferred_element_type=jnp.float32)
        grad_view = grad_pooled[bags].reshape(-1, D1 * D2, D3)
        grad_last = jnp.einsum("npa,npd->nad", left, grad_view, precision=high)
        grad_left = jnp.einsum("npd,nad->npa", grad_view, last, precision=high).reshape(-1, D1, D2 * R)
        grad_first = jnp.einsum("nib,nab->nia", grad_left, middle, precision=high)
        grad_middle = jnp.einsum("nia,nib->nab", first, grad_left, precision=high)
        sum_first = jax.ops.segment_sum(grad_first.reshape(-1, D1 * R), first_digit, num_segments=N1)
        sum_middle = jax.ops.segment_sum(grad_middle.reshape(-1, R * D2 * R), second_digit, num_segments=N2)
        sum_last = jax.ops.segment_sum(grad_last.reshape(-1, R * D3), third_digit, num_segments=N3)
        return (carry[0] + sum_first, carry[1] + sum_middle, carry[2] + sum_last, carry[3] + top_local), None

    start = (jnp.zeros((N1, D1 * R), jnp.float32), jnp.zeros((N2, R * D2 * R), jnp.float32),
             jnp.zeros((N3, R * D3), jnp.float32), jnp.zeros((2 * D1 * D2 * D3 + 2, HID), jnp.float32))
    totals, _ = lax.scan(device_terms, start, (dense_view, label_view, bag_ids, digit_one, digit_two, digit_three))
    core_grad = jnp.concatenate([totals[0].reshape(-1), totals[1].reshape(-1), totals[2].reshape(-1)])
    return core_grad, totals[3]
```

```python
import functools
import types

import jax
import jax.numpy as jnp
from jax import lax
from jax.experimental import pallas as pl
from jax.experimental.pallas import tpu as pltpu
from jax.sharding import PartitionSpec as P

D1 = 4
D2 = 4
D3 = 8
R = 32
WIDTH = D1 * D2 * D3
PAIRS = D1 * D2
SIDE = D2 * R
LANES = 128
AXES = ("gx", "gy")
F32 = jnp.float32
BF16 = jnp.bfloat16
HIGH = lax.Precision.HIGHEST
PLAIN, ACROSS, DOWN = ((1,), (0,)), ((1,), (1,)), ((0,), (0,))


def dot(a, b, dims, precision=None):
    return lax.dot_general(
        a, b, (dims, ((), ())), precision=precision, preferred_element_type=F32
    )


def parts_of(x, count):
    parts = []
    for _ in range(count):
        part = x.astype(BF16)
        parts.append(part)
        x = x - part.astype(F32)
    return parts


def dot_parts(a, b, dims, count, wide):
    total = None
    for part in parts_of((a, b)[wide], count):
        term = dot(part, b, dims) if wide == 0 else dot(a, part, dims)
        total = term if total is None else total + term
    return total


def hot(row, count, kind):
    numbers = lax.broadcasted_iota(jnp.int32, (count, row.shape[1]), 0)
    return jnp.where(numbers == row, 1.0, 0.0).astype(kind)


def by_d3(last_t):
    size = R * D3
    to = lax.broadcasted_iota(jnp.int32, (size, size), 0)
    of = lax.broadcasted_iota(jnp.int32, (size, size), 1)
    turn = jnp.where(of == (to % R) * D3 + to // R, 1.0, 0.0).astype(BF16)
    return dot(turn, last_t, PLAIN)


def up(count, step):
    return -(-count // step) * step


def plan_of(nx, ny, shape_one, shape_two, shape_three, shape_top):
    cores = 2
    if nx % cores:
        return None
    chips, planes, devices = nx // cores, ny, nx * ny
    n1, n2, n3 = (s[0] * s[1] for s in (shape_one, shape_two, shape_three))
    total = n1 + n2 + n3
    if total % devices or shape_one[1] != LANES or n1 % LANES or shape_two[1] % LANES:
        return None
    if shape_three[1] != cores * LANES or shape_top[1] != cores * LANES or shape_top[0] % (8 * chips):
        return None
    share = total // devices
    row = shape_two[1]
    window = min(-(-share // row) + 1, shape_two[0])
    segs, offset = [None] * planes, 0
    for d in range(devices):
        lo, hi = d * share, (d + 1) * share
        has_first, has_last = lo < n1, hi > n1 + n2
        if not (has_first or has_last):
            continue
        if has_first and has_last or segs[d % planes] is not None:
            return None
        seg = types.SimpleNamespace(owner=d // planes, first=has_first)
        if has_first:
            seg.lo, seg.hi = lo // LANES, -(-min(hi, n1) // LANES)
            seg.rows = up(-(-(seg.hi - seg.lo) // (cores * chips)), 8)
        else:
            seg.lo = max(lo - n1 - n2, 0) // shape_three[1] // 8 * 8
            seg.hi = -(-(hi - n1 - n2) // shape_three[1])
            seg.rows = up(-(-(seg.hi - seg.lo) // chips), 8)
        segs[d % planes] = seg
    if any(seg is None for seg in segs):
        return None
    for seg in segs:
        seg.offset = offset
        offset += seg.rows
    return types.SimpleNamespace(
        nx=nx, ny=ny, cores=cores, chips=chips, planes=planes, share=share, window=window,
        row=row, n1=n1, segs=segs, srows=offset, smost=max(seg.rows for seg in segs),
        trows=shape_top[0] // chips + 8, n2_rows=shape_two[0], n3_rows=shape_three[0])


def pieces_of(seg, cores, chips, halves):
    for core in range(cores):
        for chip in range(chips):
            n = core * chips + chip if seg.first else chip
            lo = seg.lo + n * seg.rows
            hi = min(lo + seg.rows, seg.hi)
            if lo < hi:
                yield core, chip, lo, hi, 0 if seg.first else core


def grad_left_into(gleft_s, g_s, lastd_s):
    @pl.loop(0, PAIRS)
    def _(p):
        total = None
        for d in range(D3):
            term = g_s[pl.ds(p * D3 + d, 1), :] * lastd_s[d * R:(d + 1) * R, :]
            total = term if total is None else total + term
        gleft_s[pl.ds(pl.multiple_of(p * R, R), R), :] = total


STAGES = ("dz", "dx", "dc", "gz", "gx", "gc", "t0", "t1", "t2", "t3", "t4", "s0", "s1", "s2", "s3")


def stage_sizes(plan):
    cores, chips, planes = plan.cores, plan.chips, plan.planes
    gather = dict(z=planes, x=chips * planes, c=cores * planes)
    sizes = {kind + axis: size for kind in "dg" for axis, size in gather.items()}
    sizes.update(t0=cores, t1=chips, t2=planes, t3=chips, t4=cores,
                 s0=cores, s1=chips, s2=planes, s3=cores * chips)
    return [sizes[name] for name in STAGES]


def step_kernel(plan, *refs):
    inputs, refs = refs[:12], refs[12:]
    digits_ref, gp_ref, top_ref, seg_ref = refs[:4]
    held, refs = refs[4:16], refs[16:]
    mid_s, first_s, last_s, lastd_s, left_s, gleft_s, emb_s, g_s, gf_s, gl_s = refs[:10]
    top_s, topin, top1, topx, topz, seg_s, segin, seg1, segx, seg2, segz, seg3 = refs[10:22]
    load_sems, sems = refs[22], refs[23:]
    sems = {name: (sems[2 * i], sems[2 * i + 1]) for i, name in enumerate(STAGES)}
    cores, chips, planes = plan.cores, plan.chips, plan.planes
    gx, plane = lax.axis_index("gx"), lax.axis_index("gy")
    core, chip = gx % cores, gx // cores

    loads = [pltpu.make_async_copy(a, b, load_sems.at[k])
             for k, (a, b) in enumerate(zip(inputs, held))]
    for load in loads:
        load.start()

    def at(c, q, p):
        return (q * cores + c, p)

    def on_core(k):
        return at((core + k) % cores, chip, plane)

    def on_chip(k):
        return at(core, (chip + k) % chips, plane)

    def on_plane(k):
        return at(core, chip, (plane + k) % planes)

    barrier = pltpu.get_barrier_semaphore()
    peers = [at((core + c) % cores, (chip + q) % chips, plane)
             for c in range(cores) for q in range(chips) if c or q]
    peers += [on_plane(k) for k in range(1, planes)]
    for peer in peers:
        pl.semaphore_signal(barrier, inc=1, device_id=peer, device_id_type=pl.DeviceIdType.MESH)

    sent = []

    def remote(src, dst, stage, k, peer):
        return pltpu.make_async_remote_copy(
            src_ref=src, dst_ref=dst, send_sem=sems[stage][0].at[k],
            recv_sem=sems[stage][1].at[k], device_id=peer,
            device_id_type=pl.DeviceIdType.MESH)

    def push(src, dst, stage, k, peer):
        copy = remote(src, dst, stage, k, peer)
        copy.start()
        sent.append(copy)

    def arrive(ref, stage, k):
        remote(ref, ref, stage, k, on_plane(1)).wait_recv()

    def back(me, k, size):
        return (me + size - k) % size

    class Gather:
        def __init__(self, ref, kind):
            self.ref, self.kind = ref, kind

        def own(self):
            slot = self.ref.at[core, plane, chip]
            for k in range(1, planes):
                push(slot, slot, self.kind + "z", k, on_plane(k))
            for q in range(1, chips):
                push(slot, slot, self.kind + "x", q * planes, on_chip(q))

        def relay_z(self, k):
            slot = self.ref.at[core, back(plane, k, planes), chip]
            arrive(slot, self.kind + "z", k)
            for q in range(1, chips):
                push(slot, slot, self.kind + "x", q * planes + k, on_chip(q))

        def relay_x(self, k):
            z = back(plane, k, planes)
            for q in range(1, chips):
                arrive(self.ref.at[core, z, back(chip, q, chips)], self.kind + "x", q * planes + k)
            slot = self.ref.at[core, z]
            for c in range(1, cores):
                push(slot, slot, self.kind + "c", c * planes + k, on_core(c))

        def finish(self, k):
            for c in range(1, cores):
                slot = self.ref.at[back(core, c, cores), back(plane, k, planes)]
                arrive(slot, self.kind + "c", c * planes + k)

    digits, grads = Gather(digits_ref, "d"), Gather(gp_ref, "g")

    for load in loads:
        load.wait()
    c1, c2, c3, dense, w, bias, wout, labels, bag, d1, d2, d3 = held
    samples, looks = dense.shape[0], d1.shape[1]
    per = looks // LANES
    for k, digit in enumerate((bag, d1, d2, d3)):
        for h in range(per):
            digits_ref[core, plane, chip, k * per + h:k * per + h + 1, :] = (
                digit[:, h * LANES:(h + 1) * LANES].astype(F32))

    hot1 = hot(d1[...], c1.shape[0], BF16)
    hot2 = hot(d2[...], c2.shape[0], BF16)
    hot3 = hot(d3[...], c3.shape[0], BF16)
    for start in range(0, R * SIDE, 512):
        mid_s[start:start + 512, :] = dot(c2[:, start:start + 512], hot2, DOWN)
    first_s[...] = dot(c1[...], hot1, DOWN)
    last_t = dot(c3[...], hot3, DOWN)
    last_s[...] = last_t
    lastd_s[...] = by_d3(last_t.astype(BF16))

    pl.semaphore_wait(barrier, len(peers))
    digits.own()

    lane_blocks = looks // LANES

    @pl.loop(0, D2 * lane_blocks)
    def _(step):
        j = step // lane_blocks
        lanes = pl.ds(pl.multiple_of((step % lane_blocks) * LANES, LANES), LANES)
        totals = [None] * D1
        for a in range(R):
            m = mid_s[pl.ds(pl.multiple_of(a * SIDE + j * R, R), R), lanes]
            for i in range(D1):
                term = first_s[i * R + a:i * R + a + 1, lanes] * m
                totals[i] = term if totals[i] is None else totals[i] + term
        for i in range(D1):
            left_s[pl.ds(pl.multiple_of(i * SIDE + j * R, R), R), lanes] = totals[i]

    @pl.loop(0, PAIRS)
    def _(p):
        totals = [None, None]
        for c in range(R):
            term = left_s[pl.ds(p * R + c, 1), :] * last_s[c * D3:(c + 1) * D3, :]
            k = c % 2
            totals[k] = term if totals[k] is None else totals[k] + term
        emb_s[pl.ds(pl.multiple_of(p * D3, D3), D3), :] = totals[0] + totals[1]

    for k in range(1, planes):
        digits.relay_z(k)

    bags = hot(bag[...], samples, BF16)
    pooled = dot_parts(bags, emb_s[...], ACROSS, 3, 1).astype(BF16)
    pre = (
        dot(dense[...], w[:WIDTH, :], PLAIN) + dot(pooled, w[WIDTH:, :], PLAIN)
        + bias[...]
    )
    sig = jax.nn.sigmoid(pre)
    hidden = pre * sig
    logit = jnp.sum(hidden * wout[...], axis=1, keepdims=True)
    rows = lax.broadcasted_iota(jnp.int32, (samples, samples), 0)
    cols = lax.broadcasted_iota(jnp.int32, (samples, samples), 1)
    label = jnp.sum(
        jnp.where(rows == cols, labels[...].astype(F32), 0.0), axis=1, keepdims=True
    )
    dlogit = (jax.nn.sigmoid(logit) - label) / samples
    dpre = dlogit * wout[...] * (sig * (1.0 + pre * (1.0 - sig)))
    low = dpre.astype(BF16)
    gp = dot(low, w[WIDTH:, :], ACROSS)
    gp_ref[core, plane, chip] = gp
    grads.own()

    deep = plan.trows - 8
    vectors = jnp.concatenate(
        [jnp.sum(dpre, axis=0, keepdims=True), jnp.sum(hidden * dlogit, axis=0, keepdims=True),
         jnp.zeros((6, dpre.shape[1]), F32)], axis=0)
    weight = [dot(dense[...], low, DOWN), dot(pooled, low, DOWN)]
    for h in range(cores):
        lanes = slice(h * LANES, (h + 1) * LANES)
        for q in range(chips):
            lo = q * deep
            half = weight[lo // WIDTH]
            top_s[h, q, :deep, :] = half[lo % WIDTH:lo % WIDTH + deep, lanes]
            top_s[h, q, deep:, :] = vectors[:, lanes] if q == 0 else jnp.zeros((8, LANES), F32)
    for c in range(1, cores):
        push(top_s.at[(core + c) % cores], topin.at[c], "t0", c, on_core(c))

    g_s[...] = dot_parts(gp, bags, DOWN, 2, 0)
    grad_left_into(gleft_s, g_s, lastd_s)
    for k in range(planes):
        digits.relay_x(k)

    total = top_s[core]
    for c in range(1, cores):
        arrive(topin.at[c], "t0", c)
        total = total + topin[c]
    top1[...] = total
    for k in range(1, chips):
        push(top1.at[(chip + k) % chips], topx.at[k], "t1", k, on_chip(k))

    @pl.loop(0, R)
    def _(c):
        totals = [None, None]
        for p in range(PAIRS):
            term = left_s[pl.ds(p * R + c, 1), :] * g_s[p * D3:(p + 1) * D3, :]
            k = p % 2
            totals[k] = term if totals[k] is None else totals[k] + term
        gl_s[pl.ds(pl.multiple_of(c * D3, D3), D3), :] = totals[0] + totals[1]

    @pl.loop(0, R)
    def _(a):
        totals = [None] * D1
        for t in range(0, SIDE, 8):
            m = mid_s[pl.ds(pl.multiple_of(a * SIDE + t, 8), 8), :]
            for i in range(D1):
                term = gleft_s[i * SIDE + t:i * SIDE + t + 8, :] * m
                totals[i] = term if totals[i] is None else totals[i] + term
        for i in range(D1):
            gf_s[pl.ds(i * R + a, 1), :] = jnp.sum(totals[i], axis=0, keepdims=True)

    sums = {True: dot_parts(hot1, gf_s[...], ACROSS, 2, 1),
            False: dot_parts(hot3, gl_s[...], ACROSS, 2, 1)}
    seg_s[...] = jnp.zeros_like(seg_s)
    for seg in plan.segs:
        for c, q, lo, hi, h in pieces_of(seg, cores, chips, cores):
            seg_s[c, q, seg.offset:seg.offset + hi - lo, :] = (
                sums[seg.first][lo:hi, h * LANES:(h + 1) * LANES])
    for c in range(1, cores):
        push(seg_s.at[(core + c) % cores], segin.at[c], "s0", c, on_core(c))

    for k in range(1, planes):
        grads.relay_z(k)

    total = top1[chip]
    for k in range(1, chips):
        arrive(topx.at[k], "t1", k)
        total = total + topx[k]
    topz[plane] = total
    for k in range(1, planes):
        push(topz.at[plane], topz.at[plane], "t2", k, on_plane(k))

    total = seg_s[core]
    for c in range(1, cores):
        arrive(segin.at[c], "s0", c)
        total = total + segin[c]
    seg1[...] = total
    for k in range(1, chips):
        push(seg1.at[(chip + k) % chips], segx.at[k], "s1", k, on_chip(k))

    for k in range(planes):
        grads.relay_x(k)

    total = seg1[chip]
    for k in range(1, chips):
        arrive(segx.at[k], "s1", k)
        total = total + segx[k]
    seg2[...] = total

    def out_of(p, k):
        seg = plan.segs[(p + k) % planes]
        return remote(seg2.at[seg.offset:seg.offset + seg.rows],
                      segz.at[k, :seg.rows], "s2", k, on_plane(k))

    for p in range(planes):
        @pl.when(plane == p)
        def _(p=p):
            for k in range(1, planes):
                out_of(p, k).start()

    for k in range(1, planes):
        arrive(topz.at[back(plane, k, planes)], "t2", k)
    total = topz[0]
    for k in range(1, planes):
        total = total + topz[k]
    top_ref[core, chip] = total
    for k in range(1, chips):
        push(top_ref.at[core, chip], top_ref.at[core, chip], "t3", k, on_chip(k))

    def to_owner(p):
        seg = plan.segs[p]
        return remote(seg3.at[:seg.rows], seg_ref.at[core, chip, :seg.rows], "s3",
                      core * chips + chip, (seg.owner, plane))

    for p in range(planes):
        @pl.when(plane == p)
        def _(p=p):
            seg = plan.segs[p]
            total = seg2[seg.offset:seg.offset + seg.rows]
            for k in range(1, planes):
                arrive(segz.at[k, :seg.rows], "s2", k)
                total = total + segz[k, :seg.rows]
            seg3[:seg.rows] = total

            @pl.when(gx != seg.owner)
            def _():
                to_owner(p).start()

    for k in range(1, chips):
        arrive(top_ref.at[core, back(chip, k, chips)], "t3", k)
    for c in range(1, cores):
        push(top_ref.at[core], top_ref.at[core], "t4", c, on_core(c))

    for p in range(planes):
        seg = plan.segs[p]

        @pl.when((plane == p) & (gx == seg.owner))
        def _(p=p, seg=seg):
            own_core, own_chip = seg.owner % cores, seg.owner // cores
            seg_ref[own_core, own_chip, :seg.rows] = seg3[:seg.rows]
            for c in range(cores):
                for q in range(chips):
                    if (c, q) != (own_core, own_chip):
                        arrive(seg_ref.at[c, q, :seg.rows], "s3", c * chips + q)

    for k in range(planes):
        digits.finish(k)
        grads.finish(k)
    for c in range(1, cores):
        arrive(top_ref.at[back(core, c, cores)], "t4", c)
    for copy in sent:
        copy.wait_send()
    for p in range(planes):
        @pl.when(plane == p)
        def _(p=p):
            for k in range(1, planes):
                out_of(p, k).wait_send()

            @pl.when(gx != plan.segs[p].owner)
            def _():
                to_owner(p).wait_send()


def step_part(plan, *inputs):
    c1, c2, c3, dense, w, bias, wout, labels, bag, d1, d2, d3 = inputs
    samples, looks = dense.shape[0], d1.shape[1]
    cores, chips, planes = plan.cores, plan.chips, plan.planes
    shape = lambda *dims: jax.ShapeDtypeStruct(dims, F32)
    vmem = pl.BlockSpec(memory_space=pltpu.VMEM)
    scratch = [R * SIDE, D1 * R, R * D3, R * D3, D1 * SIDE, D1 * SIDE, WIDTH, WIDTH, D1 * R, R * D3]
    top, seg = (plan.trows, LANES), (plan.srows, LANES)
    sums = [
        (cores, chips, *top), (cores, chips, *top), (chips, *top), (chips, *top), (planes, *top),
        (cores, chips, *seg), (cores, chips, *seg), (chips, *seg), (chips, *seg), seg,
        (planes, plan.smost, LANES), (plan.smost, LANES)]
    return pl.pallas_call(
        functools.partial(step_kernel, plan),
        in_specs=[pl.BlockSpec(memory_space=pltpu.HBM)] * len(inputs),
        out_specs=(vmem,) * 4,
        out_shape=(
            shape(cores, planes, chips, up(4 * looks // LANES, 8), LANES),
            shape(cores, planes, chips, samples, WIDTH),
            shape(cores, chips, *top),
            shape(cores, chips, plan.smost, LANES),
        ),
        scratch_shapes=[pltpu.VMEM(x.shape, x.dtype) for x in inputs]
        + [pltpu.VMEM((rows, looks), F32) for rows in scratch]
        + [pltpu.VMEM(dims, F32) for dims in sums]
        + [pltpu.SemaphoreType.DMA((len(inputs),))]
        + [pltpu.SemaphoreType.DMA((size,)) for size in stage_sizes(plan) for _ in range(2)],
        compiler_params=pltpu.CompilerParams(
            collective_id=0, has_side_effects=True, vmem_limit_bytes=40 << 20),
        name="step",
    )(*inputs)


def finish_kernel(
    plan, chunk, c1, c3, digits_in, gp_in, top, seg_in, core_ref, top_ref,
    rank_s, vals_s, g_s, lastd_s, gleft_s, big_s,
):
    cores, chips, planes, window = plan.cores, plan.chips, plan.planes, plan.window
    gx, plane = lax.axis_index("gx"), lax.axis_index("gy")
    start = (gx * planes + plane) * plan.share
    r0 = jnp.clip((start - plan.n1) // plan.row, 0, plan.n2_rows - window)
    samples = gp_in.shape[3]
    groups = cores * planes * chips
    gp = gp_in[...].reshape(groups * samples, WIDTH)
    blocks = digits_in[...].reshape(groups, *digits_in.shape[3:])

    deep = plan.trows - 8
    for h in range(cores):
        lanes = slice(h * LANES, (h + 1) * LANES)
        for q in range(chips):
            top_ref[q * deep:(q + 1) * deep, lanes] = top[h, q, :deep, :]
        top_ref[chips * deep:, lanes] = top[h, 0, deep:deep + 2, :]

    looks = rank_s.shape[1]
    per = looks // LANES
    digits = [
        jnp.concatenate([blocks[:, k * per + h, :] for h in range(per)], axis=1).astype(jnp.int32)
        for k in range(4)
    ]
    rel = digits[2] - r0
    inside = (rel >= 0) & (rel < window)
    low = jnp.where(inside, 1.0, 0.0).astype(BF16)
    tri = jnp.where(
        lax.broadcasted_iota(jnp.int32, (looks, looks), 0)
        < lax.broadcasted_iota(jnp.int32, (looks, looks), 1), 1.0, 0.0).astype(BF16)
    above = jnp.where(
        lax.broadcasted_iota(jnp.int32, (groups, groups), 0)
        > lax.broadcasted_iota(jnp.int32, (groups, groups), 1), 1.0, 0.0).astype(BF16)
    before = jnp.sum(dot(above, low, PLAIN), axis=1, keepdims=True)
    rank_s[...] = jnp.where(inside, dot(low, tri, PLAIN) + before, -1.0).astype(jnp.int32)
    count = jnp.sum(jnp.where(inside, 1, 0))
    group = lax.broadcasted_iota(jnp.int32, (groups, looks), 0)
    columns = (digits[0], digits[1], digits[3], group, jnp.where(inside, rel + 1, 0))
    for k, column in enumerate(columns):
        vals_s[:, k:k + 1, :] = column.astype(F32).reshape(groups, 1, looks)
    vals_s[:, len(columns):, :] = jnp.zeros((groups, 8 - len(columns), looks), F32)
    base = plan.n1 // LANES
    rows = window * R
    big_s[base:base + rows, :] = jnp.zeros((rows, LANES), F32)
    gp_high, gp_low = parts_of(gp, 2)
    slots = lax.broadcasted_iota(jnp.int32, (chunk, looks), 0)

    def body(step, carry):
        def pick(e, found):
            ranks = rank_s[pl.ds(e, 1), :] - step * chunk
            chosen = jnp.where(slots == ranks, 1.0, 0.0).astype(BF16)
            return found + dot(vals_s[e].astype(BF16), chosen, ACROSS)

        found = lax.fori_loop(0, groups, pick, jnp.zeros((8, chunk), F32), unroll=4)
        found = found.astype(jnp.int32)
        bag, d1, d3, owner, rel1 = (found[k:k + 1, :] for k in range(5))
        first = dot(c1[...], hot(d1, c1.shape[0], BF16), DOWN)
        last = dot(c3[...], hot(d3, c3.shape[0], BF16), DOWN)
        lastd_s[...] = by_d3(last.astype(BF16))
        sample = hot(owner * samples + bag, gp.shape[0], BF16)
        g_s[...] = dot(gp_high, sample, DOWN) + dot(gp_low, sample, DOWN)
        grad_left_into(gleft_s, g_s, lastd_s)
        total = big_s[base:base + rows, :]
        for i in range(D1):
            part = first[i * R:(i + 1) * R, :]
            spread = jnp.concatenate(
                [jnp.where(rel1 == r + 1, part, 0.0) for r in range(window)], axis=0
            ).astype(BF16)
            total = total + dot_parts(spread, gleft_s[i * SIDE:(i + 1) * SIDE, :], ACROSS, 2, 1)
        big_s[base:base + rows, :] = total
        return carry

    lax.fori_loop(0, (count + chunk - 1) // chunk, body, 0)

    halves = seg_in.shape[0]
    for p in range(planes):
        seg = plan.segs[p]

        @pl.when((plane == p) & (gx == seg.owner))
        def _(seg=seg):
            for c, q, lo, hi, h in pieces_of(seg, cores, chips, halves):
                piece = seg_in[c, q, :hi - lo, :]
                if seg.first:
                    big_s[lo:hi, :] = piece
                else:
                    big_s[pl.ds(base + rows + lo * halves + h, hi - lo, stride=halves), :] = piece

    at = start // LANES - r0 * (plan.row // LANES)
    shift = start % LANES
    count = core_ref.shape[0]
    here, after = big_s[pl.ds(at, count), :], big_s[pl.ds(at + 1, count), :]
    turn = (LANES - shift) % LANES
    lane = lax.broadcasted_iota(jnp.int32, (count, LANES), 1)
    core_ref[...] = jnp.where(
        lane < LANES - shift, pltpu.roll(here, turn, 1), pltpu.roll(after, turn, 1))


def finish_part(plan, looks, c1, c3, digits, gp, top, seg):
    groups = plan.cores * plan.chips * plan.planes
    chunk = 512
    vmem = pl.BlockSpec(memory_space=pltpu.VMEM)
    last_rows = plan.n3_rows * seg.shape[0]
    out_rows = up(-(-plan.share // LANES), 8)
    big = up(plan.n1 // LANES + plan.window * R + last_rows + out_rows, 8)
    return pl.pallas_call(
        functools.partial(finish_kernel, plan, chunk),
        out_shape=(
            jax.ShapeDtypeStruct((out_rows, LANES), F32),
            jax.ShapeDtypeStruct((plan.chips * (plan.trows - 8) + 2, plan.cores * LANES), F32),
        ),
        in_specs=[vmem] * 6,
        out_specs=(vmem, vmem),
        scratch_shapes=[
            pltpu.VMEM((groups, looks), jnp.int32),
            pltpu.VMEM((groups, 8, looks), F32),
            pltpu.VMEM((WIDTH, chunk), F32),
            pltpu.VMEM((R * D3, chunk), F32),
            pltpu.VMEM((D1 * SIDE, chunk), F32),
            pltpu.VMEM((big, LANES), F32),
        ],
        compiler_params=pltpu.CompilerParams(vmem_limit_bytes=40 << 20),
        name="finish",
    )(c1, c3, digits, gp, top, seg)


def per_device(plan, c1, c2, c3, dense, w, bias, wout, labels, bag, d1, d2, d3):
    digits, gp, top, seg = step_part(
        plan, c1, c2, c3, dense, w, bias[None], wout[None], labels[None], bag, d1, d2, d3)
    core, top = finish_part(plan, d1.shape[1], c1, c3, digits, gp, top, seg)
    return core.reshape(-1)[:plan.share], top


def one_hot(digits, count, kind):
    return (digits[:, None] == jnp.arange(count, dtype=jnp.int32)[None, :]).astype(kind)


def slices(digits, core):
    return jnp.dot(
        one_hot(digits, core.shape[0], jnp.bfloat16), core, preferred_element_type=jnp.float32
    )


def factors(digits, cores):
    high = lax.Precision.HIGHEST
    first = slices(digits[0], cores[0]).reshape(-1, D1, R)
    middle = slices(digits[1], cores[1]).reshape(-1, R, D2 * R)
    last = slices(digits[2], cores[2]).reshape(-1, R, D3)
    left = jnp.einsum("nia,nab->nib", first, middle, precision=high).reshape(-1, D1 * D2, R)
    return (first, middle, last, left)


def top_total(top_local):
    return lax.psum(top_local, ("gx", "gy"))


def per_device_dense(
    core_one,
    core_two,
    core_three,
    dense_rows,
    w_top,
    bias_top,
    w_out,
    labels,
    bag_ids,
    digit_one,
    digit_two,
    digit_three,
):
    high = lax.Precision.HIGHEST
    cores = (core_one, core_two, core_three)
    digits = jnp.stack([digit_one[0], digit_two[0], digit_three[0]])
    looks = digits.shape[1]
    block = min(256, looks)
    blocks = looks // block
    blocked = digits.reshape(3, blocks, block).transpose(1, 0, 2)
    width = D1 * D2 * D3

    def forward(carry, part):
        first, middle, last, left = factors(part, cores)
        return (carry, jnp.einsum("npa,nad->npd", left, last, precision=high).reshape(block, width))

    _, embedded = lax.scan(forward, jnp.zeros((), jnp.float32), blocked)
    embedded = embedded.reshape(looks, width)
    samples = dense_rows.shape[0]
    bag_table = one_hot(bag_ids[0], samples, jnp.float32)
    pooled = jnp.dot(bag_table.T, embedded, precision=high)
    joined = jnp.concatenate([dense_rows, pooled.astype(jnp.bfloat16)], axis=1)
    pre = jnp.dot(joined, w_top, preferred_element_type=jnp.float32) + bias_top[None, :]
    sig = jax.nn.sigmoid(pre)
    hidden = pre * sig
    logit = jnp.dot(hidden, w_out, precision=high)
    dlogit = (jax.nn.sigmoid(logit) - labels.astype(jnp.float32)) / samples
    dpre = dlogit[:, None] * w_out[None, :] * (sig * (1.0 + pre * (1.0 - sig)))
    dpre_low = dpre.astype(jnp.bfloat16)
    grad_weight = jnp.dot(joined.T, dpre_low, preferred_element_type=jnp.float32)
    grad_bias = jnp.sum(dpre, axis=0)
    grad_output = jnp.sum(hidden * dlogit[:, None], axis=0)
    top_local = jnp.concatenate([grad_weight, grad_bias[None, :], grad_output[None, :]], axis=0)
    grad_pooled = jnp.dot(dpre_low, w_top[width:].T, preferred_element_type=jnp.float32)
    grad_embedded = jnp.dot(bag_table, grad_pooled, precision=high).reshape(blocks, block, width)

    def backward(totals, inputs):
        part, grad_block = inputs
        first, middle, last, left = factors(part, cores)
        grad_view = grad_block.reshape(block, D1 * D2, D3)
        grad_last = jnp.einsum("npa,npd->nad", left, grad_view, precision=high)
        grad_left = jnp.einsum("npd,nad->npa", grad_view, last, precision=high).reshape(
            block, D1, D2 * R
        )
        grad_first = jnp.einsum("nib,nab->nia", grad_left, middle, precision=high)
        grad_middle = jnp.einsum("nia,nib->nab", first, grad_left, precision=high)
        pieces = (
            grad_first.reshape(block, -1),
            grad_middle.reshape(block, -1),
            grad_last.reshape(block, -1),
        )
        updated = tuple(
            (
                total
                + jnp.dot(
                    one_hot(part[number], cores[number].shape[0], jnp.float32).T,
                    pieces[number],
                    precision=high,
                )
                for number, total in enumerate(totals)
            )
        )
        return (updated, None)

    start = tuple((jnp.zeros(core.shape, jnp.float32) for core in cores))
    totals, _ = lax.scan(backward, start, (blocked, grad_embedded))
    flat = jnp.concatenate([total.reshape(-1) for total in totals])
    core_grad = lax.psum_scatter(flat, ("gx", "gy"), scatter_dimension=0, tiled=True)
    top_grad = top_total(top_local)
    return (core_grad, top_grad)


def solution(mesh):
    nx, ny = mesh.shape["gx"], mesh.shape["gy"]
    whole, split, rows = P(), P(AXES), P(AXES, None)

    def step(*args):
        cores, dense = args[:3], args[3]
        plan = None
        if dense.size < sum(core.size for core in cores):
            plan = plan_of(nx, ny, *(core.shape for core in cores), args[4].shape)
        body = functools.partial(per_device, plan) if plan else per_device_dense
        return jax.shard_map(
            body,
            mesh=mesh,
            in_specs=(
                whole, whole, whole, rows, whole, whole, whole, split,
                rows, rows, rows, rows,
            ),
            out_specs=(split, whole),
            check_vma=False,
        )(*args)

    return step
```

```python
import functools
import types

import jax
import jax.numpy as jnp
from jax import lax
from jax.experimental import pallas as pl
from jax.experimental.pallas import tpu as pltpu
from jax.sharding import PartitionSpec as P

D1 = 4
D2 = 4
D3 = 8
R = 32
WIDTH = D1 * D2 * D3
PAIRS = D1 * D2
SIDE = D2 * R
LANES = 128
AXES = ("gx", "gy")
F32 = jnp.float32
BF16 = jnp.bfloat16
HIGH = lax.Precision.HIGHEST
PLAIN, ACROSS, DOWN = ((1,), (0,)), ((1,), (1,)), ((0,), (0,))


def dot(a, b, dims, precision=None):
    return lax.dot_general(
        a, b, (dims, ((), ())), precision=precision, preferred_element_type=F32
    )


def parts_of(x, count):
    parts = []
    for _ in range(count):
        part = x.astype(BF16)
        parts.append(part)
        x = x - part.astype(F32)
    return parts


def dot_parts(a, b, dims, count, wide):
    total = None
    for part in parts_of((a, b)[wide], count):
        term = dot(part, b, dims) if wide == 0 else dot(a, part, dims)
        total = term if total is None else total + term
    return total


def hot(row, count, kind):
    numbers = lax.broadcasted_iota(jnp.int32, (count, row.shape[1]), 0)
    return jnp.where(numbers == row, 1.0, 0.0).astype(kind)


def by_d3(last_t):
    size = R * D3
    to = lax.broadcasted_iota(jnp.int32, (size, size), 0)
    of = lax.broadcasted_iota(jnp.int32, (size, size), 1)
    turn = jnp.where(of == (to % R) * D3 + to // R, 1.0, 0.0).astype(BF16)
    return dot(turn, last_t, PLAIN)


def up(count, step):
    return -(-count // step) * step


def plan_of(nx, ny, shape_one, shape_two, shape_three, shape_top):
    cores = 2
    if nx % cores:
        return None
    chips, planes, devices = nx // cores, ny, nx * ny
    n1, n2, n3 = (s[0] * s[1] for s in (shape_one, shape_two, shape_three))
    total = n1 + n2 + n3
    if total % devices or shape_one[1] != LANES or n1 % LANES or shape_two[1] % LANES:
        return None
    if shape_three[1] != cores * LANES or shape_top[1] != cores * LANES or shape_top[0] % (8 * chips):
        return None
    share = total // devices
    row = shape_two[1]
    window = min(-(-share // row) + 1, shape_two[0])
    segs, offset = [None] * planes, 0
    for d in range(devices):
        lo, hi = d * share, (d + 1) * share
        has_first, has_last = lo < n1, hi > n1 + n2
        if not (has_first or has_last):
            continue
        if has_first and has_last or segs[d % planes] is not None:
            return None
        seg = types.SimpleNamespace(owner=d // planes, first=has_first)
        if has_first:
            seg.lo, seg.hi = lo // LANES, -(-min(hi, n1) // LANES)
            seg.rows = up(-(-(seg.hi - seg.lo) // (cores * chips)), 8)
        else:
            seg.lo = max(lo - n1 - n2, 0) // shape_three[1] // 8 * 8
            seg.hi = -(-(hi - n1 - n2) // shape_three[1])
            seg.rows = up(-(-(seg.hi - seg.lo) // chips), 8)
        segs[d % planes] = seg
    if any(seg is None for seg in segs):
        return None
    for seg in segs:
        seg.offset = offset
        offset += seg.rows
    return types.SimpleNamespace(
        nx=nx, ny=ny, cores=cores, chips=chips, planes=planes, share=share, window=window,
        row=row, n1=n1, segs=segs, srows=offset, smost=max(seg.rows for seg in segs),
        trows=shape_top[0] // chips + 8, n2_rows=shape_two[0], n3_rows=shape_three[0])


def pieces_of(seg, cores, chips, halves):
    for core in range(cores):
        for chip in range(chips):
            n = core * chips + chip if seg.first else chip
            lo = seg.lo + n * seg.rows
            hi = min(lo + seg.rows, seg.hi)
            if lo < hi:
                yield core, chip, lo, hi, 0 if seg.first else core


def spans(count, step):
    return [(lo, min(step, count - lo)) for lo in range(0, count, step)]


def lane_loop(count, lanes, body):
    blocks = lanes // LANES

    @pl.loop(0, count * blocks)
    def _(step):
        body(step // blocks, pl.ds(pl.multiple_of((step % blocks) * LANES, LANES), LANES))


def add(total, term):
    return term if total is None else total + term


def left_into(left_s, first_s, mid_s):
    def body(j, lanes):
        totals = [None] * D1
        for a in range(R):
            m = mid_s[pl.ds(pl.multiple_of(a * SIDE + j * R, R), R), lanes]
            for i in range(D1):
                totals[i] = add(totals[i], first_s[i * R + a:i * R + a + 1, lanes] * m)
        for i in range(D1):
            left_s[pl.ds(pl.multiple_of(i * SIDE + j * R, R), R), lanes] = totals[i]

    lane_loop(D2, left_s.shape[1], body)


def embedded_into(emb_s, left_s, last_s, batch=8):
    @pl.loop(0, PAIRS // batch)
    def _(b):
        totals = [None] * batch
        for c in range(R):
            last = last_s[c * D3:(c + 1) * D3, :]
            for k in range(batch):
                totals[k] = add(totals[k], left_s[pl.ds((b * batch + k) * R + c, 1), :] * last)
        for k in range(batch):
            emb_s[pl.ds(pl.multiple_of((b * batch + k) * D3, D3), D3), :] = totals[k]


def grad_left_into(gleft_s, g_s, lastd_s):
    batch = 4 if gleft_s.shape[1] <= 2 * LANES else 2

    @pl.loop(0, PAIRS // batch)
    def _(b):
        totals = [None] * batch
        for d in range(D3):
            last = lastd_s[d * R:(d + 1) * R, :]
            for k in range(batch):
                totals[k] = add(totals[k], g_s[pl.ds((b * batch + k) * D3 + d, 1), :] * last)
        for k in range(batch):
            gleft_s[pl.ds(pl.multiple_of((b * batch + k) * R, R), R), :] = totals[k]


def grad_last_into(gl_s, left_s, g_s, batch=8):
    @pl.loop(0, R // batch)
    def _(b):
        totals = [None] * batch
        for p in range(PAIRS):
            g = g_s[p * D3:(p + 1) * D3, :]
            for k in range(batch):
                totals[k] = add(totals[k], left_s[pl.ds(p * R + b * batch + k, 1), :] * g)
        for k in range(batch):
            gl_s[pl.ds(pl.multiple_of((b * batch + k) * D3, D3), D3), :] = totals[k]


def grad_first_into(gf_s, gleft_s, mid_s, batch=8):
    def body(b, lanes):
        totals = [[None] * D1 for _ in range(batch)]
        for t in range(0, SIDE, 8):
            gleft = [gleft_s[i * SIDE + t:i * SIDE + t + 8, lanes] for i in range(D1)]
            for k in range(batch):
                at = pl.multiple_of((b * batch + k) * SIDE + t, 8)
                m = mid_s[pl.ds(at, 8), lanes]
                for i in range(D1):
                    totals[k][i] = add(totals[k][i], gleft[i] * m)
        for i in range(D1):
            rows = [jnp.sum(totals[k][i], axis=0, keepdims=True) for k in range(batch)]
            gf_s[pl.ds(pl.multiple_of(i * R + b * batch, 8), batch), lanes] = (
                jnp.concatenate(rows, axis=0))

    lane_loop(R // batch, gf_s.shape[1], body)


def first_row(plan):
    start = (lax.axis_index("gx") * plan.planes + lax.axis_index("gy")) * plan.share
    return jnp.clip((start - plan.n1) // plan.row, 0, plan.n2_rows - plan.window), start


def rank_lookups(plan, blocks, rank_s, vals_s):
    groups, looks = rank_s.shape
    per = looks // LANES
    r0, _ = first_row(plan)
    digits = [
        jnp.concatenate([blocks[:, k * per + h, :] for h in range(per)], axis=1).astype(jnp.int32)
        for k in range(4)
    ]
    rel = digits[2] - r0
    inside = (rel >= 0) & (rel < plan.window)
    low = jnp.where(inside, 1.0, 0.0).astype(BF16)
    tri = jnp.where(
        lax.broadcasted_iota(jnp.int32, (looks, looks), 0)
        < lax.broadcasted_iota(jnp.int32, (looks, looks), 1), 1.0, 0.0).astype(BF16)
    above = jnp.where(
        lax.broadcasted_iota(jnp.int32, (groups, groups), 0)
        > lax.broadcasted_iota(jnp.int32, (groups, groups), 1), 1.0, 0.0).astype(BF16)
    before = jnp.sum(dot(above, low, PLAIN), axis=1, keepdims=True)
    rank_s[...] = jnp.where(inside, dot(low, tri, PLAIN) + before, -1.0).astype(jnp.int32)
    group = lax.broadcasted_iota(jnp.int32, (groups, looks), 0)
    columns = (digits[0], digits[1], digits[3], group, jnp.where(inside, rel + 1, 0))
    for k, column in enumerate(columns):
        vals_s[:, k:k + 1, :] = column.astype(F32).reshape(groups, 1, looks)
    vals_s[:, len(columns):, :] = jnp.zeros((groups, 8 - len(columns), looks), F32)
    return jnp.sum(jnp.where(inside, 1.0, 0.0), axis=(0, 1), keepdims=True)


def pick_into(found_s, step, rank_s, vals_s):
    chunk = found_s.shape[1]
    groups, looks = rank_s.shape
    slots = lax.broadcasted_iota(jnp.int32, (chunk, looks), 0)

    def pick(e, found):
        ranks = rank_s[pl.ds(e, 1), :] - step * chunk
        chosen = jnp.where(slots == ranks, 1.0, 0.0).astype(BF16)
        return found + dot(vals_s[e].astype(BF16), chosen, ACROSS)

    found = lax.fori_loop(0, groups, pick, jnp.zeros(found_s.shape, F32), unroll=4)
    found_s[...] = found.astype(jnp.int32)


def factors_into(fsel_s, lsel_s, found_s, c1, c3):
    fsel_s[...] = dot(c1[...], hot(found_s[1:2, :], c1.shape[0], BF16), DOWN)
    last = dot(c3[...], hot(found_s[2:3, :], c3.shape[0], BF16), DOWN)
    lsel_s[...] = by_d3(last.astype(BF16))


def middle_sum(plan, gp, samples, found_s, fsel_s, lsel_s, gsel_s, glsel_s):
    sample = hot(found_s[3:4, :] * samples + found_s[0:1, :], gp.shape[0], BF16)
    gsel_s[...] = dot_parts(gp, sample, DOWN, 2, 0)
    grad_left_into(glsel_s, gsel_s, lsel_s)
    rel1 = found_s[4:5, :]
    total = None
    for i in range(D1):
        part = fsel_s[i * R:(i + 1) * R, :]
        spread = jnp.concatenate(
            [jnp.where(rel1 == r + 1, part, 0.0) for r in range(plan.window)], axis=0
        ).astype(BF16)
        total = add(total, dot_parts(spread, glsel_s[i * SIDE:(i + 1) * SIDE, :], ACROSS, 2, 1))
    return total


def select_scratch(groups, looks, chunk):
    return [
        pltpu.VMEM((groups, looks), jnp.int32),
        pltpu.VMEM((groups, 8, looks), F32),
        pltpu.VMEM((8, chunk), jnp.int32),
        pltpu.VMEM((D1 * R, chunk), F32),
        pltpu.VMEM((R * D3, chunk), F32),
        pltpu.VMEM((WIDTH, chunk), F32),
        pltpu.VMEM((D1 * SIDE, chunk), F32),
    ]


STAGES = ("dz", "dx", "dc", "gz", "gx", "gc", "t0", "t1", "t2", "t3", "t4", "s0", "s1", "s2", "s3")


def stage_sizes(plan):
    cores, chips, planes = plan.cores, plan.chips, plan.planes
    gather = dict(z=planes, x=chips * planes, c=cores * planes)
    sizes = {kind + axis: size for kind in "dg" for axis, size in gather.items()}
    sizes.update(t0=cores, t1=chips, t2=planes, t3=chips, t4=cores,
                 s0=cores, s1=chips, s2=planes, s3=cores * chips)
    return [sizes[name] for name in STAGES]


def step_kernel(plan, *refs):
    inputs, refs = refs[:12], refs[12:]
    digits_out, gp_out, top_ref, seg_ref, mid_ref, count_ref = refs[:6]
    held, refs = refs[6:18], refs[18:]
    mid_s, first_s, last_s, lastd_s, left_s, gleft_s, emb_s, g_s, gf_s, gl_s = refs[:10]
    digits_ref, gp_ref = refs[10:12]
    top_s, topin, top1, topx, topz, seg_s, segin, seg1, segx, seg2, segz, seg3 = refs[12:24]
    rank_s, vals_s, found_s, fsel_s, lsel_s, gsel_s, glsel_s = refs[24:31]
    load_sems, save_sems, sems = refs[31], refs[32], refs[33:]
    sems = {name: (sems[2 * i], sems[2 * i + 1]) for i, name in enumerate(STAGES)}
    cores, chips, planes = plan.cores, plan.chips, plan.planes
    gx, plane = lax.axis_index("gx"), lax.axis_index("gy")
    core, chip = gx % cores, gx // cores
    scopes = []

    def mark(name):
        if scopes:
            scopes.pop().__exit__(None, None, None)
        if name:
            scopes.append(jax.named_scope(name))
            scopes[-1].__enter__()

    mark("m_start")
    c1, c2, c3, dense, w, bias, wout, labels, bag, d1, d2, d3 = held
    wide = c2.shape[1] // 4
    loads = {}

    def load(k, columns=None):
        src, dst = inputs[k], held[k]
        if columns is not None:
            src, dst = src.at[:, columns], dst.at[:, columns]
        n = len(loads)
        loads[n] = pltpu.make_async_copy(src, dst, load_sems.at[n])
        loads[n].start()
        return n

    early = [load(k) for k in (10, 9, 11, 8)]
    tables = [load(1, slice(lo, lo + wide)) for lo in range(0, c2.shape[1], wide)]
    early += [load(0)]
    late = [load(k) for k in (2, 3, 4, 5, 6, 7)]

    def at(c, q, p):
        return (q * cores + c, p)

    def on_core(k):
        return at((core + k) % cores, chip, plane)

    def on_chip(k):
        return at(core, (chip + k) % chips, plane)

    def on_plane(k):
        return at(core, chip, (plane + k) % planes)

    barrier = pltpu.get_barrier_semaphore()
    peers = [at((core + c) % cores, (chip + q) % chips, plane)
             for c in range(cores) for q in range(chips) if c or q]
    peers += [on_plane(k) for k in range(1, planes)]
    for peer in peers:
        pl.semaphore_signal(barrier, inc=1, device_id=peer, device_id_type=pl.DeviceIdType.MESH)

    sent = []

    def remote(src, dst, stage, k, peer):
        return pltpu.make_async_remote_copy(
            src_ref=src, dst_ref=dst, send_sem=sems[stage][0].at[k],
            recv_sem=sems[stage][1].at[k], device_id=peer,
            device_id_type=pl.DeviceIdType.MESH)

    def push(src, dst, stage, k, peer):
        copy = remote(src, dst, stage, k, peer)
        copy.start()
        sent.append(copy)

    def arrive(ref, stage, k):
        remote(ref, ref, stage, k, on_plane(1)).wait_recv()

    def back(me, k, size):
        return (me + size - k) % size

    class Gather:
        def __init__(self, ref, kind):
            self.ref, self.kind = ref, kind

        def own_z(self):
            slot = self.ref.at[core, plane, chip]
            for k in range(1, planes):
                push(slot, slot, self.kind + "z", k, on_plane(k))

        def own_x(self):
            slot = self.ref.at[core, plane, chip]
            for q in range(1, chips):
                push(slot, slot, self.kind + "x", q * planes, on_chip(q))

        def relay_z(self, k):
            slot = self.ref.at[core, back(plane, k, planes), chip]
            arrive(slot, self.kind + "z", k)
            for q in range(1, chips):
                push(slot, slot, self.kind + "x", q * planes + k, on_chip(q))

        def relay_x(self, k):
            z = back(plane, k, planes)
            for q in range(1, chips):
                arrive(self.ref.at[core, z, back(chip, q, chips)], self.kind + "x", q * planes + k)
            slot = self.ref.at[core, z]
            for c in range(1, cores):
                push(slot, slot, self.kind + "c", c * planes + k, on_core(c))

        def finish(self, k):
            for c in range(1, cores):
                slot = self.ref.at[back(core, c, cores), back(plane, k, planes)]
                arrive(slot, self.kind + "c", c * planes + k)

    digits, grads = Gather(digits_ref, "d"), Gather(gp_ref, "g")

    mark("m_gather")
    for n in early:
        loads[n].wait()
    samples, looks = dense.shape[0], d1.shape[1]
    per = looks // LANES
    for k, digit in enumerate((bag, d1, d2, d3)):
        for h in range(per):
            digits_ref[core, plane, chip, k * per + h:k * per + h + 1, :] = (
                digit[:, h * LANES:(h + 1) * LANES].astype(F32))
    hot1 = hot(d1[...], c1.shape[0], BF16)
    hot2 = hot(d2[...], c2.shape[0], BF16)
    first_s[...] = dot(c1[...], hot1, DOWN)
    for k, n in enumerate(tables):
        loads[n].wait()
        for lo, size in spans(wide, 512):
            lo += k * wide
            mid_s[lo:lo + size, :] = dot(c2[:, lo:lo + size], hot2, DOWN)
    mark("m_left")
    left_into(left_s, first_s, mid_s)
    for n in late:
        loads[n].wait()
    hot3 = hot(d3[...], c3.shape[0], BF16)
    last_t = dot(c3[...], hot3, DOWN)
    last_s[...] = last_t
    lastd_s[...] = by_d3(last_t.astype(BF16))
    mark("m_barrier")
    pl.semaphore_wait(barrier, len(peers))
    digits.own_z()
    digits.own_x()
    mark("m_emb")
    embedded_into(emb_s, left_s, last_s)

    mark("m_top")
    bags = hot(bag[...], samples, BF16)
    pooled = dot_parts(bags, emb_s[...], ACROSS, 3, 1).astype(BF16)
    pre = (
        dot(dense[...], w[:WIDTH, :], PLAIN) + dot(pooled, w[WIDTH:, :], PLAIN)
        + bias[...]
    )
    sig = jax.nn.sigmoid(pre)
    hidden = pre * sig
    logit = jnp.sum(hidden * wout[...], axis=1, keepdims=True)
    rows = lax.broadcasted_iota(jnp.int32, (samples, samples), 0)
    cols = lax.broadcasted_iota(jnp.int32, (samples, samples), 1)
    label = jnp.sum(
        jnp.where(rows == cols, labels[...].astype(F32), 0.0), axis=1, keepdims=True
    )
    dlogit = (jax.nn.sigmoid(logit) - label) / samples
    dpre = dlogit * wout[...] * (sig * (1.0 + pre * (1.0 - sig)))
    low = dpre.astype(BF16)

    mark("m_topgrad")
    deep = plan.trows - 8
    vectors = jnp.concatenate(
        [jnp.sum(dpre, axis=0, keepdims=True), jnp.sum(hidden * dlogit, axis=0, keepdims=True),
         jnp.zeros((6, dpre.shape[1]), F32)], axis=0)
    weight = [dot(dense[...], low, DOWN), dot(pooled, low, DOWN)]
    for h in range(cores):
        lanes = slice(h * LANES, (h + 1) * LANES)
        for q in range(chips):
            lo = q * deep
            half = weight[lo // WIDTH]
            top_s[h, q, :deep, :] = half[lo % WIDTH:lo % WIDTH + deep, lanes]
            top_s[h, q, deep:, :] = vectors[:, lanes] if q == 0 else jnp.zeros((8, LANES), F32)
    for c in range(1, cores):
        push(top_s.at[(core + c) % cores], topin.at[c], "t0", c, on_core(c))
    gp = dot(low, w[WIDTH:, :], ACROSS)
    gp_ref[core, plane, chip] = gp
    grads.own_z()

    mark("m_gleft")
    g_s[...] = dot_parts(gp, bags, DOWN, 2, 0)
    grad_left_into(gleft_s, g_s, lastd_s)

    mark("m_t0")
    total = top_s[core]
    for c in range(1, cores):
        arrive(topin.at[c], "t0", c)
        total = total + topin[c]
    top1[...] = total
    for k in range(1, chips):
        push(top1.at[(chip + k) % chips], topx.at[k], "t1", k, on_chip(k))
    grads.own_x()

    mark("m_gl")
    grad_last_into(gl_s, left_s, g_s)
    mark("m_dz")
    for k in range(1, planes):
        digits.relay_z(k)
    mark("m_gf")
    grad_first_into(gf_s, gleft_s, mid_s)
    mark("m_segdot")
    sums = {True: dot_parts(hot1, gf_s[...], ACROSS, 2, 1),
            False: dot_parts(hot3, gl_s[...], ACROSS, 2, 1)}
    seg_s[...] = jnp.zeros_like(seg_s)
    for seg in plan.segs:
        for c, q, lo, hi, h in pieces_of(seg, cores, chips, cores):
            seg_s[c, q, seg.offset:seg.offset + hi - lo, :] = (
                sums[seg.first][lo:hi, h * LANES:(h + 1) * LANES])
    for c in range(1, cores):
        push(seg_s.at[(core + c) % cores], segin.at[c], "s0", c, on_core(c))

    mark("m_t1")
    total = top1[chip]
    for k in range(1, chips):
        arrive(topx.at[k], "t1", k)
        total = total + topx[k]
    topz[plane] = total
    for k in range(1, planes):
        push(topz.at[plane], topz.at[plane], "t2", k, on_plane(k))

    mark("m_s0")
    total = seg_s[core]
    for c in range(1, cores):
        arrive(segin.at[c], "s0", c)
        total = total + segin[c]
    seg1[...] = total
    for k in range(1, chips):
        push(seg1.at[(chip + k) % chips], segx.at[k], "s1", k, on_chip(k))

    mark("m_dx")
    for k in range(planes):
        digits.relay_x(k)
    mark("m_gz")
    for k in range(1, planes):
        grads.relay_z(k)
    mark("m_df")
    for k in range(planes):
        digits.finish(k)
    mark("m_rank")
    groups = cores * planes * chips
    count = rank_lookups(
        plan, digits_ref[...].reshape(groups, *digits_ref.shape[3:]), rank_s, vals_s)
    count_ref[...] = jnp.broadcast_to(count, count_ref.shape)
    mark("m_pick")
    pick_into(found_s, 0, rank_s, vals_s)

    mark("m_s1")
    total = seg1[chip]
    for k in range(1, chips):
        arrive(segx.at[k], "s1", k)
        total = total + segx[k]
    seg2[...] = total

    def out_of(p, k):
        seg = plan.segs[(p + k) % planes]
        return remote(seg2.at[seg.offset:seg.offset + seg.rows],
                      segz.at[k, :seg.rows], "s2", k, on_plane(k))

    for p in range(planes):
        @pl.when(plane == p)
        def _(p=p):
            for k in range(1, planes):
                out_of(p, k).start()

    mark("m_t2")
    for k in range(1, planes):
        arrive(topz.at[back(plane, k, planes)], "t2", k)
    total = topz[0]
    for k in range(1, planes):
        total = total + topz[k]
    top_ref[core, chip] = total
    for k in range(1, chips):
        push(top_ref.at[core, chip], top_ref.at[core, chip], "t3", k, on_chip(k))

    mark("m_factors")
    factors_into(fsel_s, lsel_s, found_s, c1, c3)
    mark("m_gx")
    for k in range(planes):
        grads.relay_x(k)

    mark("m_s2")

    def to_owner(p):
        seg = plan.segs[p]
        return remote(seg3.at[:seg.rows], seg_ref.at[core, chip, :seg.rows], "s3",
                      core * chips + chip, (seg.owner, plane))

    for p in range(planes):
        @pl.when(plane == p)
        def _(p=p):
            seg = plan.segs[p]
            total = seg2[seg.offset:seg.offset + seg.rows]
            for k in range(1, planes):
                arrive(segz.at[k, :seg.rows], "s2", k)
                total = total + segz[k, :seg.rows]
            seg3[:seg.rows] = total

            @pl.when(gx != seg.owner)
            def _():
                to_owner(p).start()

    mark("m_gfin")
    for k in range(planes):
        grads.finish(k)
    saves = [pltpu.make_async_copy(digits_ref, digits_out, save_sems.at[0]),
             pltpu.make_async_copy(gp_ref, gp_out, save_sems.at[1])]
    for save in saves:
        save.start()
    mark("m_mid")
    mid_ref[...] = middle_sum(
        plan, gp_ref[...].reshape(groups * samples, WIDTH), samples,
        found_s, fsel_s, lsel_s, gsel_s, glsel_s)

    mark("m_t3")
    for k in range(1, chips):
        arrive(top_ref.at[core, back(chip, k, chips)], "t3", k)
    for c in range(1, cores):
        push(top_ref.at[core], top_ref.at[core], "t4", c, on_core(c))

    mark("m_s3")
    for p in range(planes):
        seg = plan.segs[p]

        @pl.when((plane == p) & (gx == seg.owner))
        def _(p=p, seg=seg):
            own_core, own_chip = seg.owner % cores, seg.owner // cores
            seg_ref[own_core, own_chip, :seg.rows] = seg3[:seg.rows]
            for c in range(cores):
                for q in range(chips):
                    if (c, q) != (own_core, own_chip):
                        arrive(seg_ref.at[c, q, :seg.rows], "s3", c * chips + q)

    mark("m_t4")
    for c in range(1, cores):
        arrive(top_ref.at[back(core, c, cores)], "t4", c)
    mark("m_sent")
    for save in saves:
        save.wait()
    for copy in sent:
        copy.wait_send()
    for p in range(planes):
        @pl.when(plane == p)
        def _(p=p):
            for k in range(1, planes):
                out_of(p, k).wait_send()

            @pl.when(gx != plan.segs[p].owner)
            def _():
                to_owner(p).wait_send()
    mark(None)


def step_part(plan, chunk, *inputs):
    c1, c2, c3, dense, w, bias, wout, labels, bag, d1, d2, d3 = inputs
    samples, looks = dense.shape[0], d1.shape[1]
    cores, chips, planes = plan.cores, plan.chips, plan.planes
    groups = cores * chips * planes
    vmem = pl.BlockSpec(memory_space=pltpu.VMEM)
    hbm = pl.BlockSpec(memory_space=pltpu.HBM)
    scratch = [R * SIDE, D1 * R, R * D3, R * D3, D1 * SIDE, D1 * SIDE, WIDTH, WIDTH, D1 * R, R * D3]
    top, seg = (plan.trows, LANES), (plan.srows, LANES)
    digits = (cores, planes, chips, up(4 * looks // LANES, 8), LANES)
    grads = (cores, planes, chips, samples, WIDTH)
    sums = [
        digits, grads,
        (cores, chips, *top), (cores, chips, *top), (chips, *top), (chips, *top), (planes, *top),
        (cores, chips, *seg), (cores, chips, *seg), (chips, *seg), (chips, *seg), seg,
        (planes, plan.smost, LANES), (plan.smost, LANES)]
    inputs = [pltpu.with_memory_space_constraint(x, pltpu.HBM) for x in inputs]
    return pl.pallas_call(
        functools.partial(step_kernel, plan),
        in_specs=[hbm] * len(inputs),
        out_specs=(hbm, hbm, vmem, vmem, vmem, vmem),
        out_shape=(
            pltpu.HBM(digits, F32),
            pltpu.HBM(grads, F32),
            pltpu.VMEM((cores, chips, *top), F32),
            pltpu.VMEM((cores, chips, plan.smost, LANES), F32),
            pltpu.VMEM((plan.window * R, SIDE), F32),
            pltpu.VMEM((8, LANES), F32),
        ),
        scratch_shapes=[pltpu.VMEM(x.shape, x.dtype) for x in inputs]
        + [pltpu.VMEM((rows, looks), F32) for rows in scratch]
        + [pltpu.VMEM(dims, F32) for dims in sums]
        + select_scratch(groups, looks, chunk)
        + [pltpu.SemaphoreType.DMA((len(inputs) + 3,)), pltpu.SemaphoreType.DMA((2,))]
        + [pltpu.SemaphoreType.DMA((size,)) for size in stage_sizes(plan) for _ in range(2)],
        compiler_params=pltpu.CompilerParams(
            collective_id=0, has_side_effects=True, vmem_limit_bytes=40 << 20),
        name="step",
    )(*inputs)


def finish_kernel(
    plan, c1_in, c3_in, digits_in, gp_in, top, seg_in, mid, count_in, core_out, top_out,
    c1, c3, blocks_s, gp_s, rank_s, vals_s, found_s, fsel_s, lsel_s, gsel_s, glsel_s,
    big_s, core_s, top_s, more_sems, out_sems,
):
    cores, chips, planes, window = plan.cores, plan.chips, plan.planes, plan.window
    gx, plane = lax.axis_index("gx"), lax.axis_index("gy")
    r0, start = first_row(plan)
    chunk = found_s.shape[1]

    deep = plan.trows - 8
    for h in range(cores):
        lanes = slice(h * LANES, (h + 1) * LANES)
        for q in range(chips):
            top_s[q * deep:(q + 1) * deep, lanes] = top[h, q, :deep, :]
        top_s[chips * deep:, lanes] = top[h, 0, deep:deep + 2, :]
    save_top = pltpu.make_async_copy(top_s, top_out, out_sems.at[0])
    save_top.start()

    base, rows = plan.n1 // LANES, window * R
    big_s[base:base + rows, :] = mid[...]
    count = jnp.max(count_in[...]).astype(jnp.int32)

    @pl.when(count > chunk)
    def _():
        pairs = zip((c1_in, c3_in, digits_in, gp_in), (c1, c3, blocks_s, gp_s))
        loads = [pltpu.make_async_copy(a, b, more_sems.at[k]) for k, (a, b) in enumerate(pairs)]
        for load in loads:
            load.start()
        for load in loads:
            load.wait()
        groups, samples = rank_s.shape[0], gp_s.shape[3]
        rank_lookups(plan, blocks_s[...].reshape(groups, *blocks_s.shape[3:]), rank_s, vals_s)

        def body(step, carry):
            pick_into(found_s, step, rank_s, vals_s)
            factors_into(fsel_s, lsel_s, found_s, c1, c3)
            big_s[base:base + rows, :] = big_s[base:base + rows, :] + middle_sum(
                plan, gp_s[...].reshape(groups * samples, WIDTH), samples,
                found_s, fsel_s, lsel_s, gsel_s, glsel_s)
            return carry

        lax.fori_loop(1, (count + chunk - 1) // chunk, body, 0)

    halves = seg_in.shape[0]
    for p in range(planes):
        seg = plan.segs[p]

        @pl.when((plane == p) & (gx == seg.owner))
        def _(seg=seg):
            for c, q, lo, hi, h in pieces_of(seg, cores, chips, halves):
                piece = seg_in[c, q, :hi - lo, :]
                if seg.first:
                    big_s[lo:hi, :] = piece
                else:
                    big_s[pl.ds(base + rows + lo * halves + h, hi - lo, stride=halves), :] = piece

    at = start // LANES - r0 * (plan.row // LANES)
    shift = start % LANES
    size = core_s.shape[0]
    here, after = big_s[pl.ds(at, size), :], big_s[pl.ds(at + 1, size), :]
    turn = (LANES - shift) % LANES
    lane = lax.broadcasted_iota(jnp.int32, (size, LANES), 1)
    core_s[...] = jnp.where(
        lane < LANES - shift, pltpu.roll(here, turn, 1), pltpu.roll(after, turn, 1))
    save_core = pltpu.make_async_copy(core_s, core_out, out_sems.at[1])
    save_core.start()
    save_top.wait()
    save_core.wait()


def finish_part(plan, chunk, looks, c1, c3, digits, gp, top, seg, mid, count):
    groups = plan.cores * plan.chips * plan.planes
    vmem = pl.BlockSpec(memory_space=pltpu.VMEM)
    hbm = pl.BlockSpec(memory_space=pltpu.HBM)
    out_rows = up(-(-plan.share // LANES), 8)
    big = up(plan.n1 // LANES + plan.window * R + plan.n3_rows * seg.shape[0] + out_rows, 8)
    core_shape = (out_rows, LANES)
    top_shape = (plan.chips * (plan.trows - 8) + 2, plan.cores * LANES)
    far = [pltpu.with_memory_space_constraint(x, pltpu.HBM) for x in (c1, c3, digits, gp)]
    return pl.pallas_call(
        functools.partial(finish_kernel, plan),
        out_shape=(pltpu.HBM(core_shape, F32), pltpu.HBM(top_shape, F32)),
        in_specs=[hbm] * 4 + [vmem] * 4,
        out_specs=(hbm, hbm),
        scratch_shapes=[pltpu.VMEM(x.shape, x.dtype) for x in (c1, c3, digits, gp)]
        + select_scratch(groups, looks, chunk)
        + [pltpu.VMEM((big, LANES), F32), pltpu.VMEM(core_shape, F32),
           pltpu.VMEM(top_shape, F32), pltpu.SemaphoreType.DMA((4,)), pltpu.SemaphoreType.DMA((2,))],
        compiler_params=pltpu.CompilerParams(vmem_limit_bytes=40 << 20),
        name="finish",
    )(*far, top, seg, mid, count)


def per_device(plan, c1, c2, c3, dense, w, bias, wout, labels, bag, d1, d2, d3):
    looks = d1.shape[1]
    expected = plan.nx * plan.ny * looks * plan.window // plan.n2_rows
    chunk = up(expected * 9 // 8, LANES)
    digits, gp, top, seg, mid, count = step_part(
        plan, chunk, c1, c2, c3, dense, w, bias[None], wout[None], labels[None], bag, d1, d2, d3)
    core, top = finish_part(plan, chunk, looks, c1, c3, digits, gp, top, seg, mid, count)
    return core.reshape(-1)[:plan.share], top


def one_hot(digits, count, kind):
    return (digits[:, None] == jnp.arange(count, dtype=jnp.int32)[None, :]).astype(kind)


def slices(digits, core):
    return jnp.dot(
        one_hot(digits, core.shape[0], jnp.bfloat16), core, preferred_element_type=jnp.float32
    )


def factors(digits, cores):
    high = lax.Precision.HIGHEST
    first = slices(digits[0], cores[0]).reshape(-1, D1, R)
    middle = slices(digits[1], cores[1]).reshape(-1, R, D2 * R)
    last = slices(digits[2], cores[2]).reshape(-1, R, D3)
    left = jnp.einsum("nia,nab->nib", first, middle, precision=high).reshape(-1, D1 * D2, R)
    return (first, middle, last, left)


def top_total(top_local):
    return lax.psum(top_local, ("gx", "gy"))


def per_device_dense(
    core_one,
    core_two,
    core_three,
    dense_rows,
    w_top,
    bias_top,
    w_out,
    labels,
    bag_ids,
    digit_one,
    digit_two,
    digit_three,
):
    high = lax.Precision.HIGHEST
    cores = (core_one, core_two, core_three)
    digits = jnp.stack([digit_one[0], digit_two[0], digit_three[0]])
    looks = digits.shape[1]
    block = min(256, looks)
    blocks = looks // block
    blocked = digits.reshape(3, blocks, block).transpose(1, 0, 2)
    width = D1 * D2 * D3

    def forward(carry, part):
        first, middle, last, left = factors(part, cores)
        return (carry, jnp.einsum("npa,nad->npd", left, last, precision=high).reshape(block, width))

    _, embedded = lax.scan(forward, jnp.zeros((), jnp.float32), blocked)
    embedded = embedded.reshape(looks, width)
    samples = dense_rows.shape[0]
    bag_table = one_hot(bag_ids[0], samples, jnp.float32)
    pooled = jnp.dot(bag_table.T, embedded, precision=high)
    joined = jnp.concatenate([dense_rows, pooled.astype(jnp.bfloat16)], axis=1)
    pre = jnp.dot(joined, w_top, preferred_element_type=jnp.float32) + bias_top[None, :]
    sig = jax.nn.sigmoid(pre)
    hidden = pre * sig
    logit = jnp.dot(hidden, w_out, precision=high)
    dlogit = (jax.nn.sigmoid(logit) - labels.astype(jnp.float32)) / samples
    dpre = dlogit[:, None] * w_out[None, :] * (sig * (1.0 + pre * (1.0 - sig)))
    dpre_low = dpre.astype(jnp.bfloat16)
    grad_weight = jnp.dot(joined.T, dpre_low, preferred_element_type=jnp.float32)
    grad_bias = jnp.sum(dpre, axis=0)
    grad_output = jnp.sum(hidden * dlogit[:, None], axis=0)
    top_local = jnp.concatenate([grad_weight, grad_bias[None, :], grad_output[None, :]], axis=0)
    grad_pooled = jnp.dot(dpre_low, w_top[width:].T, preferred_element_type=jnp.float32)
    grad_embedded = jnp.dot(bag_table, grad_pooled, precision=high).reshape(blocks, block, width)

    def backward(totals, inputs):
        part, grad_block = inputs
        first, middle, last, left = factors(part, cores)
        grad_view = grad_block.reshape(block, D1 * D2, D3)
        grad_last = jnp.einsum("npa,npd->nad", left, grad_view, precision=high)
        grad_left = jnp.einsum("npd,nad->npa", grad_view, last, precision=high).reshape(
            block, D1, D2 * R
        )
        grad_first = jnp.einsum("nib,nab->nia", grad_left, middle, precision=high)
        grad_middle = jnp.einsum("nia,nib->nab", first, grad_left, precision=high)
        pieces = (
            grad_first.reshape(block, -1),
            grad_middle.reshape(block, -1),
            grad_last.reshape(block, -1),
        )
        updated = tuple(
            (
                total
                + jnp.dot(
                    one_hot(part[number], cores[number].shape[0], jnp.float32).T,
                    pieces[number],
                    precision=high,
                )
                for number, total in enumerate(totals)
            )
        )
        return (updated, None)

    start = tuple((jnp.zeros(core.shape, jnp.float32) for core in cores))
    totals, _ = lax.scan(backward, start, (blocked, grad_embedded))
    flat = jnp.concatenate([total.reshape(-1) for total in totals])
    core_grad = lax.psum_scatter(flat, ("gx", "gy"), scatter_dimension=0, tiled=True)
    top_grad = top_total(top_local)
    return (core_grad, top_grad)


def solution(mesh):
    nx, ny = mesh.shape["gx"], mesh.shape["gy"]
    whole, split, rows = P(), P(AXES), P(AXES, None)

    def step(*args):
        cores, dense = args[:3], args[3]
        plan = None
        if dense.size < sum(core.size for core in cores):
            plan = plan_of(nx, ny, *(core.shape for core in cores), args[4].shape)
        body = functools.partial(per_device, plan) if plan else per_device_dense
        return jax.shard_map(
            body,
            mesh=mesh,
            in_specs=(
                whole, whole, whole, rows, whole, whole, whole, split,
                rows, rows, rows, rows,
            ),
            out_specs=(split, whole),
            check_vma=False,
        )(*args)

    return step
```

```python
import functools
import types

import jax
import jax.numpy as jnp
from jax import lax
from jax.experimental import pallas as pl
from jax.experimental.pallas import tpu as pltpu
from jax.sharding import PartitionSpec as P

D1 = 4
D2 = 4
D3 = 8
R = 32
WIDTH = D1 * D2 * D3
PAIRS = D1 * D2
SIDE = D2 * R
LANES = 128
LOCAL = 32
AXES = ("gx", "gy")
F32 = jnp.float32
BF16 = jnp.bfloat16
HIGH = lax.Precision.HIGHEST
PLAIN, ACROSS, DOWN = ((1,), (0,)), ((1,), (1,)), ((0,), (0,))


def dot(a, b, dims, precision=None):
    return lax.dot_general(
        a, b, (dims, ((), ())), precision=precision, preferred_element_type=F32
    )


def parts_of(x, count):
    parts = []
    for _ in range(count):
        part = x.astype(BF16)
        parts.append(part)
        x = x - part.astype(F32)
    return parts


def dot_parts(a, b, dims, count, wide):
    free = 1 - dims[wide][0]
    joined = jnp.concatenate(parts_of((a, b)[wide], count), axis=free)
    out = dot(joined, b, dims) if wide == 0 else dot(a, joined, dims)
    size = out.shape[wide] // count
    total = None
    for k in range(count):
        part = lax.slice_in_dim(out, k * size, (k + 1) * size, axis=wide)
        total = part if total is None else total + part
    return total


def hot(row, count, kind):
    numbers = lax.broadcasted_iota(jnp.int32, (count, row.shape[1]), 0)
    return jnp.where(numbers == row, 1.0, 0.0).astype(kind)


def by_d3(last_t):
    size = R * D3
    to = lax.broadcasted_iota(jnp.int32, (size, size), 0)
    of = lax.broadcasted_iota(jnp.int32, (size, size), 1)
    turn = jnp.where(of == (to % R) * D3 + to // R, 1.0, 0.0).astype(BF16)
    return dot(turn, last_t, PLAIN)


def up(count, step):
    return -(-count // step) * step


def plan_of(nx, ny, shape_one, shape_two, shape_three, shape_top):
    cores = 2
    if nx % cores:
        return None
    chips, planes, devices = nx // cores, ny, nx * ny
    n1, n2, n3 = (s[0] * s[1] for s in (shape_one, shape_two, shape_three))
    total = n1 + n2 + n3
    if total % devices or shape_one[1] != LANES or n1 % LANES or shape_two[1] % LANES:
        return None
    if shape_three[1] != cores * LANES or shape_top[1] != cores * LANES or shape_top[0] % (8 * chips):
        return None
    share = total // devices
    row = shape_two[1]
    window = min(-(-share // row) + 1, shape_two[0])
    segs, offset = [None] * planes, 0
    for d in range(devices):
        lo, hi = d * share, (d + 1) * share
        has_first, has_last = lo < n1, hi > n1 + n2
        if not (has_first or has_last):
            continue
        if has_first and has_last or segs[d % planes] is not None:
            return None
        seg = types.SimpleNamespace(owner=d // planes, first=has_first)
        if has_first:
            seg.lo, seg.hi = lo // LANES, -(-min(hi, n1) // LANES)
            seg.rows = up(-(-(seg.hi - seg.lo) // (cores * chips)), 8)
        else:
            seg.lo = max(lo - n1 - n2, 0) // shape_three[1] // 8 * 8
            seg.hi = -(-(hi - n1 - n2) // shape_three[1])
            seg.rows = up(-(-(seg.hi - seg.lo) // chips), 8)
        segs[d % planes] = seg
    if any(seg is None for seg in segs):
        return None
    for seg in segs:
        seg.offset = offset
        offset += seg.rows
    return types.SimpleNamespace(
        nx=nx, ny=ny, cores=cores, chips=chips, planes=planes, share=share, window=window,
        row=row, n1=n1, segs=segs, srows=offset, smost=max(seg.rows for seg in segs),
        trows=shape_top[0] // chips + 8, n2_rows=shape_two[0], n3_rows=shape_three[0])


def pieces_of(seg, cores, chips, halves):
    for core in range(cores):
        for chip in range(chips):
            n = core * chips + chip if seg.first else chip
            lo = seg.lo + n * seg.rows
            hi = min(lo + seg.rows, seg.hi)
            if lo < hi:
                yield core, chip, lo, hi, 0 if seg.first else core


def spans(count, step):
    return [(lo, min(step, count - lo)) for lo in range(0, count, step)]


def lane_loop(count, lanes, body):
    blocks = lanes // LANES

    @pl.loop(0, count * blocks)
    def _(step):
        body(step // blocks, pl.ds(pl.multiple_of((step % blocks) * LANES, LANES), LANES))


def add(total, term):
    return term if total is None else total + term


def left_into(left_s, first_s, mid_s):
    def body(j, lanes):
        totals = [None] * D1
        for a in range(R):
            m = mid_s[pl.ds(pl.multiple_of(a * SIDE + j * R, R), R), lanes]
            for i in range(D1):
                totals[i] = add(totals[i], first_s[i * R + a:i * R + a + 1, lanes] * m)
        for i in range(D1):
            left_s[pl.ds(pl.multiple_of(i * SIDE + j * R, R), R), lanes] = totals[i]

    lane_loop(D2, left_s.shape[1], body)


def embedded_into(emb_s, left_s, last_s, batch=8):
    @pl.loop(0, PAIRS // batch)
    def _(b):
        totals = [None] * batch
        left = left_s.at[pl.ds(pl.multiple_of(b * batch * R, batch * R), batch * R), :]
        for c in range(R):
            last = last_s[c * D3:(c + 1) * D3, :]
            for k in range(batch):
                row = k * R + c
                totals[k] = add(totals[k], left[row:row + 1, :] * last)
        for k in range(batch):
            emb_s[pl.ds(pl.multiple_of((b * batch + k) * D3, D3), D3), :] = totals[k]


def grad_left_into(gleft_s, g_s, lastd_s):
    batch = 4 if gleft_s.shape[1] <= 2 * LANES else 2

    @pl.loop(0, PAIRS // batch)
    def _(b):
        totals = [None] * batch
        g = g_s.at[pl.ds(pl.multiple_of(b * batch * D3, batch * D3), batch * D3), :]
        for d in range(D3):
            last = lastd_s[d * R:(d + 1) * R, :]
            for k in range(batch):
                row = k * D3 + d
                totals[k] = add(totals[k], g[row:row + 1, :] * last)
        for k in range(batch):
            gleft_s[pl.ds(pl.multiple_of((b * batch + k) * R, R), R), :] = totals[k]


def grad_last_into(gl_s, left_s, g_s, batch=8):
    @pl.loop(0, R // batch)
    def _(b):
        totals = [None] * batch
        left = left_s.at[pl.ds(pl.multiple_of(b * batch, batch), (PAIRS - 1) * R + batch), :]
        for p in range(PAIRS):
            g = g_s[p * D3:(p + 1) * D3, :]
            for k in range(batch):
                row = p * R + k
                totals[k] = add(totals[k], left[row:row + 1, :] * g)
        for k in range(batch):
            gl_s[pl.ds(pl.multiple_of((b * batch + k) * D3, D3), D3), :] = totals[k]


def grad_first_into(gf_s, gleft_s, mid_s, batch=8):
    def body(b, lanes):
        totals = [[None] * D1 for _ in range(batch)]
        size = batch * SIDE
        mid = mid_s.at[pl.ds(pl.multiple_of(b * size, size), size), lanes]
        gleft = gleft_s.at[:, lanes]
        for t in range(0, SIDE, 8):
            rows = [gleft[i * SIDE + t:i * SIDE + t + 8, :] for i in range(D1)]
            for k in range(batch):
                m = mid[k * SIDE + t:k * SIDE + t + 8, :]
                for i in range(D1):
                    totals[k][i] = add(totals[k][i], rows[i] * m)
        for i in range(D1):
            rows = [jnp.sum(totals[k][i], axis=0, keepdims=True) for k in range(batch)]
            gf_s[pl.ds(pl.multiple_of(i * R + b * batch, 8), batch), lanes] = (
                jnp.concatenate(rows, axis=0))

    lane_loop(R // batch, gf_s.shape[1], body)


def first_row(plan):
    start = (lax.axis_index("gx") * plan.planes + lax.axis_index("gy")) * plan.share
    return jnp.clip((start - plan.n1) // plan.row, 0, plan.n2_rows - plan.window), start


def rank_lookups(plan, blocks, rank_s, vals_s, local_s=None):
    groups, looks = rank_s.shape
    per = looks // LANES
    r0, _ = first_row(plan)
    digits = [
        jnp.concatenate([blocks[:, k * per + h, :] for h in range(per)], axis=1).astype(jnp.int32)
        for k in range(4)
    ]
    rel = digits[2] - r0
    inside = (rel >= 0) & (rel < plan.window)
    low = jnp.where(inside, 1.0, 0.0).astype(BF16)
    tri = jnp.where(
        lax.broadcasted_iota(jnp.int32, (looks, looks), 0)
        < lax.broadcasted_iota(jnp.int32, (looks, looks), 1), 1.0, 0.0).astype(BF16)
    above = jnp.where(
        lax.broadcasted_iota(jnp.int32, (groups, groups), 0)
        > lax.broadcasted_iota(jnp.int32, (groups, groups), 1), 1.0, 0.0).astype(BF16)
    before = jnp.sum(dot(above, low, PLAIN), axis=1, keepdims=True)
    local = dot(low, tri, PLAIN)
    rank = jnp.where(inside, local + before, -1.0).astype(jnp.int32)
    rank_s[...] = rank
    if local_s is not None:
        local_s[...] = jnp.where(inside, local, -1.0).astype(jnp.int32)
    group = lax.broadcasted_iota(jnp.int32, (groups, looks), 0)
    columns = (digits[0], digits[1], digits[3], group, jnp.where(inside, rel + 1, 0),
               (rank + 1) // LANES, (rank + 1) % LANES)
    for k, column in enumerate(columns):
        vals_s[:, k:k + 1, :] = column.astype(F32).reshape(groups, 1, looks)
    vals_s[:, len(columns):, :] = jnp.zeros((groups, 8 - len(columns), looks), F32)
    each = jnp.sum(jnp.where(inside, 1.0, 0.0), axis=1, keepdims=True)
    return jnp.sum(each, axis=0, keepdims=True), jnp.max(each, axis=0, keepdims=True)


def pick_into(found_s, step, rank_s, vals_s):
    chunk = found_s.shape[1]
    groups, looks = rank_s.shape
    slots = lax.broadcasted_iota(jnp.int32, (chunk, looks), 0)

    def pick(e, found):
        ranks = rank_s[pl.ds(e, 1), :] - step * chunk
        chosen = jnp.where(slots == ranks, 1.0, 0.0).astype(BF16)
        return found + dot(vals_s[e].astype(BF16), chosen, ACROSS)

    found = lax.fori_loop(0, groups, pick, jnp.zeros(found_s.shape, F32), unroll=4)
    found_s[...] = found.astype(jnp.int32)


def pick_few_into(found_s, local_s, vals_s, few_s):
    groups, looks = local_s.shape
    cap = few_s.shape[0] // groups
    slots = lax.broadcasted_iota(jnp.int32, (cap, looks), 0)
    for e in range(groups):
        chosen = jnp.where(slots == local_s[e:e + 1, :], 1.0, 0.0).astype(BF16)
        few_s[e * cap:(e + 1) * cap, :] = dot(chosen, vals_s[e].astype(BF16), ACROSS)
    few = few_s[...]
    ranks = (few[:, 5:6] * LANES + few[:, 6:7]).astype(jnp.int32) - 1
    slots = lax.broadcasted_iota(jnp.int32, (few.shape[0], found_s.shape[1]), 1)
    chosen = jnp.where(slots == ranks, 1.0, 0.0).astype(BF16)
    found_s[...] = dot(few.astype(BF16), chosen, DOWN).astype(jnp.int32)


def factors_into(plan, samples, spread_s, lsel_s, sample_s, found_s, c1, c3):
    first = dot(c1[...], hot(found_s[1:2, :], c1.shape[0], BF16), DOWN)
    last = dot(c3[...], hot(found_s[2:3, :], c3.shape[0], BF16), DOWN)
    lsel_s[...] = by_d3(last.astype(BF16))
    rel1 = found_s[4:5, :]
    for i in range(D1):
        part = first[i * R:(i + 1) * R, :]
        for r in range(plan.window):
            row = (i * plan.window + r) * R
            spread_s[row:row + R, :] = jnp.where(rel1 == r + 1, part, 0.0).astype(BF16)
    sample_s[...] = hot(found_s[3:4, :] * samples + found_s[0:1, :], sample_s.shape[0], BF16)


def middle_sum(plan, spread_s, lsel_s, gsel_s, glsel_s):
    grad_left_into(glsel_s, gsel_s, lsel_s)
    rows = plan.window * R
    total = None
    for i in range(D1):
        total = add(total, dot_parts(
            spread_s[i * rows:(i + 1) * rows, :], glsel_s[i * SIDE:(i + 1) * SIDE, :],
            ACROSS, 2, 1))
    return total


def select_scratch(plan, looks, samples, chunk):
    groups = plan.cores * plan.chips * plan.planes
    return [
        pltpu.VMEM((groups, looks), jnp.int32),
        pltpu.VMEM((groups, 8, looks), F32),
        pltpu.VMEM((8, chunk), jnp.int32),
        pltpu.VMEM((D1 * plan.window * R, chunk), BF16),
        pltpu.VMEM((R * D3, chunk), F32),
        pltpu.VMEM((groups * samples, chunk), BF16),
        pltpu.VMEM((WIDTH, chunk), F32),
        pltpu.VMEM((D1 * SIDE, chunk), F32),
    ]


STAGES = ("dz", "dx", "dc", "gz", "gx", "gc", "bx", "bz", "t0", "t1", "t2", "t3", "t4", "s0", "s1", "s2", "s3")


def step_kernel(plan, *refs):
    inputs, refs = refs[:12], refs[12:]
    digits_out, gp_out, top_ref, seg_ref, mid_ref, rest_ref = refs[:6]
    held, refs = refs[6:18], refs[18:]
    mid_s, first_s, last_s, lastd_s, left_s, gleft_s, emb_s, g_s, gf_s, gl_s = refs[:10]
    digits_ref, gp_ref = refs[10:12]
    top_s, topin, top1, topx, topz, seg_s, segin, seg1, segx, seg2, segz, seg3, segall = refs[12:25]
    rank_s, vals_s, found_s, spread_s, lsel_s, sample_s, gsel_s, glsel_s = refs[25:33]
    local_s, few_s, load_sems, save_sems, send_sems, recv_sems, grad_sems = refs[33:40]
    cores, chips, planes = plan.cores, plan.chips, plan.planes
    gx, plane = lax.axis_index("gx"), lax.axis_index("gy")
    core, chip = gx % cores, gx // cores
    scopes = []

    def mark(name):
        if scopes:
            scopes.pop().__exit__(None, None, None)
        if name:
            scopes.append(jax.named_scope(name))
            scopes[-1].__enter__()

    mark("m_start")
    c1, c2, c3, dense, w, bias, wout, labels, bag, d1, d2, d3 = held
    wide = c2.shape[1] // 2
    loads = {}

    def load(k, columns=None):
        src, dst = inputs[k], held[k]
        if columns is not None:
            src, dst = src.at[:, columns], dst.at[:, columns]
        n = len(loads)
        loads[n] = pltpu.make_async_copy(src, dst, load_sems.at[n])
        loads[n].start()
        return n

    early = [load(k) for k in (10, 9, 11, 8)]
    early += [load(k) for k in (0, 2)]
    tables = [load(1, slice(lo, lo + wide)) for lo in range(0, c2.shape[1], wide)]
    late = [load(k) for k in (3, 4, 5, 6, 7)]

    def at(c, q, p):
        return (q * cores + c, p)

    def on_core(k):
        return at((core + k) % cores, chip, plane)

    def on_chip(k):
        return at(core, (chip + k) % chips, plane)

    def on_plane(k):
        return at(core, chip, (plane + k) % planes)

    barrier = pltpu.get_barrier_semaphore()
    peers = [at((core + c) % cores, (chip + q) % chips, plane)
             for c in range(cores) for q in range(chips) if c or q]
    peers += [on_plane(k) for k in range(1, planes)]
    for peer in peers:
        pl.semaphore_signal(barrier, inc=1, device_id=peer, device_id_type=pl.DeviceIdType.MESH)

    def remote(src, dst, stage, peer, grad=None):
        n = STAGES.index(stage)
        return pltpu.make_async_remote_copy(
            src_ref=src, dst_ref=dst, send_sem=send_sems.at[n],
            recv_sem=recv_sems.at[n] if grad is None else grad_sems.at[grad], device_id=peer,
            device_id_type=pl.DeviceIdType.MESH)

    def push(src, dst, stage, peer, grad=None):
        remote(src, dst, stage, peer, grad).start()

    def arrive(like, stage, grad=None):
        remote(like, like, stage, on_core(1), grad).wait_recv()

    def leave(like, stage):
        remote(like, like, stage, on_core(1)).wait_send()

    def back(me, k, size):
        return (me + size - k) % size

    def own_z(ref, kind, rows=slice(None)):
        slot = ref.at[core, plane, chip, rows]
        for k in range(1, planes):
            push(slot, slot, kind + "z", on_plane(k))

    def push_x(ref, kind, k, grad=None, rows=slice(None)):
        slot = ref.at[core, back(plane, k, planes), chip, rows]
        for q in range(1, chips):
            push(slot, slot, kind + "x", on_chip(q), grad)

    def of_z(ref, rows=slice(None)):
        return ref.at[0, :planes - 1, 0, rows]

    def of_x(ref, rows=slice(None)):
        return ref.at[0, :, :chips - 1, rows]

    mark("m_gather")
    for n in early:
        loads[n].wait()
    samples, looks = dense.shape[0], d1.shape[1]
    per = looks // LANES
    for k, digit in enumerate((bag, d1, d2, d3)):
        for h in range(per):
            digits_ref[core, plane, chip, k * per + h:k * per + h + 1, :] = (
                digit[:, h * LANES:(h + 1) * LANES].astype(F32))
    hot1 = hot(d1[...], c1.shape[0], BF16)
    hot2 = hot(d2[...], c2.shape[0], BF16)
    hot3 = hot(d3[...], c3.shape[0], BF16)
    first_s[...] = dot(c1[...], hot1, DOWN)
    last_t = dot(c3[...], hot3, DOWN)
    last_s[...] = last_t
    lastd_s[...] = by_d3(last_t.astype(BF16))
    for k, n in enumerate(tables):
        loads[n].wait()
        for lo, size in spans(wide, 512):
            lo += k * wide
            mid_s[lo:lo + size, :] = dot(c2[:, lo:lo + size], hot2, DOWN)
    mark("m_barrier")
    pl.semaphore_wait(barrier, len(peers))
    own_z(digits_ref, "d")
    push_x(digits_ref, "d", 0)
    mark("m_left")
    left_into(left_s, first_s, mid_s)
    for n in late:
        loads[n].wait()
    mark("m_emb")
    embedded_into(emb_s, left_s, last_s)

    mark("m_top")
    bags = hot(bag[...], samples, BF16)
    pooled = dot_parts(bags, emb_s[...], ACROSS, 3, 1).astype(BF16)
    pre = (
        dot(dense[...], w[:WIDTH, :], PLAIN) + dot(pooled, w[WIDTH:, :], PLAIN)
        + bias[...]
    )
    sig = jax.nn.sigmoid(pre)
    hidden = pre * sig
    logit = jnp.sum(hidden * wout[...], axis=1, keepdims=True)
    rows = lax.broadcasted_iota(jnp.int32, (samples, samples), 0)
    cols = lax.broadcasted_iota(jnp.int32, (samples, samples), 1)
    label = jnp.sum(
        jnp.where(rows == cols, labels[...].astype(F32), 0.0), axis=1, keepdims=True
    )
    dlogit = (jax.nn.sigmoid(logit) - label) / samples
    dpre = dlogit * wout[...] * (sig * (1.0 + pre * (1.0 - sig)))
    low = dpre.astype(BF16)

    mark("m_topgrad")
    deep = plan.trows - 8
    vectors = jnp.concatenate(
        [jnp.sum(dpre, axis=0, keepdims=True), jnp.sum(hidden * dlogit, axis=0, keepdims=True),
         jnp.zeros((6, dpre.shape[1]), F32)], axis=0)
    weight = [dot(dense[...], low, DOWN), dot(pooled, low, DOWN)]
    for h in range(cores):
        lanes = slice(h * LANES, (h + 1) * LANES)
        for q in range(chips):
            lo = q * deep
            half = weight[lo // WIDTH]
            top_s[h, q, :deep, :] = half[lo % WIDTH:lo % WIDTH + deep, lanes]
            top_s[h, q, deep:, :] = vectors[:, lanes] if q == 0 else jnp.zeros((8, LANES), F32)
    push(top_s.at[1 - core], topin, "t0", on_core(1))
    gp = dot(low, w[WIDTH:, :], ACROSS)
    gp_ref[core, plane, chip] = gp
    split = samples - samples // 4
    most, others = slice(0, split), slice(split, samples)
    push_x(gp_ref, "b", 0, None, others)
    own_z(gp_ref, "g", most)

    mark("m_gleft")
    g_s[...] = dot_parts(gp, bags, DOWN, 2, 0)
    mark("m_gl")
    grad_last_into(gl_s, left_s, g_s)
    mark("m_gleft2")
    grad_left_into(gleft_s, g_s, lastd_s)
    mark("m_t0")
    arrive(topin, "t0")
    top1[...] = top_s[core] + topin[...]
    for k in range(1, chips):
        push(top1.at[(chip + k) % chips], topx.at[k], "t1", on_chip(k))
    mark("m_dz")
    arrive(of_z(digits_ref), "dz")
    for k in range(1, planes):
        push_x(digits_ref, "d", k)
    push_x(gp_ref, "g", 0, 0, most)

    mark("m_gf")
    grad_first_into(gf_s, gleft_s, mid_s)
    mark("m_segdot")
    sums = {True: dot_parts(hot1, gf_s[...], ACROSS, 2, 1),
            False: dot_parts(hot3, gl_s[...], ACROSS, 2, 1)}
    seg_s[...] = jnp.zeros_like(seg_s)
    for seg in plan.segs:
        for c, q, lo, hi, h in pieces_of(seg, cores, chips, cores):
            seg_s[c, q, seg.offset:seg.offset + hi - lo, :] = (
                sums[seg.first][lo:hi, h * LANES:(h + 1) * LANES])
    push(seg_s.at[1 - core], segin, "s0", on_core(1))

    mark("m_bx")
    arrive(gp_ref.at[0, 0, :chips - 1, others], "bx")
    slot = gp_ref.at[core, plane, :, others]
    for k in range(1, planes):
        push(slot, slot, "bz", on_plane(k))
    mark("m_s0")
    arrive(segin, "s0")
    seg1[...] = seg_s[core] + segin[...]
    for k in range(1, chips):
        push(seg1.at[(chip + k) % chips], segx.at[k], "s1", on_chip(k))

    mark("m_gz")
    arrive(of_z(gp_ref, most), "gz")
    for k in range(1, planes):
        push_x(gp_ref, "g", k, k, most)
    mark("m_t1")
    arrive(topx.at[1:], "t1")
    total = top1[chip]
    for k in range(1, chips):
        total = total + topx[k]
    topz[plane] = total
    for k in range(1, planes):
        push(topz.at[plane], topz.at[plane], "t2", on_plane(k))

    mark("m_dx")
    arrive(of_x(digits_ref), "dx")
    push(digits_ref.at[core], digits_ref.at[core], "dc", on_core(1))
    mark("m_df")
    arrive(digits_ref.at[1 - core], "dc")
    mark("m_rank")
    groups = cores * planes * chips
    count, fullest = rank_lookups(
        plan, digits_ref[...].reshape(groups, *digits_ref.shape[3:]), rank_s, vals_s, local_s)
    fits = (count <= found_s.shape[1]) & (fullest <= few_s.shape[0] // groups)
    rest_ref[...] = jnp.broadcast_to(jnp.where(fits, 0.0, 1.0), rest_ref.shape)
    mark("m_pick")
    pick_few_into(found_s, local_s, vals_s, few_s)

    mark("m_s1")
    arrive(segx.at[1:], "s1")
    total = seg1[chip]
    for k in range(1, chips):
        total = total + segx[k]
    seg2[...] = total

    def out_of(p, k):
        seg = plan.segs[(p + k) % planes]
        return remote(seg2.at[seg.offset:seg.offset + seg.rows],
                      segz.at[k, :seg.rows], "s2", on_plane(k))

    for p in range(planes):
        @pl.when(plane == p)
        def _(p=p):
            for k in range(1, planes):
                out_of(p, k).start()

    mark("m_factors")
    factors_into(plan, samples, spread_s, lsel_s, sample_s, found_s, c1, c3)
    mark("m_t2")
    arrive(topz.at[1:], "t2")
    total = topz[0]
    for k in range(1, planes):
        total = total + topz[k]
    top_ref[core, chip] = total
    for k in range(1, chips):
        push(top_ref.at[core, chip], top_ref.at[core, chip], "t3", on_chip(k))

    mark("m_bz")
    arrive(gp_ref.at[0, :planes - 1, :, others], "bz")
    mark("m_gx")

    def chosen_sum(c, z):
        size = chips * samples
        at = pl.multiple_of((c * planes + z) * size, size)
        return dot_parts(
            gp_ref[pl.ds(c, 1), pl.ds(z, 1)].reshape(size, WIDTH), sample_s[pl.ds(at, size), :], DOWN, 2, 0)

    total = None
    for k in range(planes):
        z = back(plane, k, planes)
        arrive(gp_ref.at[0, 0, :chips - 1, most], "gx", k)
        push(gp_ref.at[core, z], gp_ref.at[core, z], "gc", on_core(1), planes + k)
        total = add(total, chosen_sum(core, z))
    gsel_s[...] = total

    mark("m_s2")

    def to_owner(p):
        seg = plan.segs[p]
        return remote(seg3.at[:seg.rows], seg_ref.at[core, chip, :seg.rows], "s3",
                      (seg.owner, plane))

    for p in range(planes):
        @pl.when(plane == p)
        def _(p=p):
            seg = plan.segs[p]
            arrive(segz.at[1:, :seg.rows], "s2")
            total = seg2[seg.offset:seg.offset + seg.rows]
            for k in range(1, planes):
                total = total + segz[k, :seg.rows]
            seg3[:seg.rows] = total

            @pl.when(gx != seg.owner)
            def _():
                to_owner(p).start()

    mark("m_gfin")
    total = gsel_s[...]
    for k in range(planes):
        arrive(gp_ref.at[0, 0], "gc", planes + k)
        total = total + chosen_sum(1 - core, back(plane, k, planes))
    gsel_s[...] = total
    saves = [pltpu.make_async_copy(digits_ref, digits_out, save_sems.at[0]),
             pltpu.make_async_copy(gp_ref, gp_out, save_sems.at[1])]
    for save in saves:
        save.start()
    mark("m_t3")
    arrive(top_ref.at[0, 1:], "t3")
    push(top_ref.at[core], top_ref.at[core], "t4", on_core(1))

    mark("m_mid")
    mid_ref[...] = middle_sum(plan, spread_s, lsel_s, gsel_s, glsel_s)

    mark("m_s3")
    for p in range(planes):
        seg = plan.segs[p]

        @pl.when((plane == p) & (gx == seg.owner))
        def _(p=p, seg=seg):
            own_core, own_chip = seg.owner % cores, seg.owner // cores
            seg_ref[own_core, own_chip, :seg.rows] = seg3[:seg.rows]
            arrive(segall.at[:(cores * chips - 1) * seg.rows], "s3")

    mark("m_t4")
    arrive(top_ref.at[1 - core], "t4")
    mark("m_sent")
    for save in saves:
        save.wait()
    for kind, ref in (("d", digits_ref), ("g", gp_ref)):
        rows = most if kind == "g" else slice(None)
        leave(of_z(ref, rows), kind + "z")
        leave(of_x(ref, rows), kind + "x")
        leave(ref.at[0], kind + "c")
    leave(gp_ref.at[0, 0, :chips - 1, others], "bx")
    leave(gp_ref.at[0, :planes - 1, :, others], "bz")
    for stage, like in (
        ("t0", topin), ("t1", topx.at[1:]), ("t2", topz.at[1:]), ("t3", top_ref.at[0, 1:]),
        ("t4", top_ref.at[0]), ("s0", segin), ("s1", segx.at[1:])):
        leave(like, stage)
    for p in range(planes):
        @pl.when(plane == p)
        def _(p=p):
            seg = plan.segs[p]
            leave(seg2.at[:plan.srows - seg.rows], "s2")

            @pl.when(gx != seg.owner)
            def _():
                to_owner(p).wait_send()
    mark(None)


def step_part(plan, chunk, *inputs):
    c1, c2, c3, dense, w, bias, wout, labels, bag, d1, d2, d3 = inputs
    samples, looks = dense.shape[0], d1.shape[1]
    cores, chips, planes = plan.cores, plan.chips, plan.planes
    groups = cores * chips * planes
    vmem = pl.BlockSpec(memory_space=pltpu.VMEM)
    hbm = pl.BlockSpec(memory_space=pltpu.HBM)
    scratch = [R * SIDE, D1 * R, R * D3, R * D3, D1 * SIDE, D1 * SIDE, WIDTH, WIDTH, D1 * R, R * D3]
    top, seg = (plan.trows, LANES), (plan.srows, LANES)
    digits = (cores, planes, chips, up(4 * looks // LANES, 8), LANES)
    grads = (cores, planes, chips, samples, WIDTH)
    sums = [
        digits, grads,
        (cores, chips, *top), (chips, *top), (chips, *top), (chips, *top), (planes, *top),
        (cores, chips, *seg), (chips, *seg), (chips, *seg), (chips, *seg), seg,
        (planes, plan.smost, LANES), (plan.smost, LANES), (cores * chips * plan.smost, LANES)]
    inputs = [pltpu.with_memory_space_constraint(x, pltpu.HBM) for x in inputs]
    return pl.pallas_call(
        functools.partial(step_kernel, plan),
        in_specs=[hbm] * len(inputs),
        out_specs=(hbm, hbm, vmem, vmem, vmem, vmem),
        out_shape=(
            pltpu.HBM(digits, F32),
            pltpu.HBM(grads, F32),
            pltpu.VMEM((cores, chips, *top), F32),
            pltpu.VMEM((cores, chips, plan.smost, LANES), F32),
            pltpu.VMEM((plan.window * R, SIDE), F32),
            pltpu.VMEM((8, LANES), F32),
        ),
        scratch_shapes=[pltpu.VMEM(x.shape, x.dtype) for x in inputs]
        + [pltpu.VMEM((rows, looks), F32) for rows in scratch]
        + [pltpu.VMEM(dims, F32) for dims in sums]
        + select_scratch(plan, looks, samples, chunk)
        + [pltpu.VMEM((groups, looks), jnp.int32), pltpu.VMEM((groups * LOCAL, 8), F32)]
        + [pltpu.SemaphoreType.DMA((len(inputs) + 1,)), pltpu.SemaphoreType.DMA((2,))]
        + [pltpu.SemaphoreType.DMA((len(STAGES),)) for _ in range(2)]
        + [pltpu.SemaphoreType.DMA((2 * planes,))],
        compiler_params=pltpu.CompilerParams(
            collective_id=0, has_side_effects=True, vmem_limit_bytes=40 << 20),
        name="step",
    )(*inputs)


def finish_kernel(
    plan, c1_in, c3_in, digits_in, gp_in, top, seg_in, mid, rest_in, core_out, top_out,
    c1, c3, blocks_s, gp_s, rank_s, vals_s, found_s, spread_s, lsel_s, sample_s, gsel_s, glsel_s,
    big_s, core_s, top_s, more_sems, out_sems,
):
    cores, chips, planes, window = plan.cores, plan.chips, plan.planes, plan.window
    gx, plane = lax.axis_index("gx"), lax.axis_index("gy")
    r0, start = first_row(plan)
    chunk = found_s.shape[1]

    deep = plan.trows - 8
    for h in range(cores):
        lanes = slice(h * LANES, (h + 1) * LANES)
        for q in range(chips):
            top_s[q * deep:(q + 1) * deep, lanes] = top[h, q, :deep, :]
        top_s[chips * deep:, lanes] = top[h, 0, deep:deep + 2, :]
    save_top = pltpu.make_async_copy(top_s, top_out, out_sems.at[0])
    save_top.start()

    base, rows = plan.n1 // LANES, window * R
    big_s[base:base + rows, :] = mid[...]

    @pl.when(jnp.max(rest_in[...]) > 0.0)
    def _():
        pairs = zip((c1_in, c3_in, digits_in, gp_in), (c1, c3, blocks_s, gp_s))
        loads = [pltpu.make_async_copy(a, b, more_sems.at[k]) for k, (a, b) in enumerate(pairs)]
        for load in loads:
            load.start()
        for load in loads:
            load.wait()
        groups, samples = rank_s.shape[0], gp_s.shape[3]
        count, _ = rank_lookups(
            plan, blocks_s[...].reshape(groups, *blocks_s.shape[3:]), rank_s, vals_s)
        count = jnp.max(count).astype(jnp.int32)
        big_s[base:base + rows, :] = jnp.zeros((rows, LANES), F32)

        def body(step, carry):
            pick_into(found_s, step, rank_s, vals_s)
            factors_into(plan, samples, spread_s, lsel_s, sample_s, found_s, c1, c3)
            gsel_s[...] = dot_parts(
                gp_s[...].reshape(groups * samples, WIDTH), sample_s[...], DOWN, 2, 0)
            big_s[base:base + rows, :] = big_s[base:base + rows, :] + middle_sum(
                plan, spread_s, lsel_s, gsel_s, glsel_s)
            return carry

        lax.fori_loop(0, (count + chunk - 1) // chunk, body, 0)

    halves = seg_in.shape[0]
    for p in range(planes):
        seg = plan.segs[p]

        @pl.when((plane == p) & (gx == seg.owner))
        def _(seg=seg):
            for c, q, lo, hi, h in pieces_of(seg, cores, chips, halves):
                piece = seg_in[c, q, :hi - lo, :]
                if seg.first:
                    big_s[lo:hi, :] = piece
                else:
                    big_s[pl.ds(base + rows + lo * halves + h, hi - lo, stride=halves), :] = piece

    at = start // LANES - r0 * (plan.row // LANES)
    shift = start % LANES
    size = core_s.shape[0]
    here, after = big_s[pl.ds(at, size), :], big_s[pl.ds(at + 1, size), :]
    turn = (LANES - shift) % LANES
    lane = lax.broadcasted_iota(jnp.int32, (size, LANES), 1)
    core_s[...] = jnp.where(
        lane < LANES - shift, pltpu.roll(here, turn, 1), pltpu.roll(after, turn, 1))
    save_core = pltpu.make_async_copy(core_s, core_out, out_sems.at[1])
    save_core.start()
    save_top.wait()
    save_core.wait()


def finish_part(plan, chunk, looks, c1, c3, digits, gp, top, seg, mid, rest):
    vmem = pl.BlockSpec(memory_space=pltpu.VMEM)
    hbm = pl.BlockSpec(memory_space=pltpu.HBM)
    out_rows = up(-(-plan.share // LANES), 8)
    big = up(plan.n1 // LANES + plan.window * R + plan.n3_rows * seg.shape[0] + out_rows, 8)
    core_shape = (out_rows, LANES)
    top_shape = (plan.chips * (plan.trows - 8) + 2, plan.cores * LANES)
    far = [pltpu.with_memory_space_constraint(x, pltpu.HBM) for x in (c1, c3, digits, gp)]
    return pl.pallas_call(
        functools.partial(finish_kernel, plan),
        out_shape=(pltpu.HBM(core_shape, F32), pltpu.HBM(top_shape, F32)),
        in_specs=[hbm] * 4 + [vmem] * 4,
        out_specs=(hbm, hbm),
        scratch_shapes=[pltpu.VMEM(x.shape, x.dtype) for x in (c1, c3, digits, gp)]
        + select_scratch(plan, looks, gp.shape[3], chunk)
        + [pltpu.VMEM((big, LANES), F32), pltpu.VMEM(core_shape, F32),
           pltpu.VMEM(top_shape, F32), pltpu.SemaphoreType.DMA((4,)), pltpu.SemaphoreType.DMA((2,))],
        compiler_params=pltpu.CompilerParams(vmem_limit_bytes=40 << 20),
        name="finish",
    )(*far, top, seg, mid, rest)


def per_device(plan, c1, c2, c3, dense, w, bias, wout, labels, bag, d1, d2, d3):
    looks = d1.shape[1]
    expected = plan.nx * plan.ny * looks * plan.window // plan.n2_rows
    chunk = up(expected * 9 // 8, LANES)
    digits, gp, top, seg, mid, rest = step_part(
        plan, chunk, c1, c2, c3, dense, w, bias[None], wout[None], labels[None], bag, d1, d2, d3)
    core, top = finish_part(plan, chunk, looks, c1, c3, digits, gp, top, seg, mid, rest)
    return core.reshape(-1)[:plan.share], top


def one_hot(digits, count, kind):
    return (digits[:, None] == jnp.arange(count, dtype=jnp.int32)[None, :]).astype(kind)


def slices(digits, core):
    return jnp.dot(
        one_hot(digits, core.shape[0], jnp.bfloat16), core, preferred_element_type=jnp.float32
    )


def factors(digits, cores):
    high = lax.Precision.HIGHEST
    first = slices(digits[0], cores[0]).reshape(-1, D1, R)
    middle = slices(digits[1], cores[1]).reshape(-1, R, D2 * R)
    last = slices(digits[2], cores[2]).reshape(-1, R, D3)
    left = jnp.einsum("nia,nab->nib", first, middle, precision=high).reshape(-1, D1 * D2, R)
    return (first, middle, last, left)


def top_total(top_local):
    return lax.psum(top_local, ("gx", "gy"))


def per_device_dense(
    core_one,
    core_two,
    core_three,
    dense_rows,
    w_top,
    bias_top,
    w_out,
    labels,
    bag_ids,
    digit_one,
    digit_two,
    digit_three,
):
    high = lax.Precision.HIGHEST
    cores = (core_one, core_two, core_three)
    digits = jnp.stack([digit_one[0], digit_two[0], digit_three[0]])
    looks = digits.shape[1]
    block = min(256, looks)
    blocks = looks // block
    blocked = digits.reshape(3, blocks, block).transpose(1, 0, 2)
    width = D1 * D2 * D3

    def forward(carry, part):
        first, middle, last, left = factors(part, cores)
        return (carry, jnp.einsum("npa,nad->npd", left, last, precision=high).reshape(block, width))

    _, embedded = lax.scan(forward, jnp.zeros((), jnp.float32), blocked)
    embedded = embedded.reshape(looks, width)
    samples = dense_rows.shape[0]
    bag_table = one_hot(bag_ids[0], samples, jnp.float32)
    pooled = jnp.dot(bag_table.T, embedded, precision=high)
    joined = jnp.concatenate([dense_rows, pooled.astype(jnp.bfloat16)], axis=1)
    pre = jnp.dot(joined, w_top, preferred_element_type=jnp.float32) + bias_top[None, :]
    sig = jax.nn.sigmoid(pre)
    hidden = pre * sig
    logit = jnp.dot(hidden, w_out, precision=high)
    dlogit = (jax.nn.sigmoid(logit) - labels.astype(jnp.float32)) / samples
    dpre = dlogit[:, None] * w_out[None, :] * (sig * (1.0 + pre * (1.0 - sig)))
    dpre_low = dpre.astype(jnp.bfloat16)
    grad_weight = jnp.dot(joined.T, dpre_low, preferred_element_type=jnp.float32)
    grad_bias = jnp.sum(dpre, axis=0)
    grad_output = jnp.sum(hidden * dlogit[:, None], axis=0)
    top_local = jnp.concatenate([grad_weight, grad_bias[None, :], grad_output[None, :]], axis=0)
    grad_pooled = jnp.dot(dpre_low, w_top[width:].T, preferred_element_type=jnp.float32)
    grad_embedded = jnp.dot(bag_table, grad_pooled, precision=high).reshape(blocks, block, width)

    def backward(totals, inputs):
        part, grad_block = inputs
        first, middle, last, left = factors(part, cores)
        grad_view = grad_block.reshape(block, D1 * D2, D3)
        grad_last = jnp.einsum("npa,npd->nad", left, grad_view, precision=high)
        grad_left = jnp.einsum("npd,nad->npa", grad_view, last, precision=high).reshape(
            block, D1, D2 * R
        )
        grad_first = jnp.einsum("nib,nab->nia", grad_left, middle, precision=high)
        grad_middle = jnp.einsum("nia,nib->nab", first, grad_left, precision=high)
        pieces = (
            grad_first.reshape(block, -1),
            grad_middle.reshape(block, -1),
            grad_last.reshape(block, -1),
        )
        updated = tuple(
            (
                total
                + jnp.dot(
                    one_hot(part[number], cores[number].shape[0], jnp.float32).T,
                    pieces[number],
                    precision=high,
                )
                for number, total in enumerate(totals)
            )
        )
        return (updated, None)

    start = tuple((jnp.zeros(core.shape, jnp.float32) for core in cores))
    totals, _ = lax.scan(backward, start, (blocked, grad_embedded))
    flat = jnp.concatenate([total.reshape(-1) for total in totals])
    core_grad = lax.psum_scatter(flat, ("gx", "gy"), scatter_dimension=0, tiled=True)
    top_grad = top_total(top_local)
    return (core_grad, top_grad)


def solution(mesh):
    nx, ny = mesh.shape["gx"], mesh.shape["gy"]
    whole, split, rows = P(), P(AXES), P(AXES, None)

    def step(*args):
        cores, dense = args[:3], args[3]
        plan = None
        if dense.size < sum(core.size for core in cores):
            plan = plan_of(nx, ny, *(core.shape for core in cores), args[4].shape)
        body = functools.partial(per_device, plan) if plan else per_device_dense
        return jax.shard_map(
            body,
            mesh=mesh,
            in_specs=(
                whole, whole, whole, rows, whole, whole, whole, split,
                rows, rows, rows, rows,
            ),
            out_specs=(split, whole),
            check_vma=False,
        )(*args)

    return step
```

```python
import functools
import types

import jax
import jax.numpy as jnp
from jax import lax
from jax.experimental import pallas as pl
from jax.experimental.pallas import tpu as pltpu
from jax.sharding import PartitionSpec as P

D1 = 4
D2 = 4
D3 = 8
R = 32
WIDTH = D1 * D2 * D3
PAIRS = D1 * D2
SIDE = D2 * R
LANES = 128
LOCAL = 32
AXES = ("gx", "gy")
F32 = jnp.float32
BF16 = jnp.bfloat16
HIGH = lax.Precision.HIGHEST
PLAIN, ACROSS, DOWN = ((1,), (0,)), ((1,), (1,)), ((0,), (0,))


def dot(a, b, dims, precision=None):
    return lax.dot_general(
        a, b, (dims, ((), ())), precision=precision, preferred_element_type=F32
    )


def parts_of(x, count):
    parts = []
    for _ in range(count):
        part = x.astype(BF16)
        parts.append(part)
        x = x - part.astype(F32)
    return parts


def dot_parts(a, b, dims, count, wide):
    free = 1 - dims[wide][0]
    joined = jnp.concatenate(parts_of((a, b)[wide], count), axis=free)
    out = dot(joined, b, dims) if wide == 0 else dot(a, joined, dims)
    size = out.shape[wide] // count
    total = None
    for k in range(count):
        part = lax.slice_in_dim(out, k * size, (k + 1) * size, axis=wide)
        total = part if total is None else total + part
    return total


def hot(row, count, kind):
    numbers = lax.broadcasted_iota(jnp.int32, (count, row.shape[1]), 0)
    return jnp.where(numbers == row, 1.0, 0.0).astype(kind)


def by_d3(last_t):
    size = R * D3
    to = lax.broadcasted_iota(jnp.int32, (size, size), 0)
    of = lax.broadcasted_iota(jnp.int32, (size, size), 1)
    turn = jnp.where(of == (to % R) * D3 + to // R, 1.0, 0.0).astype(BF16)
    return dot(turn, last_t, PLAIN)


def up(count, step):
    return -(-count // step) * step


def plan_of(nx, ny, shape_one, shape_two, shape_three, shape_top):
    cores = 2
    if nx % cores:
        return None
    chips, planes, devices = nx // cores, ny, nx * ny
    n1, n2, n3 = (s[0] * s[1] for s in (shape_one, shape_two, shape_three))
    total = n1 + n2 + n3
    if total % devices or shape_one[1] != LANES or n1 % LANES or shape_two[1] % LANES:
        return None
    if shape_three[1] != cores * LANES or shape_top[1] != cores * LANES or shape_top[0] % (8 * chips):
        return None
    share = total // devices
    row = shape_two[1]
    window = min(-(-share // row) + 1, shape_two[0])
    segs, offset = [None] * planes, 0
    for d in range(devices):
        lo, hi = d * share, (d + 1) * share
        has_first, has_last = lo < n1, hi > n1 + n2
        if not (has_first or has_last):
            continue
        if has_first and has_last or segs[d % planes] is not None:
            return None
        seg = types.SimpleNamespace(owner=d // planes, first=has_first)
        if has_first:
            seg.lo, seg.hi = lo // LANES, -(-min(hi, n1) // LANES)
            seg.rows = up(-(-(seg.hi - seg.lo) // (cores * chips)), 8)
        else:
            seg.lo = max(lo - n1 - n2, 0) // shape_three[1] // 8 * 8
            seg.hi = -(-(hi - n1 - n2) // shape_three[1])
            seg.rows = up(-(-(seg.hi - seg.lo) // chips), 8)
        segs[d % planes] = seg
    if any(seg is None for seg in segs):
        return None
    for seg in sorted(segs, key=lambda seg: not seg.first):
        seg.offset = offset
        offset += seg.rows
    return types.SimpleNamespace(
        nx=nx, ny=ny, cores=cores, chips=chips, planes=planes, share=share, window=window,
        row=row, n1=n1, segs=segs, srows=offset, frows=sum(seg.rows for seg in segs if seg.first), smost=max(seg.rows for seg in segs),
        trows=shape_top[0] // chips + 8, n2_rows=shape_two[0], n3_rows=shape_three[0])


def pieces_of(seg, cores, chips, halves):
    for core in range(cores):
        for chip in range(chips):
            n = core * chips + chip if seg.first else chip
            lo = seg.lo + n * seg.rows
            hi = min(lo + seg.rows, seg.hi)
            if lo < hi:
                yield core, chip, lo, hi, 0 if seg.first else core


def spans(count, step):
    return [(lo, min(step, count - lo)) for lo in range(0, count, step)]


def lane_loop(count, lanes, body, start=0):
    blocks = lanes // LANES

    @pl.loop(start * blocks, count * blocks)
    def _(step):
        body(step // blocks, pl.ds(pl.multiple_of((step % blocks) * LANES, LANES), LANES))


def add(total, term):
    return term if total is None else total + term


def left_into(left_s, first_s, mid_s):
    def body(j, lanes):
        totals = [None] * D1
        for a in range(R):
            m = mid_s[pl.ds(pl.multiple_of(a * SIDE + j * R, R), R), lanes]
            for i in range(D1):
                totals[i] = add(totals[i], first_s[i * R + a:i * R + a + 1, lanes] * m)
        for i in range(D1):
            left_s[pl.ds(pl.multiple_of(i * SIDE + j * R, R), R), lanes] = totals[i]

    lane_loop(D2, left_s.shape[1], body)


def embedded_into(emb_s, left_s, last_s, batch=8):
    @pl.loop(0, PAIRS // batch)
    def _(b):
        totals = [None] * batch
        left = left_s.at[pl.ds(pl.multiple_of(b * batch * R, batch * R), batch * R), :]
        for c in range(R):
            last = last_s[c * D3:(c + 1) * D3, :]
            for k in range(batch):
                row = k * R + c
                totals[k] = add(totals[k], left[row:row + 1, :] * last)
        for k in range(batch):
            emb_s[pl.ds(pl.multiple_of((b * batch + k) * D3, D3), D3), :] = totals[k]


def grad_left_into(gleft_s, g_s, lastd_s):
    batch = 4 if gleft_s.shape[1] <= 2 * LANES else 2

    @pl.loop(0, PAIRS // batch)
    def _(b):
        totals = [None] * batch
        g = g_s.at[pl.ds(pl.multiple_of(b * batch * D3, batch * D3), batch * D3), :]
        for d in range(D3):
            last = lastd_s[d * R:(d + 1) * R, :]
            for k in range(batch):
                row = k * D3 + d
                totals[k] = add(totals[k], g[row:row + 1, :] * last)
        for k in range(batch):
            gleft_s[pl.ds(pl.multiple_of((b * batch + k) * R, R), R), :] = totals[k]


def grad_last_into(gl_s, left_s, g_s, batch=8):
    @pl.loop(0, R // batch)
    def _(b):
        totals = [None] * batch
        left = left_s.at[pl.ds(pl.multiple_of(b * batch, batch), (PAIRS - 1) * R + batch), :]
        for p in range(PAIRS):
            g = g_s[p * D3:(p + 1) * D3, :]
            for k in range(batch):
                row = p * R + k
                totals[k] = add(totals[k], left[row:row + 1, :] * g)
        for k in range(batch):
            gl_s[pl.ds(pl.multiple_of((b * batch + k) * D3, D3), D3), :] = totals[k]


def grad_first_into(gf_s, gleft_s, mid_s, part, parts, batch=8):
    def body(b, lanes):
        totals = [[None] * D1 for _ in range(batch)]
        size = batch * SIDE
        mid = mid_s.at[pl.ds(pl.multiple_of(b * size, size), size), lanes]
        gleft = gleft_s.at[:, lanes]
        for t in range(0, SIDE, 8):
            rows = [gleft[i * SIDE + t:i * SIDE + t + 8, :] for i in range(D1)]
            for k in range(batch):
                m = mid[k * SIDE + t:k * SIDE + t + 8, :]
                for i in range(D1):
                    totals[k][i] = add(totals[k][i], rows[i] * m)
        for i in range(D1):
            rows = [jnp.sum(totals[k][i], axis=0, keepdims=True) for k in range(batch)]
            gf_s[pl.ds(pl.multiple_of(i * R + b * batch, 8), batch), lanes] = (
                jnp.concatenate(rows, axis=0))

    count = R // batch
    lane_loop((part + 1) * count // parts, gf_s.shape[1], body, part * count // parts)


def first_row(plan):
    start = (lax.axis_index("gx") * plan.planes + lax.axis_index("gy")) * plan.share
    return jnp.clip((start - plan.n1) // plan.row, 0, plan.n2_rows - plan.window), start


def rank_lookups(plan, blocks, rank_s, vals_s, local_s=None):
    groups, looks = rank_s.shape
    per = looks // LANES
    r0, _ = first_row(plan)
    digits = [
        jnp.concatenate([blocks[:, k * per + h, :] for h in range(per)], axis=1).astype(jnp.int32)
        for k in range(4)
    ]
    rel = digits[2] - r0
    inside = (rel >= 0) & (rel < plan.window)
    low = jnp.where(inside, 1.0, 0.0).astype(BF16)
    tri = jnp.where(
        lax.broadcasted_iota(jnp.int32, (looks, looks), 0)
        < lax.broadcasted_iota(jnp.int32, (looks, looks), 1), 1.0, 0.0).astype(BF16)
    above = jnp.where(
        lax.broadcasted_iota(jnp.int32, (groups, groups), 0)
        > lax.broadcasted_iota(jnp.int32, (groups, groups), 1), 1.0, 0.0).astype(BF16)
    before = jnp.sum(dot(above, low, PLAIN), axis=1, keepdims=True)
    local = dot(low, tri, PLAIN)
    rank = jnp.where(inside, local + before, -1.0).astype(jnp.int32)
    rank_s[...] = rank
    if local_s is not None:
        local_s[...] = jnp.where(inside, local, -1.0).astype(jnp.int32)
    group = lax.broadcasted_iota(jnp.int32, (groups, looks), 0)
    columns = (digits[0], digits[1], digits[3], group, jnp.where(inside, rel + 1, 0),
               (rank + 1) // LANES, (rank + 1) % LANES)
    for k, column in enumerate(columns):
        vals_s[:, k:k + 1, :] = column.astype(F32).reshape(groups, 1, looks)
    vals_s[:, len(columns):, :] = jnp.zeros((groups, 8 - len(columns), looks), F32)
    each = jnp.sum(jnp.where(inside, 1.0, 0.0), axis=1, keepdims=True)
    return jnp.sum(each, axis=0, keepdims=True), jnp.max(each, axis=0, keepdims=True)


def pick_into(found_s, step, rank_s, vals_s):
    chunk = found_s.shape[1]
    groups, looks = rank_s.shape
    slots = lax.broadcasted_iota(jnp.int32, (chunk, looks), 0)

    def pick(e, found):
        ranks = rank_s[pl.ds(e, 1), :] - step * chunk
        chosen = jnp.where(slots == ranks, 1.0, 0.0).astype(BF16)
        return found + dot(vals_s[e].astype(BF16), chosen, ACROSS)

    found = lax.fori_loop(0, groups, pick, jnp.zeros(found_s.shape, F32), unroll=4)
    found_s[...] = found.astype(jnp.int32)


def pick_few_into(found_s, local_s, vals_s, few_s):
    groups, looks = local_s.shape
    cap = few_s.shape[0] // groups
    slots = lax.broadcasted_iota(jnp.int32, (cap, looks), 0)
    for e in range(groups):
        chosen = jnp.where(slots == local_s[e:e + 1, :], 1.0, 0.0).astype(BF16)
        few_s[e * cap:(e + 1) * cap, :] = dot(chosen, vals_s[e].astype(BF16), ACROSS)
    few = few_s[...]
    ranks = (few[:, 5:6] * LANES + few[:, 6:7]).astype(jnp.int32) - 1
    slots = lax.broadcasted_iota(jnp.int32, (few.shape[0], found_s.shape[1]), 1)
    chosen = jnp.where(slots == ranks, 1.0, 0.0).astype(BF16)
    found_s[...] = dot(few.astype(BF16), chosen, DOWN).astype(jnp.int32)


def factors_into(plan, samples, spread_s, lsel_s, sample_s, found_s, c1, c3):
    first = dot(c1[...], hot(found_s[1:2, :], c1.shape[0], BF16), DOWN)
    last = dot(c3[...], hot(found_s[2:3, :], c3.shape[0], BF16), DOWN)
    lsel_s[...] = by_d3(last.astype(BF16))
    rel1 = found_s[4:5, :]
    for i in range(D1):
        part = first[i * R:(i + 1) * R, :]
        for r in range(plan.window):
            row = (i * plan.window + r) * R
            spread_s[row:row + R, :] = jnp.where(rel1 == r + 1, part, 0.0).astype(BF16)
    sample_s[...] = hot(found_s[3:4, :] * samples + found_s[0:1, :], sample_s.shape[0], BF16)


def middle_sum(plan, spread_s, lsel_s, gsel_s, glsel_s):
    grad_left_into(glsel_s, gsel_s, lsel_s)
    rows = plan.window * R
    total = None
    for i in range(D1):
        total = add(total, dot_parts(
            spread_s[i * rows:(i + 1) * rows, :], glsel_s[i * SIDE:(i + 1) * SIDE, :],
            ACROSS, 2, 1))
    return total


def select_scratch(plan, looks, samples, chunk):
    groups = plan.cores * plan.chips * plan.planes
    return [
        pltpu.VMEM((groups, looks), jnp.int32),
        pltpu.VMEM((groups, 8, looks), F32),
        pltpu.VMEM((8, chunk), jnp.int32),
        pltpu.VMEM((D1 * plan.window * R, chunk), BF16),
        pltpu.VMEM((R * D3, chunk), F32),
        pltpu.VMEM((groups * samples, chunk), BF16),
        pltpu.VMEM((WIDTH, chunk), F32),
        pltpu.VMEM((D1 * SIDE, chunk), F32),
    ]


STAGES = ("dz", "dx", "dc", "gz", "gx", "gc", "t0", "t1", "t2", "t3", "t4", "l0", "l1", "f0", "f1", "s2", "s3")


def step_kernel(plan, *refs):
    inputs, refs = refs[:12], refs[12:]
    digits_out, gp_out, top_ref, seg_ref, mid_ref, rest_ref = refs[:6]
    held, refs = refs[6:18], refs[18:]
    mid_s, first_s, last_s, lastd_s, left_s, gleft_s, emb_s, g_s, gf_s, gl_s = refs[:10]
    digits_ref, gp_ref = refs[10:12]
    top_s, topin, top1, topx, topz, seg_s, segin, seg1, segx, seg2, segz, seg3, segall = refs[12:25]
    rank_s, vals_s, found_s, spread_s, lsel_s, sample_s, gsel_s, glsel_s = refs[25:33]
    local_s, few_s, load_sems, save_sems, send_sems, recv_sems, grad_sems = refs[33:40]
    cores, chips, planes = plan.cores, plan.chips, plan.planes
    gx, plane = lax.axis_index("gx"), lax.axis_index("gy")
    core, chip = gx % cores, gx // cores
    scopes = []

    def mark(name):
        if scopes:
            scopes.pop().__exit__(None, None, None)
        if name:
            scopes.append(jax.named_scope(name))
            scopes[-1].__enter__()

    mark("m_start")
    c1, c2, c3, dense, w, bias, wout, labels, bag, d1, d2, d3 = held
    wide = c2.shape[1] // 2
    loads = {}

    def load(k, columns=None):
        src, dst = inputs[k], held[k]
        if columns is not None:
            src, dst = src.at[:, columns], dst.at[:, columns]
        n = len(loads)
        loads[n] = pltpu.make_async_copy(src, dst, load_sems.at[n])
        loads[n].start()
        return n

    early = [load(k) for k in (10, 9, 11, 8)]
    early += [load(k) for k in (0, 2)]
    tables = [load(1, slice(lo, lo + wide)) for lo in range(0, c2.shape[1], wide)]
    late = [load(k) for k in (3, 4, 5, 6, 7)]

    def at(c, q, p):
        return (q * cores + c, p)

    def on_core(k):
        return at((core + k) % cores, chip, plane)

    def on_chip(k):
        return at(core, (chip + k) % chips, plane)

    def on_plane(k):
        return at(core, chip, (plane + k) % planes)

    barrier = pltpu.get_barrier_semaphore()
    peers = [at((core + c) % cores, (chip + q) % chips, plane)
             for c in range(cores) for q in range(chips) if c or q]
    peers += [on_plane(k) for k in range(1, planes)]
    for peer in peers:
        pl.semaphore_signal(barrier, inc=1, device_id=peer, device_id_type=pl.DeviceIdType.MESH)

    def remote(src, dst, stage, peer, grad=None):
        n = STAGES.index(stage)
        return pltpu.make_async_remote_copy(
            src_ref=src, dst_ref=dst, send_sem=send_sems.at[n],
            recv_sem=recv_sems.at[n] if grad is None else grad_sems.at[grad], device_id=peer,
            device_id_type=pl.DeviceIdType.MESH)

    def push(src, dst, stage, peer, grad=None):
        remote(src, dst, stage, peer, grad).start()

    def arrive(like, stage, grad=None):
        remote(like, like, stage, on_core(1), grad).wait_recv()

    def leave(like, stage):
        remote(like, like, stage, on_core(1)).wait_send()

    def back(me, k, size):
        return (me + size - k) % size

    def own_z(ref, kind, rows=slice(None)):
        slot = ref.at[core, plane, chip, rows]
        for k in range(1, planes):
            push(slot, slot, kind + "z", on_plane(k))

    def push_x(ref, kind, k, grad=None, rows=slice(None)):
        slot = ref.at[core, back(plane, k, planes), chip, rows]
        for q in range(1, chips):
            push(slot, slot, kind + "x", on_chip(q), grad)

    def of_z(ref, rows=slice(None)):
        return ref.at[0, :planes - 1, 0, rows]

    def of_x(ref, rows=slice(None)):
        return ref.at[0, :, :chips - 1, rows]

    seg_s[...] = jnp.zeros_like(seg_s)
    mark("m_gather")
    for n in early:
        loads[n].wait()
    samples, looks = dense.shape[0], d1.shape[1]
    per = looks // LANES
    for k, digit in enumerate((bag, d1, d2, d3)):
        for h in range(per):
            digits_ref[core, plane, chip, k * per + h:k * per + h + 1, :] = (
                digit[:, h * LANES:(h + 1) * LANES].astype(F32))
    hot1 = hot(d1[...], c1.shape[0], BF16)
    hot2 = hot(d2[...], c2.shape[0], BF16)
    hot3 = hot(d3[...], c3.shape[0], BF16)
    first_s[...] = dot(c1[...], hot1, DOWN)
    last_t = dot(c3[...], hot3, DOWN)
    last_s[...] = last_t
    lastd_s[...] = by_d3(last_t.astype(BF16))
    for k, n in enumerate(tables):
        loads[n].wait()
        for lo, size in spans(wide, 512):
            lo += k * wide
            mid_s[lo:lo + size, :] = dot(c2[:, lo:lo + size], hot2, DOWN)
    mark("m_left")
    left_into(left_s, first_s, mid_s)
    for n in late:
        loads[n].wait()
    mark("m_emb")
    embedded_into(emb_s, left_s, last_s)

    mark("m_top")
    bags = hot(bag[...], samples, BF16)
    pooled = dot_parts(bags, emb_s[...], ACROSS, 3, 1).astype(BF16)
    pre = (
        dot(dense[...], w[:WIDTH, :], PLAIN) + dot(pooled, w[WIDTH:, :], PLAIN)
        + bias[...]
    )
    sig = jax.nn.sigmoid(pre)
    hidden = pre * sig
    logit = jnp.sum(hidden * wout[...], axis=1, keepdims=True)
    rows = lax.broadcasted_iota(jnp.int32, (samples, samples), 0)
    cols = lax.broadcasted_iota(jnp.int32, (samples, samples), 1)
    label = jnp.sum(
        jnp.where(rows == cols, labels[...].astype(F32), 0.0), axis=1, keepdims=True
    )
    dlogit = (jax.nn.sigmoid(logit) - label) / samples
    dpre = dlogit * wout[...] * (sig * (1.0 + pre * (1.0 - sig)))
    low = dpre.astype(BF16)

    mark("m_topgrad")
    deep = plan.trows - 8
    vectors = jnp.concatenate(
        [jnp.sum(dpre, axis=0, keepdims=True), jnp.sum(hidden * dlogit, axis=0, keepdims=True),
         jnp.zeros((6, dpre.shape[1]), F32)], axis=0)
    weight = [dot(dense[...], low, DOWN), dot(pooled, low, DOWN)]
    for h in range(cores):
        lanes = slice(h * LANES, (h + 1) * LANES)
        for q in range(chips):
            lo = q * deep
            half = weight[lo // WIDTH]
            top_s[h, q, :deep, :] = half[lo % WIDTH:lo % WIDTH + deep, lanes]
            top_s[h, q, deep:, :] = vectors[:, lanes] if q == 0 else jnp.zeros((8, LANES), F32)
    mark("m_barrier")
    pl.semaphore_wait(barrier, len(peers))
    mark("m_send")
    push(top_s.at[1 - core], topin, "t0", on_core(1))
    push_x(digits_ref, "d", 0)
    gp = dot(low, w[WIDTH:, :], ACROSS)
    gp_ref[core, plane, chip] = gp
    most = slice(None)
    own_z(gp_ref, "g", most)

    mark("m_gleft")
    g_s[...] = dot_parts(gp, bags, DOWN, 2, 0)
    mark("m_gl")
    grad_last_into(gl_s, left_s, g_s)

    def seg_rows(first):
        return slice(0, plan.frows) if first else slice(plan.frows, plan.srows)

    def seg_start(first, value):
        for seg in plan.segs:
            if seg.first == first:
                for c, q, lo, hi, h in pieces_of(seg, cores, chips, cores):
                    seg_s[c, q, seg.offset:seg.offset + hi - lo, :] = (
                        value[lo:hi, h * LANES:(h + 1) * LANES])
        rows = seg_rows(first)
        push(seg_s.at[1 - core, :, rows], segin.at[:, rows], "f0" if first else "l0", on_core(1))

    def seg_chips(first):
        rows = seg_rows(first)
        arrive(segin.at[:, rows], "f0" if first else "l0")
        seg1[:, rows] = seg_s[core, :, rows] + segin[:, rows]
        for k in range(1, chips):
            push(seg1.at[(chip + k) % chips, rows], segx.at[k, rows],
                 "f1" if first else "l1", on_chip(k))

    def out_of(p, k):
        seg = plan.segs[(p + k) % planes]
        return remote(seg2.at[seg.offset:seg.offset + seg.rows],
                      segz.at[k, :seg.rows], "s2", on_plane(k))

    def seg_planes(first):
        rows = seg_rows(first)
        arrive(segx.at[1:, rows], "f1" if first else "l1")
        total = seg1[chip, rows]
        for k in range(1, chips):
            total = total + segx[k, rows]
        seg2[rows] = total
        for p in range(planes):
            @pl.when(plane == p)
            def _(p=p):
                for k in range(1, planes):
                    if plan.segs[(p + k) % planes].first == first:
                        out_of(p, k).start()

    mark("m_ldot")
    seg_start(False, dot_parts(hot3, gl_s[...], ACROSS, 2, 1))
    mark("m_gleft2")
    grad_left_into(gleft_s, g_s, lastd_s)
    mark("m_t0")
    arrive(topin, "t0")
    top1[...] = top_s[core] + topin[...]
    for k in range(1, chips):
        push(top1.at[(chip + k) % chips], topx.at[k], "t1", on_chip(k))
    push_x(gp_ref, "g", 0, 0, most)

    mark("m_gf")
    grad_first_into(gf_s, gleft_s, mid_s, 0, 2)
    mark("m_l0")
    seg_chips(False)
    mark("m_dx")
    arrive(digits_ref.at[0, 0, :chips - 1], "dx")
    for k in range(1, planes):
        push(digits_ref.at[core, plane], digits_ref.at[core, plane], "dz", on_plane(k))
    mark("m_gf2")
    grad_first_into(gf_s, gleft_s, mid_s, 1, 2)
    mark("m_fdot")
    seg_start(True, dot_parts(hot1, gf_s[...], ACROSS, 2, 1))
    mark("m_f0")
    seg_chips(True)

    mark("m_gz")
    arrive(of_z(gp_ref, most), "gz")
    for k in range(1, planes):
        push_x(gp_ref, "g", k, k, most)
    mark("m_t1")
    arrive(topx.at[1:], "t1")
    total = top1[chip]
    for k in range(1, chips):
        total = total + topx[k]
    topz[plane] = total
    for k in range(1, planes):
        push(topz.at[plane], topz.at[plane], "t2", on_plane(k))

    mark("m_dz")
    arrive(digits_ref.at[0, :planes - 1], "dz")
    push(digits_ref.at[core], digits_ref.at[core], "dc", on_core(1))
    mark("m_df")
    arrive(digits_ref.at[1 - core], "dc")
    mark("m_rank")
    groups = cores * planes * chips
    count, fullest = rank_lookups(
        plan, digits_ref[...].reshape(groups, *digits_ref.shape[3:]), rank_s, vals_s, local_s)
    fits = (count <= found_s.shape[1]) & (fullest <= few_s.shape[0] // groups)
    rest_ref[...] = jnp.broadcast_to(jnp.where(fits, 0.0, 1.0), rest_ref.shape)
    mark("m_pick")
    pick_few_into(found_s, local_s, vals_s, few_s)

    mark("m_l1")
    seg_planes(False)
    mark("m_f1")
    seg_planes(True)
    mark("m_factors")
    factors_into(plan, samples, spread_s, lsel_s, sample_s, found_s, c1, c3)
    mark("m_t2")
    arrive(topz.at[1:], "t2")
    total = topz[0]
    for k in range(1, planes):
        total = total + topz[k]
    top_ref[core, chip] = total
    for k in range(1, chips):
        push(top_ref.at[core, chip], top_ref.at[core, chip], "t3", on_chip(k))

    mark("m_gx")

    def chosen_sum(c):
        size = planes * chips * samples
        return dot_parts(
            gp_ref[c].reshape(size, WIDTH), sample_s[pl.ds(pl.multiple_of(c * size, size), size), :],
            DOWN, 2, 0)

    for k in range(planes):
        slot = gp_ref.at[core, back(plane, k, planes)]
        arrive(gp_ref.at[0, 0, :chips - 1, most], "gx", k)
        push(slot, slot, "gc", on_core(1), planes + k)
    gsel_s[...] = chosen_sum(core)

    mark("m_s2")

    def to_owner(p):
        seg = plan.segs[p]
        return remote(seg3.at[:seg.rows], seg_ref.at[core, chip, :seg.rows], "s3",
                      (seg.owner, plane))

    for p in range(planes):
        @pl.when(plane == p)
        def _(p=p):
            seg = plan.segs[p]
            arrive(segz.at[1:, :seg.rows], "s2")
            total = seg2[seg.offset:seg.offset + seg.rows]
            for k in range(1, planes):
                total = total + segz[k, :seg.rows]
            seg3[:seg.rows] = total

            @pl.when(gx != seg.owner)
            def _():
                to_owner(p).start()

    mark("m_t3")
    arrive(top_ref.at[0, 1:], "t3")
    push(top_ref.at[core], top_ref.at[core], "t4", on_core(1))

    mark("m_gfin")
    for k in range(planes):
        arrive(gp_ref.at[0, 0], "gc", planes + k)
    gsel_s[...] = gsel_s[...] + chosen_sum(1 - core)
    saves = [pltpu.make_async_copy(digits_ref, digits_out, save_sems.at[0]),
             pltpu.make_async_copy(gp_ref, gp_out, save_sems.at[1])]
    for save in saves:
        save.start()
    mark("m_mid")
    mid_ref[...] = middle_sum(plan, spread_s, lsel_s, gsel_s, glsel_s)

    mark("m_s3")
    for p in range(planes):
        seg = plan.segs[p]

        @pl.when((plane == p) & (gx == seg.owner))
        def _(p=p, seg=seg):
            own_core, own_chip = seg.owner % cores, seg.owner // cores
            seg_ref[own_core, own_chip, :seg.rows] = seg3[:seg.rows]
            arrive(segall.at[:(cores * chips - 1) * seg.rows], "s3")

    mark("m_t4")
    arrive(top_ref.at[1 - core], "t4")
    mark("m_sent")
    for save in saves:
        save.wait()
    leave(digits_ref.at[0, 0, :chips - 1], "dx")
    leave(digits_ref.at[0, :planes - 1], "dz")
    leave(of_z(gp_ref, most), "gz")
    leave(of_x(gp_ref, most), "gx")
    for ref, stage in ((digits_ref, "dc"), (gp_ref, "gc")):
        leave(ref.at[0], stage)
    for stage, like in (
        ("t0", topin), ("t1", topx.at[1:]), ("t2", topz.at[1:]), ("t3", top_ref.at[0, 1:]),
        ("t4", top_ref.at[0]), ("l0", segin.at[:, seg_rows(False)]),
        ("l1", segx.at[1:, seg_rows(False)]), ("f0", segin.at[:, seg_rows(True)]),
        ("f1", segx.at[1:, seg_rows(True)])):
        leave(like, stage)
    for p in range(planes):
        @pl.when(plane == p)
        def _(p=p):
            seg = plan.segs[p]
            leave(seg2.at[:plan.srows - seg.rows], "s2")

            @pl.when(gx != seg.owner)
            def _():
                to_owner(p).wait_send()
    mark(None)


def step_part(plan, chunk, *inputs):
    c1, c2, c3, dense, w, bias, wout, labels, bag, d1, d2, d3 = inputs
    samples, looks = dense.shape[0], d1.shape[1]
    cores, chips, planes = plan.cores, plan.chips, plan.planes
    groups = cores * chips * planes
    vmem = pl.BlockSpec(memory_space=pltpu.VMEM)
    hbm = pl.BlockSpec(memory_space=pltpu.HBM)
    scratch = [R * SIDE, D1 * R, R * D3, R * D3, D1 * SIDE, D1 * SIDE, WIDTH, WIDTH, D1 * R, R * D3]
    top, seg = (plan.trows, LANES), (plan.srows, LANES)
    digits = (cores, planes, chips, up(4 * looks // LANES, 8), LANES)
    grads = (cores, planes, chips, samples, WIDTH)
    sums = [
        digits, grads,
        (cores, chips, *top), (chips, *top), (chips, *top), (chips, *top), (planes, *top),
        (cores, chips, *seg), (chips, *seg), (chips, *seg), (chips, *seg), seg,
        (planes, plan.smost, LANES), (plan.smost, LANES), (cores * chips * plan.smost, LANES)]
    inputs = [pltpu.with_memory_space_constraint(x, pltpu.HBM) for x in inputs]
    return pl.pallas_call(
        functools.partial(step_kernel, plan),
        in_specs=[hbm] * len(inputs),
        out_specs=(hbm, hbm, vmem, vmem, vmem, vmem),
        out_shape=(
            pltpu.HBM(digits, F32),
            pltpu.HBM(grads, F32),
            pltpu.VMEM((cores, chips, *top), F32),
            pltpu.VMEM((cores, chips, plan.smost, LANES), F32),
            pltpu.VMEM((plan.window * R, SIDE), F32),
            pltpu.VMEM((8, LANES), F32),
        ),
        scratch_shapes=[pltpu.VMEM(x.shape, x.dtype) for x in inputs]
        + [pltpu.VMEM((rows, looks), F32) for rows in scratch]
        + [pltpu.VMEM(dims, F32) for dims in sums]
        + select_scratch(plan, looks, samples, chunk)
        + [pltpu.VMEM((groups, looks), jnp.int32), pltpu.VMEM((groups * LOCAL, 8), F32)]
        + [pltpu.SemaphoreType.DMA((len(inputs) + 1,)), pltpu.SemaphoreType.DMA((2,))]
        + [pltpu.SemaphoreType.DMA((len(STAGES),)) for _ in range(2)]
        + [pltpu.SemaphoreType.DMA((2 * planes,))],
        compiler_params=pltpu.CompilerParams(
            collective_id=0, has_side_effects=True, vmem_limit_bytes=40 << 20),
        name="step",
    )(*inputs)


def finish_kernel(
    plan, c1_in, c3_in, digits_in, gp_in, top, seg_in, mid, rest_in, core_out, top_out,
    c1, c3, blocks_s, gp_s, rank_s, vals_s, found_s, spread_s, lsel_s, sample_s, gsel_s, glsel_s,
    big_s, core_s, top_s, more_sems, out_sems,
):
    cores, chips, planes, window = plan.cores, plan.chips, plan.planes, plan.window
    gx, plane = lax.axis_index("gx"), lax.axis_index("gy")
    r0, start = first_row(plan)
    chunk = found_s.shape[1]

    deep = plan.trows - 8
    for h in range(cores):
        lanes = slice(h * LANES, (h + 1) * LANES)
        for q in range(chips):
            top_s[q * deep:(q + 1) * deep, lanes] = top[h, q, :deep, :]
        top_s[chips * deep:, lanes] = top[h, 0, deep:deep + 2, :]
    save_top = pltpu.make_async_copy(top_s, top_out, out_sems.at[0])
    save_top.start()

    base, rows = plan.n1 // LANES, window * R
    big_s[base:base + rows, :] = mid[...]

    @pl.when(jnp.max(rest_in[...]) > 0.0)
    def _():
        pairs = zip((c1_in, c3_in, digits_in, gp_in), (c1, c3, blocks_s, gp_s))
        loads = [pltpu.make_async_copy(a, b, more_sems.at[k]) for k, (a, b) in enumerate(pairs)]
        for load in loads:
            load.start()
        for load in loads:
            load.wait()
        groups, samples = rank_s.shape[0], gp_s.shape[3]
        count, _ = rank_lookups(
            plan, blocks_s[...].reshape(groups, *blocks_s.shape[3:]), rank_s, vals_s)
        count = jnp.max(count).astype(jnp.int32)
        big_s[base:base + rows, :] = jnp.zeros((rows, LANES), F32)

        def body(step, carry):
            pick_into(found_s, step, rank_s, vals_s)
            factors_into(plan, samples, spread_s, lsel_s, sample_s, found_s, c1, c3)
            gsel_s[...] = dot_parts(
                gp_s[...].reshape(groups * samples, WIDTH), sample_s[...], DOWN, 2, 0)
            big_s[base:base + rows, :] = big_s[base:base + rows, :] + middle_sum(
                plan, spread_s, lsel_s, gsel_s, glsel_s)
            return carry

        lax.fori_loop(0, (count + chunk - 1) // chunk, body, 0)

    halves = seg_in.shape[0]
    for p in range(planes):
        seg = plan.segs[p]

        @pl.when((plane == p) & (gx == seg.owner))
        def _(seg=seg):
            for c, q, lo, hi, h in pieces_of(seg, cores, chips, halves):
                piece = seg_in[c, q, :hi - lo, :]
                if seg.first:
                    big_s[lo:hi, :] = piece
                else:
                    big_s[pl.ds(base + rows + lo * halves + h, hi - lo, stride=halves), :] = piece

    at = start // LANES - r0 * (plan.row // LANES)
    shift = start % LANES
    size = core_s.shape[0]
    here, after = big_s[pl.ds(at, size), :], big_s[pl.ds(at + 1, size), :]
    turn = (LANES - shift) % LANES
    lane = lax.broadcasted_iota(jnp.int32, (size, LANES), 1)
    core_s[...] = jnp.where(
        lane < LANES - shift, pltpu.roll(here, turn, 1), pltpu.roll(after, turn, 1))
    save_core = pltpu.make_async_copy(core_s, core_out, out_sems.at[1])
    save_core.start()
    save_top.wait()
    save_core.wait()


def finish_part(plan, chunk, looks, c1, c3, digits, gp, top, seg, mid, rest):
    vmem = pl.BlockSpec(memory_space=pltpu.VMEM)
    hbm = pl.BlockSpec(memory_space=pltpu.HBM)
    out_rows = up(-(-plan.share // LANES), 8)
    big = up(plan.n1 // LANES + plan.window * R + plan.n3_rows * seg.shape[0] + out_rows, 8)
    core_shape = (out_rows, LANES)
    top_shape = (plan.chips * (plan.trows - 8) + 2, plan.cores * LANES)
    far = [pltpu.with_memory_space_constraint(x, pltpu.HBM) for x in (c1, c3, digits, gp)]
    return pl.pallas_call(
        functools.partial(finish_kernel, plan),
        out_shape=(pltpu.HBM(core_shape, F32), pltpu.HBM(top_shape, F32)),
        in_specs=[hbm] * 4 + [vmem] * 4,
        out_specs=(hbm, hbm),
        scratch_shapes=[pltpu.VMEM(x.shape, x.dtype) for x in (c1, c3, digits, gp)]
        + select_scratch(plan, looks, gp.shape[3], chunk)
        + [pltpu.VMEM((big, LANES), F32), pltpu.VMEM(core_shape, F32),
           pltpu.VMEM(top_shape, F32), pltpu.SemaphoreType.DMA((4,)), pltpu.SemaphoreType.DMA((2,))],
        compiler_params=pltpu.CompilerParams(vmem_limit_bytes=40 << 20),
        name="finish",
    )(*far, top, seg, mid, rest)


def per_device(plan, c1, c2, c3, dense, w, bias, wout, labels, bag, d1, d2, d3):
    looks = d1.shape[1]
    expected = plan.nx * plan.ny * looks * plan.window // plan.n2_rows
    chunk = up(expected * 9 // 8, LANES)
    digits, gp, top, seg, mid, rest = step_part(
        plan, chunk, c1, c2, c3, dense, w, bias[None], wout[None], labels[None], bag, d1, d2, d3)
    core, top = finish_part(plan, chunk, looks, c1, c3, digits, gp, top, seg, mid, rest)
    return core.reshape(-1)[:plan.share], top


def one_hot(digits, count, kind):
    return (digits[:, None] == jnp.arange(count, dtype=jnp.int32)[None, :]).astype(kind)


def slices(digits, core):
    return jnp.dot(
        one_hot(digits, core.shape[0], jnp.bfloat16), core, preferred_element_type=jnp.float32
    )


def factors(digits, cores):
    high = lax.Precision.HIGHEST
    first = slices(digits[0], cores[0]).reshape(-1, D1, R)
    middle = slices(digits[1], cores[1]).reshape(-1, R, D2 * R)
    last = slices(digits[2], cores[2]).reshape(-1, R, D3)
    left = jnp.einsum("nia,nab->nib", first, middle, precision=high).reshape(-1, D1 * D2, R)
    return (first, middle, last, left)


def top_total(top_local):
    return lax.psum(top_local, ("gx", "gy"))


def per_device_dense(
    core_one,
    core_two,
    core_three,
    dense_rows,
    w_top,
    bias_top,
    w_out,
    labels,
    bag_ids,
    digit_one,
    digit_two,
    digit_three,
):
    high = lax.Precision.HIGHEST
    cores = (core_one, core_two, core_three)
    digits = jnp.stack([digit_one[0], digit_two[0], digit_three[0]])
    looks = digits.shape[1]
    block = min(256, looks)
    blocks = looks // block
    blocked = digits.reshape(3, blocks, block).transpose(1, 0, 2)
    width = D1 * D2 * D3

    def forward(carry, part):
        first, middle, last, left = factors(part, cores)
        return (carry, jnp.einsum("npa,nad->npd", left, last, precision=high).reshape(block, width))

    _, embedded = lax.scan(forward, jnp.zeros((), jnp.float32), blocked)
    embedded = embedded.reshape(looks, width)
    samples = dense_rows.shape[0]
    bag_table = one_hot(bag_ids[0], samples, jnp.float32)
    pooled = jnp.dot(bag_table.T, embedded, precision=high)
    joined = jnp.concatenate([dense_rows, pooled.astype(jnp.bfloat16)], axis=1)
    pre = jnp.dot(joined, w_top, preferred_element_type=jnp.float32) + bias_top[None, :]
    sig = jax.nn.sigmoid(pre)
    hidden = pre * sig
    logit = jnp.dot(hidden, w_out, precision=high)
    dlogit = (jax.nn.sigmoid(logit) - labels.astype(jnp.float32)) / samples
    dpre = dlogit[:, None] * w_out[None, :] * (sig * (1.0 + pre * (1.0 - sig)))
    dpre_low = dpre.astype(jnp.bfloat16)
    grad_weight = jnp.dot(joined.T, dpre_low, preferred_element_type=jnp.float32)
    grad_bias = jnp.sum(dpre, axis=0)
    grad_output = jnp.sum(hidden * dlogit[:, None], axis=0)
    top_local = jnp.concatenate([grad_weight, grad_bias[None, :], grad_output[None, :]], axis=0)
    grad_pooled = jnp.dot(dpre_low, w_top[width:].T, preferred_element_type=jnp.float32)
    grad_embedded = jnp.dot(bag_table, grad_pooled, precision=high).reshape(blocks, block, width)

    def backward(totals, inputs):
        part, grad_block = inputs
        first, middle, last, left = factors(part, cores)
        grad_view = grad_block.reshape(block, D1 * D2, D3)
        grad_last = jnp.einsum("npa,npd->nad", left, grad_view, precision=high)
        grad_left = jnp.einsum("npd,nad->npa", grad_view, last, precision=high).reshape(
            block, D1, D2 * R
        )
        grad_first = jnp.einsum("nib,nab->nia", grad_left, middle, precision=high)
        grad_middle = jnp.einsum("nia,nib->nab", first, grad_left, precision=high)
        pieces = (
            grad_first.reshape(block, -1),
            grad_middle.reshape(block, -1),
            grad_last.reshape(block, -1),
        )
        updated = tuple(
            (
                total
                + jnp.dot(
                    one_hot(part[number], cores[number].shape[0], jnp.float32).T,
                    pieces[number],
                    precision=high,
                )
                for number, total in enumerate(totals)
            )
        )
        return (updated, None)

    start = tuple((jnp.zeros(core.shape, jnp.float32) for core in cores))
    totals, _ = lax.scan(backward, start, (blocked, grad_embedded))
    flat = jnp.concatenate([total.reshape(-1) for total in totals])
    core_grad = lax.psum_scatter(flat, ("gx", "gy"), scatter_dimension=0, tiled=True)
    top_grad = top_total(top_local)
    return (core_grad, top_grad)


def solution(mesh):
    nx, ny = mesh.shape["gx"], mesh.shape["gy"]
    whole, split, rows = P(), P(AXES), P(AXES, None)

    def step(*args):
        cores, dense = args[:3], args[3]
        plan = None
        if dense.size < sum(core.size for core in cores):
            plan = plan_of(nx, ny, *(core.shape for core in cores), args[4].shape)
        body = functools.partial(per_device, plan) if plan else per_device_dense
        return jax.shard_map(
            body,
            mesh=mesh,
            in_specs=(
                whole, whole, whole, rows, whole, whole, whole, split,
                rows, rows, rows, rows,
            ),
            out_specs=(split, whole),
            check_vma=False,
        )(*args)

    return step
```

```python
import functools
import types

import jax
import jax.numpy as jnp
from jax import lax
from jax.experimental import pallas as pl
from jax.experimental.pallas import tpu as pltpu
from jax.sharding import PartitionSpec as P

D1 = 4
D2 = 4
D3 = 8
R = 32
WIDTH = D1 * D2 * D3
PAIRS = D1 * D2
SIDE = D2 * R
LANES = 128
LOCAL = 32
AXES = ("gx", "gy")
F32 = jnp.float32
BF16 = jnp.bfloat16
HIGH = lax.Precision.HIGHEST
PLAIN, ACROSS, DOWN = ((1,), (0,)), ((1,), (1,)), ((0,), (0,))


def dot(a, b, dims, precision=None):
    return lax.dot_general(
        a, b, (dims, ((), ())), precision=precision, preferred_element_type=F32
    )


def parts_of(x, count):
    parts = []
    for _ in range(count):
        part = x.astype(BF16)
        parts.append(part)
        x = x - part.astype(F32)
    return parts


def dot_parts(a, b, dims, count, wide):
    free = 1 - dims[wide][0]
    joined = jnp.concatenate(parts_of((a, b)[wide], count), axis=free)
    out = dot(joined, b, dims) if wide == 0 else dot(a, joined, dims)
    size = out.shape[wide] // count
    total = None
    for k in range(count):
        part = lax.slice_in_dim(out, k * size, (k + 1) * size, axis=wide)
        total = part if total is None else total + part
    return total


def hot(row, count, kind):
    numbers = lax.broadcasted_iota(jnp.int32, (count, row.shape[1]), 0)
    return jnp.where(numbers == row, 1.0, 0.0).astype(kind)


def by_d3(last_t):
    size = R * D3
    to = lax.broadcasted_iota(jnp.int32, (size, size), 0)
    of = lax.broadcasted_iota(jnp.int32, (size, size), 1)
    turn = jnp.where(of == (to % R) * D3 + to // R, 1.0, 0.0).astype(BF16)
    return dot(turn, last_t, PLAIN)


def up(count, step):
    return -(-count // step) * step


def plan_of(nx, ny, shape_one, shape_two, shape_three, shape_top):
    cores = 2
    if nx % cores:
        return None
    chips, planes, devices = nx // cores, ny, nx * ny
    n1, n2, n3 = (s[0] * s[1] for s in (shape_one, shape_two, shape_three))
    total = n1 + n2 + n3
    if total % devices or shape_one[1] != LANES or n1 % LANES or shape_two[1] % LANES:
        return None
    if shape_three[1] != cores * LANES or shape_top[1] != cores * LANES or shape_top[0] % (8 * chips):
        return None
    share = total // devices
    row = shape_two[1]
    window = min(-(-share // row) + 1, shape_two[0])
    segs, offset = [None] * planes, 0
    for d in range(devices):
        lo, hi = d * share, (d + 1) * share
        has_first, has_last = lo < n1, hi > n1 + n2
        if not (has_first or has_last):
            continue
        if has_first and has_last or segs[d % planes] is not None:
            return None
        seg = types.SimpleNamespace(owner=d // planes, first=has_first)
        if has_first:
            seg.lo, seg.hi = lo // LANES, -(-min(hi, n1) // LANES)
            seg.rows = up(-(-(seg.hi - seg.lo) // (cores * chips)), 8)
        else:
            seg.lo = max(lo - n1 - n2, 0) // shape_three[1] // 8 * 8
            seg.hi = -(-(hi - n1 - n2) // shape_three[1])
            seg.rows = up(-(-(seg.hi - seg.lo) // chips), 8)
        segs[d % planes] = seg
    if any(seg is None for seg in segs):
        return None
    for seg in sorted(segs, key=lambda seg: not seg.first):
        seg.offset = offset
        offset += seg.rows
    return types.SimpleNamespace(
        nx=nx, ny=ny, cores=cores, chips=chips, planes=planes, share=share, window=window,
        row=row, n1=n1, segs=segs, srows=offset, frows=sum(seg.rows for seg in segs if seg.first), smost=max(seg.rows for seg in segs),
        trows=shape_top[0] // chips + 8, n2_rows=shape_two[0], n3_rows=shape_three[0])


def pieces_of(seg, cores, chips, halves):
    for core in range(cores):
        for chip in range(chips):
            n = core * chips + chip if seg.first else chip
            lo = seg.lo + n * seg.rows
            hi = min(lo + seg.rows, seg.hi)
            if lo < hi:
                yield core, chip, lo, hi, 0 if seg.first else core


def spans(count, step):
    return [(lo, min(step, count - lo)) for lo in range(0, count, step)]


def lane_loop(count, lanes, body, start=0):
    blocks = lanes // LANES

    @pl.loop(start * blocks, count * blocks)
    def _(step):
        body(step // blocks, pl.ds(pl.multiple_of((step % blocks) * LANES, LANES), LANES))


def add(total, term):
    return term if total is None else total + term


def left_into(left_s, first_s, mid_s):
    def body(j, lanes):
        totals = [None] * D1
        for a in range(R):
            m = mid_s[pl.ds(pl.multiple_of(a * SIDE + j * R, R), R), lanes]
            for i in range(D1):
                totals[i] = add(totals[i], first_s[i * R + a:i * R + a + 1, lanes] * m)
        for i in range(D1):
            left_s[pl.ds(pl.multiple_of(i * SIDE + j * R, R), R), lanes] = totals[i]

    lane_loop(D2, left_s.shape[1], body)


def embedded_into(emb_s, left_s, last_s, batch=8):
    @pl.loop(0, PAIRS // batch)
    def _(b):
        totals = [None] * batch
        left = left_s.at[pl.ds(pl.multiple_of(b * batch * R, batch * R), batch * R), :]
        for c in range(R):
            last = last_s[c * D3:(c + 1) * D3, :]
            for k in range(batch):
                row = k * R + c
                totals[k] = add(totals[k], left[row:row + 1, :] * last)
        for k in range(batch):
            emb_s[pl.ds(pl.multiple_of((b * batch + k) * D3, D3), D3), :] = totals[k]


def grad_left_into(gleft_s, g_s, lastd_s):
    batch = 4 if gleft_s.shape[1] <= 2 * LANES else 2

    @pl.loop(0, PAIRS // batch)
    def _(b):
        totals = [None] * batch
        g = g_s.at[pl.ds(pl.multiple_of(b * batch * D3, batch * D3), batch * D3), :]
        for d in range(D3):
            last = lastd_s[d * R:(d + 1) * R, :]
            for k in range(batch):
                row = k * D3 + d
                totals[k] = add(totals[k], g[row:row + 1, :] * last)
        for k in range(batch):
            gleft_s[pl.ds(pl.multiple_of((b * batch + k) * R, R), R), :] = totals[k]


def grad_last_into(gl_s, left_s, g_s, batch=8):
    @pl.loop(0, R // batch)
    def _(b):
        totals = [None] * batch
        left = left_s.at[pl.ds(pl.multiple_of(b * batch, batch), (PAIRS - 1) * R + batch), :]
        for p in range(PAIRS):
            g = g_s[p * D3:(p + 1) * D3, :]
            for k in range(batch):
                row = p * R + k
                totals[k] = add(totals[k], left[row:row + 1, :] * g)
        for k in range(batch):
            gl_s[pl.ds(pl.multiple_of((b * batch + k) * D3, D3), D3), :] = totals[k]


def grad_first_into(gf_s, gleft_s, mid_s, part, parts, batch=8):
    def body(b, lanes):
        totals = [[None] * D1 for _ in range(batch)]
        size = batch * SIDE
        mid = mid_s.at[pl.ds(pl.multiple_of(b * size, size), size), lanes]
        gleft = gleft_s.at[:, lanes]
        for t in range(0, SIDE, 8):
            rows = [gleft[i * SIDE + t:i * SIDE + t + 8, :] for i in range(D1)]
            for k in range(batch):
                m = mid[k * SIDE + t:k * SIDE + t + 8, :]
                for i in range(D1):
                    totals[k][i] = add(totals[k][i], rows[i] * m)
        for i in range(D1):
            rows = [jnp.sum(totals[k][i], axis=0, keepdims=True) for k in range(batch)]
            gf_s[pl.ds(pl.multiple_of(i * R + b * batch, 8), batch), lanes] = (
                jnp.concatenate(rows, axis=0))

    count = R // batch
    lane_loop((part + 1) * count // parts, gf_s.shape[1], body, part * count // parts)


def first_row(plan):
    start = (lax.axis_index("gx") * plan.planes + lax.axis_index("gy")) * plan.share
    return jnp.clip((start - plan.n1) // plan.row, 0, plan.n2_rows - plan.window), start


def rank_lookups(plan, blocks, rank_s, vals_s, local_s=None):
    groups, looks = rank_s.shape
    per = looks // LANES
    r0, _ = first_row(plan)
    digits = [
        jnp.concatenate([blocks[:, k * per + h, :] for h in range(per)], axis=1).astype(jnp.int32)
        for k in range(4)
    ]
    rel = digits[2] - r0
    inside = (rel >= 0) & (rel < plan.window)
    low = jnp.where(inside, 1.0, 0.0).astype(BF16)
    tri = jnp.where(
        lax.broadcasted_iota(jnp.int32, (looks, looks), 0)
        < lax.broadcasted_iota(jnp.int32, (looks, looks), 1), 1.0, 0.0).astype(BF16)
    above = jnp.where(
        lax.broadcasted_iota(jnp.int32, (groups, groups), 0)
        > lax.broadcasted_iota(jnp.int32, (groups, groups), 1), 1.0, 0.0).astype(BF16)
    before = jnp.sum(dot(above, low, PLAIN), axis=1, keepdims=True)
    local = dot(low, tri, PLAIN)
    rank = jnp.where(inside, local + before, -1.0).astype(jnp.int32)
    rank_s[...] = rank
    if local_s is not None:
        local_s[...] = jnp.where(inside, local, -1.0).astype(jnp.int32)
    group = lax.broadcasted_iota(jnp.int32, (groups, looks), 0)
    columns = (digits[0], digits[1], digits[3], group, jnp.where(inside, rel + 1, 0),
               (rank + 1) // LANES, (rank + 1) % LANES)
    for k, column in enumerate(columns):
        vals_s[:, k:k + 1, :] = column.astype(F32).reshape(groups, 1, looks)
    vals_s[:, len(columns):, :] = jnp.zeros((groups, 8 - len(columns), looks), F32)
    each = jnp.sum(jnp.where(inside, 1.0, 0.0), axis=1, keepdims=True)
    return jnp.sum(each, axis=0, keepdims=True), jnp.max(each, axis=0, keepdims=True)


def pick_into(found_s, step, rank_s, vals_s):
    chunk = found_s.shape[1]
    groups, looks = rank_s.shape
    slots = lax.broadcasted_iota(jnp.int32, (chunk, looks), 0)

    def pick(e, found):
        ranks = rank_s[pl.ds(e, 1), :] - step * chunk
        chosen = jnp.where(slots == ranks, 1.0, 0.0).astype(BF16)
        return found + dot(vals_s[e].astype(BF16), chosen, ACROSS)

    found = lax.fori_loop(0, groups, pick, jnp.zeros(found_s.shape, F32), unroll=4)
    found_s[...] = found.astype(jnp.int32)


def pick_few_into(found_s, local_s, vals_s, few_s):
    groups, looks = local_s.shape
    cap = few_s.shape[0] // groups
    slots = lax.broadcasted_iota(jnp.int32, (cap, looks), 0)
    for e in range(groups):
        chosen = jnp.where(slots == local_s[e:e + 1, :], 1.0, 0.0).astype(BF16)
        few_s[e * cap:(e + 1) * cap, :] = dot(chosen, vals_s[e].astype(BF16), ACROSS)
    few = few_s[...]
    ranks = (few[:, 5:6] * LANES + few[:, 6:7]).astype(jnp.int32) - 1
    slots = lax.broadcasted_iota(jnp.int32, (few.shape[0], found_s.shape[1]), 1)
    chosen = jnp.where(slots == ranks, 1.0, 0.0).astype(BF16)
    found_s[...] = dot(few.astype(BF16), chosen, DOWN).astype(jnp.int32)


def factors_into(plan, samples, spread_s, lsel_s, sample_s, found_s, c1, c3):
    first = dot(c1[...], hot(found_s[1:2, :], c1.shape[0], BF16), DOWN)
    last = dot(c3[...], hot(found_s[2:3, :], c3.shape[0], BF16), DOWN)
    lsel_s[...] = by_d3(last.astype(BF16))
    rel1 = found_s[4:5, :]
    for i in range(D1):
        part = first[i * R:(i + 1) * R, :]
        for r in range(plan.window):
            row = (i * plan.window + r) * R
            spread_s[row:row + R, :] = jnp.where(rel1 == r + 1, part, 0.0).astype(BF16)
    sample_s[...] = hot(found_s[3:4, :] * samples + found_s[0:1, :], sample_s.shape[0], BF16)


def middle_sum(plan, spread_s, lsel_s, gsel_s, glsel_s):
    grad_left_into(glsel_s, gsel_s, lsel_s)
    rows = plan.window * R
    total = None
    for i in range(D1):
        total = add(total, dot_parts(
            spread_s[i * rows:(i + 1) * rows, :], glsel_s[i * SIDE:(i + 1) * SIDE, :],
            ACROSS, 2, 1))
    return total


def select_scratch(plan, looks, samples, chunk):
    groups = plan.cores * plan.chips * plan.planes
    return [
        pltpu.VMEM((groups, looks), jnp.int32),
        pltpu.VMEM((groups, 8, looks), F32),
        pltpu.VMEM((8, chunk), jnp.int32),
        pltpu.VMEM((D1 * plan.window * R, chunk), BF16),
        pltpu.VMEM((R * D3, chunk), F32),
        pltpu.VMEM((groups * samples, chunk), BF16),
        pltpu.VMEM((WIDTH, chunk), F32),
        pltpu.VMEM((D1 * SIDE, chunk), F32),
    ]


STAGES = ("dz", "dx", "dc", "gz", "gx", "gc", "t0", "t1", "t2", "t3", "t4", "l0", "l1", "f0", "f1", "s2", "s3")


def step_kernel(plan, *refs):
    inputs, refs = refs[:12], refs[12:]
    digits_out, gp_out, top_ref, seg_ref, mid_ref, rest_ref = refs[:6]
    held, refs = refs[6:18], refs[18:]
    mid_s, first_s, last_s, lastd_s, left_s, gleft_s, emb_s, g_s, gf_s, gl_s = refs[:10]
    digits_ref, gp_ref = refs[10:12]
    top_s, topin, top1, topx, topz, seg_s, segin, seg1, segx, seg2, segz, seg3, segall = refs[12:25]
    rank_s, vals_s, found_s, spread_s, lsel_s, sample_s, gsel_s, glsel_s = refs[25:33]
    local_s, few_s, load_sems, save_sems, send_sems, recv_sems, grad_sems = refs[33:40]
    cores, chips, planes = plan.cores, plan.chips, plan.planes
    gx, plane = lax.axis_index("gx"), lax.axis_index("gy")
    core, chip = gx % cores, gx // cores
    scopes = []

    def mark(name):
        if scopes:
            scopes.pop().__exit__(None, None, None)
        if name:
            scopes.append(jax.named_scope(name))
            scopes[-1].__enter__()

    mark("m_start")
    c1, c2, c3, dense, w, bias, wout, labels, bag, d1, d2, d3 = held
    wide = c2.shape[1] // 2
    loads = {}

    def load(k, columns=None):
        src, dst = inputs[k], held[k]
        if columns is not None:
            src, dst = src.at[:, columns], dst.at[:, columns]
        n = len(loads)
        loads[n] = pltpu.make_async_copy(src, dst, load_sems.at[n])
        loads[n].start()
        return n

    early = [load(k) for k in (10, 9, 11, 8)]
    early += [load(k) for k in (0, 2)]
    tables = [load(1, slice(lo, lo + wide)) for lo in range(0, c2.shape[1], wide)]
    late = [load(k) for k in (3, 4, 5, 6, 7)]

    def at(c, q, p):
        return (q * cores + c, p)

    def on_core(k):
        return at((core + k) % cores, chip, plane)

    def on_chip(k):
        return at(core, (chip + k) % chips, plane)

    def on_plane(k):
        return at(core, chip, (plane + k) % planes)

    barrier = pltpu.get_barrier_semaphore()
    peers = [at((core + c) % cores, (chip + q) % chips, plane)
             for c in range(cores) for q in range(chips) if c or q]
    peers += [on_plane(k) for k in range(1, planes)]
    for peer in peers:
        pl.semaphore_signal(barrier, inc=1, device_id=peer, device_id_type=pl.DeviceIdType.MESH)

    def remote(src, dst, stage, peer, grad=None):
        n = STAGES.index(stage)
        return pltpu.make_async_remote_copy(
            src_ref=src, dst_ref=dst, send_sem=send_sems.at[n],
            recv_sem=recv_sems.at[n] if grad is None else grad_sems.at[grad], device_id=peer,
            device_id_type=pl.DeviceIdType.MESH)

    def push(src, dst, stage, peer, grad=None):
        remote(src, dst, stage, peer, grad).start()

    def arrive(like, stage, grad=None):
        remote(like, like, stage, on_core(1), grad).wait_recv()

    def leave(like, stage):
        remote(like, like, stage, on_core(1)).wait_send()

    def back(me, k, size):
        return (me + size - k) % size

    def own_z(ref, kind, rows=slice(None)):
        slot = ref.at[core, plane, chip, rows]
        for k in range(1, planes):
            push(slot, slot, kind + "z", on_plane(k))

    def push_x(ref, kind, k, grad=None, rows=slice(None)):
        slot = ref.at[core, back(plane, k, planes), chip, rows]
        for q in range(1, chips):
            push(slot, slot, kind + "x", on_chip(q), grad)

    def of_z(ref, rows=slice(None)):
        return ref.at[0, :planes - 1, 0, rows]

    def of_x(ref, rows=slice(None)):
        return ref.at[0, :, :chips - 1, rows]

    seg_s[...] = jnp.zeros_like(seg_s)
    mark("m_gather")
    for n in early:
        loads[n].wait()
    samples, looks = dense.shape[0], d1.shape[1]
    per = looks // LANES
    for k, digit in enumerate((bag, d1, d2, d3)):
        for h in range(per):
            digits_ref[core, plane, chip, k * per + h:k * per + h + 1, :] = (
                digit[:, h * LANES:(h + 1) * LANES].astype(F32))
    hot1 = hot(d1[...], c1.shape[0], BF16)
    hot2 = hot(d2[...], c2.shape[0], BF16)
    hot3 = hot(d3[...], c3.shape[0], BF16)
    first_s[...] = dot(c1[...], hot1, DOWN)
    last_t = dot(c3[...], hot3, DOWN)
    last_s[...] = last_t
    lastd_s[...] = by_d3(last_t.astype(BF16))
    for k, n in enumerate(tables):
        loads[n].wait()
        for lo, size in spans(wide, 512):
            lo += k * wide
            mid_s[lo:lo + size, :] = dot(c2[:, lo:lo + size], hot2, DOWN)
    mark("m_left")
    left_into(left_s, first_s, mid_s)
    for n in late:
        loads[n].wait()
    mark("m_emb")
    embedded_into(emb_s, left_s, last_s)

    mark("m_top")
    bags = hot(bag[...], samples, BF16)
    pooled = dot_parts(bags, emb_s[...], ACROSS, 3, 1).astype(BF16)
    pre = (
        dot(dense[...], w[:WIDTH, :], PLAIN) + dot(pooled, w[WIDTH:, :], PLAIN)
        + bias[...]
    )
    sig = jax.nn.sigmoid(pre)
    hidden = pre * sig
    logit = jnp.sum(hidden * wout[...], axis=1, keepdims=True)
    rows = lax.broadcasted_iota(jnp.int32, (samples, samples), 0)
    cols = lax.broadcasted_iota(jnp.int32, (samples, samples), 1)
    label = jnp.sum(
        jnp.where(rows == cols, labels[...].astype(F32), 0.0), axis=1, keepdims=True
    )
    dlogit = (jax.nn.sigmoid(logit) - label) / samples
    dpre = dlogit * wout[...] * (sig * (1.0 + pre * (1.0 - sig)))
    low = dpre.astype(BF16)

    mark("m_topgrad")
    deep = plan.trows - 8
    vectors = jnp.concatenate(
        [jnp.sum(dpre, axis=0, keepdims=True), jnp.sum(hidden * dlogit, axis=0, keepdims=True),
         jnp.zeros((6, dpre.shape[1]), F32)], axis=0)
    weight = [dot(dense[...], low, DOWN), dot(pooled, low, DOWN)]
    for h in range(cores):
        lanes = slice(h * LANES, (h + 1) * LANES)
        for q in range(chips):
            lo = q * deep
            half = weight[lo // WIDTH]
            top_s[h, q, :deep, :] = half[lo % WIDTH:lo % WIDTH + deep, lanes]
            top_s[h, q, deep:, :] = vectors[:, lanes] if q == 0 else jnp.zeros((8, LANES), F32)
    mark("m_barrier")
    pl.semaphore_wait(barrier, len(peers))
    mark("m_send")
    push(top_s.at[1 - core], topin, "t0", on_core(1))
    push_x(digits_ref, "d", 0)
    gp = dot(low, w[WIDTH:, :], ACROSS)
    gp_ref[core, plane, chip] = gp
    most = slice(None)
    own_z(gp_ref, "g", most)

    mark("m_gleft")
    g_s[...] = dot_parts(gp, bags, DOWN, 2, 0)
    mark("m_gl")
    grad_last_into(gl_s, left_s, g_s)

    def seg_rows(first):
        return slice(0, plan.frows) if first else slice(plan.frows, plan.srows)

    def seg_start(first, value):
        for seg in plan.segs:
            if seg.first == first:
                for c, q, lo, hi, h in pieces_of(seg, cores, chips, cores):
                    seg_s[c, q, seg.offset:seg.offset + hi - lo, :] = (
                        value[lo:hi, h * LANES:(h + 1) * LANES])
        rows = seg_rows(first)
        push(seg_s.at[1 - core, :, rows], segin.at[:, rows], "f0" if first else "l0", on_core(1))

    def seg_chips(first):
        rows = seg_rows(first)
        arrive(segin.at[:, rows], "f0" if first else "l0")
        seg1[:, rows] = seg_s[core, :, rows] + segin[:, rows]
        for k in range(1, chips):
            push(seg1.at[(chip + k) % chips, rows], segx.at[k, rows],
                 "f1" if first else "l1", on_chip(k))

    def out_of(p, k):
        seg = plan.segs[(p + k) % planes]
        return remote(seg2.at[seg.offset:seg.offset + seg.rows],
                      segz.at[k, :seg.rows], "s2", on_plane(k))

    def seg_planes(first):
        rows = seg_rows(first)
        arrive(segx.at[1:, rows], "f1" if first else "l1")
        total = seg1[chip, rows]
        for k in range(1, chips):
            total = total + segx[k, rows]
        seg2[rows] = total
        for p in range(planes):
            @pl.when(plane == p)
            def _(p=p):
                for k in range(1, planes):
                    if plan.segs[(p + k) % planes].first == first:
                        out_of(p, k).start()

    mark("m_ldot")
    seg_start(False, dot_parts(hot3, gl_s[...], ACROSS, 2, 1))
    mark("m_gleft2")
    grad_left_into(gleft_s, g_s, lastd_s)
    mark("m_t0")
    arrive(topin, "t0")
    top1[...] = top_s[core] + topin[...]
    for k in range(1, chips):
        push(top1.at[(chip + k) % chips], topx.at[k], "t1", on_chip(k))

    mark("m_gf")
    grad_first_into(gf_s, gleft_s, mid_s, 0, 2)
    mark("m_l0")
    seg_chips(False)
    mark("m_dx")
    arrive(digits_ref.at[0, 0, :chips - 1], "dx")
    for k in range(1, planes):
        push(digits_ref.at[core, plane], digits_ref.at[core, plane], "dz", on_plane(k))
    push_x(gp_ref, "g", 0, 0, most)
    mark("m_gf2")
    grad_first_into(gf_s, gleft_s, mid_s, 1, 2)
    mark("m_fdot")
    seg_start(True, dot_parts(hot1, gf_s[...], ACROSS, 2, 1))
    mark("m_f0")
    seg_chips(True)

    mark("m_gz")
    arrive(of_z(gp_ref, most), "gz")
    for k in range(1, planes):
        push_x(gp_ref, "g", k, k, most)
    mark("m_t1")
    arrive(topx.at[1:], "t1")
    total = top1[chip]
    for k in range(1, chips):
        total = total + topx[k]
    topz[plane] = total
    for k in range(1, planes):
        push(topz.at[plane], topz.at[plane], "t2", on_plane(k))

    mark("m_dz")
    arrive(digits_ref.at[0, :planes - 1], "dz")
    push(digits_ref.at[core], digits_ref.at[core], "dc", on_core(1))
    mark("m_df")
    arrive(digits_ref.at[1 - core], "dc")
    mark("m_rank")
    groups = cores * planes * chips
    count, fullest = rank_lookups(
        plan, digits_ref[...].reshape(groups, *digits_ref.shape[3:]), rank_s, vals_s, local_s)
    fits = (count <= found_s.shape[1]) & (fullest <= few_s.shape[0] // groups)
    rest_ref[...] = jnp.broadcast_to(jnp.where(fits, 0.0, 1.0), rest_ref.shape)
    mark("m_pick")
    pick_few_into(found_s, local_s, vals_s, few_s)

    mark("m_l1")
    seg_planes(False)
    mark("m_f1")
    seg_planes(True)
    mark("m_factors")
    factors_into(plan, samples, spread_s, lsel_s, sample_s, found_s, c1, c3)
    mark("m_t2")
    arrive(topz.at[1:], "t2")
    total = topz[0]
    for k in range(1, planes):
        total = total + topz[k]
    top_ref[core, chip] = total
    for k in range(1, chips):
        push(top_ref.at[core, chip], top_ref.at[core, chip], "t3", on_chip(k))

    mark("m_gx")

    def chosen_sum(c):
        size = planes * chips * samples
        return dot_parts(
            gp_ref[c].reshape(size, WIDTH), sample_s[pl.ds(pl.multiple_of(c * size, size), size), :],
            DOWN, 2, 0)

    for k in range(planes):
        slot = gp_ref.at[core, back(plane, k, planes)]
        arrive(gp_ref.at[0, 0, :chips - 1, most], "gx", k)
        push(slot, slot, "gc", on_core(1))
    gsel_s[...] = chosen_sum(core)

    mark("m_s2")

    def to_owner(p):
        seg = plan.segs[p]
        return remote(seg3.at[:seg.rows], seg_ref.at[core, chip, :seg.rows], "s3",
                      (seg.owner, plane))

    for p in range(planes):
        @pl.when(plane == p)
        def _(p=p):
            seg = plan.segs[p]
            arrive(segz.at[1:, :seg.rows], "s2")
            total = seg2[seg.offset:seg.offset + seg.rows]
            for k in range(1, planes):
                total = total + segz[k, :seg.rows]
            seg3[:seg.rows] = total

            @pl.when(gx != seg.owner)
            def _():
                to_owner(p).start()

    mark("m_t3")
    arrive(top_ref.at[0, 1:], "t3")
    push(top_ref.at[core], top_ref.at[core], "t4", on_core(1))

    mark("m_gfin")
    arrive(gp_ref.at[0], "gc")
    gsel_s[...] = gsel_s[...] + chosen_sum(1 - core)
    saves = [pltpu.make_async_copy(digits_ref, digits_out, save_sems.at[0]),
             pltpu.make_async_copy(gp_ref, gp_out, save_sems.at[1])]
    for save in saves:
        save.start()
    mark("m_mid")
    mid_ref[...] = middle_sum(plan, spread_s, lsel_s, gsel_s, glsel_s)

    mark("m_s3")
    for p in range(planes):
        seg = plan.segs[p]

        @pl.when((plane == p) & (gx == seg.owner))
        def _(p=p, seg=seg):
            own_core, own_chip = seg.owner % cores, seg.owner // cores
            seg_ref[own_core, own_chip, :seg.rows] = seg3[:seg.rows]
            arrive(segall.at[:(cores * chips - 1) * seg.rows], "s3")

    mark("m_t4")
    arrive(top_ref.at[1 - core], "t4")
    mark("m_sent")
    for save in saves:
        save.wait()
    leave(digits_ref.at[0, 0, :chips - 1], "dx")
    leave(digits_ref.at[0, :planes - 1], "dz")
    leave(of_z(gp_ref, most), "gz")
    leave(of_x(gp_ref, most), "gx")
    for ref, stage in ((digits_ref, "dc"), (gp_ref, "gc")):
        leave(ref.at[0], stage)
    for stage, like in (
        ("t0", topin), ("t1", topx.at[1:]), ("t2", topz.at[1:]), ("t3", top_ref.at[0, 1:]),
        ("t4", top_ref.at[0]), ("l0", segin.at[:, seg_rows(False)]),
        ("l1", segx.at[1:, seg_rows(False)]), ("f0", segin.at[:, seg_rows(True)]),
        ("f1", segx.at[1:, seg_rows(True)])):
        leave(like, stage)
    for p in range(planes):
        @pl.when(plane == p)
        def _(p=p):
            seg = plan.segs[p]
            leave(seg2.at[:plan.srows - seg.rows], "s2")

            @pl.when(gx != seg.owner)
            def _():
                to_owner(p).wait_send()
    mark(None)


def step_part(plan, chunk, *inputs):
    c1, c2, c3, dense, w, bias, wout, labels, bag, d1, d2, d3 = inputs
    samples, looks = dense.shape[0], d1.shape[1]
    cores, chips, planes = plan.cores, plan.chips, plan.planes
    groups = cores * chips * planes
    vmem = pl.BlockSpec(memory_space=pltpu.VMEM)
    hbm = pl.BlockSpec(memory_space=pltpu.HBM)
    scratch = [R * SIDE, D1 * R, R * D3, R * D3, D1 * SIDE, D1 * SIDE, WIDTH, WIDTH, D1 * R, R * D3]
    top, seg = (plan.trows, LANES), (plan.srows, LANES)
    digits = (cores, planes, chips, up(4 * looks // LANES, 8), LANES)
    grads = (cores, planes, chips, samples, WIDTH)
    sums = [
        digits, grads,
        (cores, chips, *top), (chips, *top), (chips, *top), (chips, *top), (planes, *top),
        (cores, chips, *seg), (chips, *seg), (chips, *seg), (chips, *seg), seg,
        (planes, plan.smost, LANES), (plan.smost, LANES), (cores * chips * plan.smost, LANES)]
    inputs = [pltpu.with_memory_space_constraint(x, pltpu.HBM) for x in inputs]
    return pl.pallas_call(
        functools.partial(step_kernel, plan),
        in_specs=[hbm] * len(inputs),
        out_specs=(hbm, hbm, vmem, vmem, vmem, vmem),
        out_shape=(
            pltpu.HBM(digits, F32),
            pltpu.HBM(grads, F32),
            pltpu.VMEM((cores, chips, *top), F32),
            pltpu.VMEM((cores, chips, plan.smost, LANES), F32),
            pltpu.VMEM((plan.window * R, SIDE), F32),
            pltpu.VMEM((8, LANES), F32),
        ),
        scratch_shapes=[pltpu.VMEM(x.shape, x.dtype) for x in inputs]
        + [pltpu.VMEM((rows, looks), F32) for rows in scratch]
        + [pltpu.VMEM(dims, F32) for dims in sums]
        + select_scratch(plan, looks, samples, chunk)
        + [pltpu.VMEM((groups, looks), jnp.int32), pltpu.VMEM((groups * LOCAL, 8), F32)]
        + [pltpu.SemaphoreType.DMA((len(inputs) + 1,)), pltpu.SemaphoreType.DMA((2,))]
        + [pltpu.SemaphoreType.DMA((len(STAGES),)) for _ in range(2)]
        + [pltpu.SemaphoreType.DMA((planes,))],
        compiler_params=pltpu.CompilerParams(
            collective_id=0, has_side_effects=True, vmem_limit_bytes=40 << 20),
        name="step",
    )(*inputs)


def finish_kernel(
    plan, c1_in, c3_in, digits_in, gp_in, top, seg_in, mid, rest_in, core_out, top_out,
    c1, c3, blocks_s, gp_s, rank_s, vals_s, found_s, spread_s, lsel_s, sample_s, gsel_s, glsel_s,
    big_s, core_s, top_s, more_sems, out_sems,
):
    cores, chips, planes, window = plan.cores, plan.chips, plan.planes, plan.window
    gx, plane = lax.axis_index("gx"), lax.axis_index("gy")
    r0, start = first_row(plan)
    chunk = found_s.shape[1]

    deep = plan.trows - 8
    for h in range(cores):
        lanes = slice(h * LANES, (h + 1) * LANES)
        for q in range(chips):
            top_s[q * deep:(q + 1) * deep, lanes] = top[h, q, :deep, :]
        top_s[chips * deep:, lanes] = top[h, 0, deep:deep + 2, :]
    save_top = pltpu.make_async_copy(top_s, top_out, out_sems.at[0])
    save_top.start()

    base, rows = plan.n1 // LANES, window * R
    big_s[base:base + rows, :] = mid[...]

    @pl.when(jnp.max(rest_in[...]) > 0.0)
    def _():
        pairs = zip((c1_in, c3_in, digits_in, gp_in), (c1, c3, blocks_s, gp_s))
        loads = [pltpu.make_async_copy(a, b, more_sems.at[k]) for k, (a, b) in enumerate(pairs)]
        for load in loads:
            load.start()
        for load in loads:
            load.wait()
        groups, samples = rank_s.shape[0], gp_s.shape[3]
        count, _ = rank_lookups(
            plan, blocks_s[...].reshape(groups, *blocks_s.shape[3:]), rank_s, vals_s)
        count = jnp.max(count).astype(jnp.int32)
        big_s[base:base + rows, :] = jnp.zeros((rows, LANES), F32)

        def body(step, carry):
            pick_into(found_s, step, rank_s, vals_s)
            factors_into(plan, samples, spread_s, lsel_s, sample_s, found_s, c1, c3)
            gsel_s[...] = dot_parts(
                gp_s[...].reshape(groups * samples, WIDTH), sample_s[...], DOWN, 2, 0)
            big_s[base:base + rows, :] = big_s[base:base + rows, :] + middle_sum(
                plan, spread_s, lsel_s, gsel_s, glsel_s)
            return carry

        lax.fori_loop(0, (count + chunk - 1) // chunk, body, 0)

    halves = seg_in.shape[0]
    for p in range(planes):
        seg = plan.segs[p]

        @pl.when((plane == p) & (gx == seg.owner))
        def _(seg=seg):
            for c, q, lo, hi, h in pieces_of(seg, cores, chips, halves):
                piece = seg_in[c, q, :hi - lo, :]
                if seg.first:
                    big_s[lo:hi, :] = piece
                else:
                    big_s[pl.ds(base + rows + lo * halves + h, hi - lo, stride=halves), :] = piece

    at = start // LANES - r0 * (plan.row // LANES)
    shift = start % LANES
    size = core_s.shape[0]
    here, after = big_s[pl.ds(at, size), :], big_s[pl.ds(at + 1, size), :]
    turn = (LANES - shift) % LANES
    lane = lax.broadcasted_iota(jnp.int32, (size, LANES), 1)
    core_s[...] = jnp.where(
        lane < LANES - shift, pltpu.roll(here, turn, 1), pltpu.roll(after, turn, 1))
    save_core = pltpu.make_async_copy(core_s, core_out, out_sems.at[1])
    save_core.start()
    save_top.wait()
    save_core.wait()


def finish_part(plan, chunk, looks, c1, c3, digits, gp, top, seg, mid, rest):
    vmem = pl.BlockSpec(memory_space=pltpu.VMEM)
    hbm = pl.BlockSpec(memory_space=pltpu.HBM)
    out_rows = up(-(-plan.share // LANES), 8)
    big = up(plan.n1 // LANES + plan.window * R + plan.n3_rows * seg.shape[0] + out_rows, 8)
    core_shape = (out_rows, LANES)
    top_shape = (plan.chips * (plan.trows - 8) + 2, plan.cores * LANES)
    far = [pltpu.with_memory_space_constraint(x, pltpu.HBM) for x in (c1, c3, digits, gp)]
    return pl.pallas_call(
        functools.partial(finish_kernel, plan),
        out_shape=(pltpu.HBM(core_shape, F32), pltpu.HBM(top_shape, F32)),
        in_specs=[hbm] * 4 + [vmem] * 4,
        out_specs=(hbm, hbm),
        scratch_shapes=[pltpu.VMEM(x.shape, x.dtype) for x in (c1, c3, digits, gp)]
        + select_scratch(plan, looks, gp.shape[3], chunk)
        + [pltpu.VMEM((big, LANES), F32), pltpu.VMEM(core_shape, F32),
           pltpu.VMEM(top_shape, F32), pltpu.SemaphoreType.DMA((4,)), pltpu.SemaphoreType.DMA((2,))],
        compiler_params=pltpu.CompilerParams(vmem_limit_bytes=40 << 20),
        name="finish",
    )(*far, top, seg, mid, rest)


def per_device(plan, c1, c2, c3, dense, w, bias, wout, labels, bag, d1, d2, d3):
    looks = d1.shape[1]
    expected = plan.nx * plan.ny * looks * plan.window // plan.n2_rows
    chunk = up(expected * 9 // 8, LANES)
    digits, gp, top, seg, mid, rest = step_part(
        plan, chunk, c1, c2, c3, dense, w, bias[None], wout[None], labels[None], bag, d1, d2, d3)
    core, top = finish_part(plan, chunk, looks, c1, c3, digits, gp, top, seg, mid, rest)
    return core.reshape(-1)[:plan.share], top


def one_hot(digits, count, kind):
    return (digits[:, None] == jnp.arange(count, dtype=jnp.int32)[None, :]).astype(kind)


def slices(digits, core):
    return jnp.dot(
        one_hot(digits, core.shape[0], jnp.bfloat16), core, preferred_element_type=jnp.float32
    )


def factors(digits, cores):
    high = lax.Precision.HIGHEST
    first = slices(digits[0], cores[0]).reshape(-1, D1, R)
    middle = slices(digits[1], cores[1]).reshape(-1, R, D2 * R)
    last = slices(digits[2], cores[2]).reshape(-1, R, D3)
    left = jnp.einsum("nia,nab->nib", first, middle, precision=high).reshape(-1, D1 * D2, R)
    return (first, middle, last, left)


def top_total(top_local):
    return lax.psum(top_local, ("gx", "gy"))


def per_device_dense(
    core_one,
    core_two,
    core_three,
    dense_rows,
    w_top,
    bias_top,
    w_out,
    labels,
    bag_ids,
    digit_one,
    digit_two,
    digit_three,
):
    high = lax.Precision.HIGHEST
    cores = (core_one, core_two, core_three)
    digits = jnp.stack([digit_one[0], digit_two[0], digit_three[0]])
    looks = digits.shape[1]
    block = min(256, looks)
    blocks = looks // block
    blocked = digits.reshape(3, blocks, block).transpose(1, 0, 2)
    width = D1 * D2 * D3

    def forward(carry, part):
        first, middle, last, left = factors(part, cores)
        return (carry, jnp.einsum("npa,nad->npd", left, last, precision=high).reshape(block, width))

    _, embedded = lax.scan(forward, jnp.zeros((), jnp.float32), blocked)
    embedded = embedded.reshape(looks, width)
    samples = dense_rows.shape[0]
    bag_table = one_hot(bag_ids[0], samples, jnp.float32)
    pooled = jnp.dot(bag_table.T, embedded, precision=high)
    joined = jnp.concatenate([dense_rows, pooled.astype(jnp.bfloat16)], axis=1)
    pre = jnp.dot(joined, w_top, preferred_element_type=jnp.float32) + bias_top[None, :]
    sig = jax.nn.sigmoid(pre)
    hidden = pre * sig
    logit = jnp.dot(hidden, w_out, precision=high)
    dlogit = (jax.nn.sigmoid(logit) - labels.astype(jnp.float32)) / samples
    dpre = dlogit[:, None] * w_out[None, :] * (sig * (1.0 + pre * (1.0 - sig)))
    dpre_low = dpre.astype(jnp.bfloat16)
    grad_weight = jnp.dot(joined.T, dpre_low, preferred_element_type=jnp.float32)
    grad_bias = jnp.sum(dpre, axis=0)
    grad_output = jnp.sum(hidden * dlogit[:, None], axis=0)
    top_local = jnp.concatenate([grad_weight, grad_bias[None, :], grad_output[None, :]], axis=0)
    grad_pooled = jnp.dot(dpre_low, w_top[width:].T, preferred_element_type=jnp.float32)
    grad_embedded = jnp.dot(bag_table, grad_pooled, precision=high).reshape(blocks, block, width)

    def backward(totals, inputs):
        part, grad_block = inputs
        first, middle, last, left = factors(part, cores)
        grad_view = grad_block.reshape(block, D1 * D2, D3)
        grad_last = jnp.einsum("npa,npd->nad", left, grad_view, precision=high)
        grad_left = jnp.einsum("npd,nad->npa", grad_view, last, precision=high).reshape(
            block, D1, D2 * R
        )
        grad_first = jnp.einsum("nib,nab->nia", grad_left, middle, precision=high)
        grad_middle = jnp.einsum("nia,nib->nab", first, grad_left, precision=high)
        pieces = (
            grad_first.reshape(block, -1),
            grad_middle.reshape(block, -1),
            grad_last.reshape(block, -1),
        )
        updated = tuple(
            (
                total
                + jnp.dot(
                    one_hot(part[number], cores[number].shape[0], jnp.float32).T,
                    pieces[number],
                    precision=high,
                )
                for number, total in enumerate(totals)
            )
        )
        return (updated, None)

    start = tuple((jnp.zeros(core.shape, jnp.float32) for core in cores))
    totals, _ = lax.scan(backward, start, (blocked, grad_embedded))
    flat = jnp.concatenate([total.reshape(-1) for total in totals])
    core_grad = lax.psum_scatter(flat, ("gx", "gy"), scatter_dimension=0, tiled=True)
    top_grad = top_total(top_local)
    return (core_grad, top_grad)


def solution(mesh):
    nx, ny = mesh.shape["gx"], mesh.shape["gy"]
    whole, split, rows = P(), P(AXES), P(AXES, None)

    def step(*args):
        cores, dense = args[:3], args[3]
        plan = None
        if dense.size < sum(core.size for core in cores):
            plan = plan_of(nx, ny, *(core.shape for core in cores), args[4].shape)
        body = functools.partial(per_device, plan) if plan else per_device_dense
        return jax.shard_map(
            body,
            mesh=mesh,
            in_specs=(
                whole, whole, whole, rows, whole, whole, whole, split,
                rows, rows, rows, rows,
            ),
            out_specs=(split, whole),
            check_vma=False,
        )(*args)

    return step
```
